1024 devices in a mesh: dp: 64 (over y_lo, z), tp: 16 (over x, y_hi, core).
Axes of the slice: x: 4, y: 8 (y_hi: 2, y_lo: 4; y = y_hi * 4 + y_lo), z: 16, core: 2. Of those that a mesh axis runs over, the one named last changes fastest.
Arguments:
- queries: bfloat16 [16384, 4096], P('dp', 'tp'), may hold values from -6 to 6
- keys: bfloat16 [16384, 512], P(('dp', 'tp')), may hold values from -6 to 6
- values: bfloat16 [16384, 512], P(('dp', 'tp')), may hold values from -6 to 6
- out_weight: bfloat16 [4096, 8192], P('tp', 'dp'), may hold values from -0.09375 to 0.09375
- residual: bfloat16 [16384, 8192], P(('dp', 'tp')), may hold values from -40 to 40
- norm_gain: float32 [8192], replicated, may hold values from 0.5 to 1.5
Outputs:
- hidden_out: bfloat16 [16384, 8192], P(('dp', 'tp'))
- normed: bfloat16 [16384, 8192], P(('dp', 'tp'))
The draws below stay inside these ranges and needn't reach their ends.
All inputs are finite; a program needn't handle non-finite values.
Results may differ from the reference program's by a relative error of at most 0.012.
Values may be sent and summed in bfloat16 or wider, within the bound.
A program may use at most 32 MiB of HBM per device.

```python
import math
import jax
import jax.numpy as jnp
from jax import lax

D = 8192
HQ = 32
KVH = 4
HDIM = 128
LEN = 32
TOKENS = 16384
N_TP = 16


def draw_queries(key, part):
    base = jax.random.truncated_normal(jax.random.fold_in(key, 1), -6.0, 6.0, (TOKENS, HQ * HDIM), jnp.float32)
    return base.astype(jnp.bfloat16)


def draw_keys(key, part):
    base = jax.random.truncated_normal(jax.random.fold_in(key, 2), -6.0, 6.0, (TOKENS, KVH * HDIM), jnp.float32)
    return base.astype(jnp.bfloat16)


def draw_residual(key, part):
    base = jax.random.truncated_normal(jax.random.fold_in(key, 3), -6.0, 6.0, (TOKENS, D), jnp.float32)
    lowest = 0.08
    row_scale = jnp.exp(jax.random.uniform(jax.random.fold_in(key, 4), (TOKENS, 1), jnp.float32, math.log(lowest), math.log(10.0 * lowest)))
    column_scale = jnp.exp(jax.random.uniform(jax.random.fold_in(key, 5), (1, D), jnp.float32, math.log(0.35), math.log(3.5)))
    return jnp.clip(base * row_scale * column_scale, -40.0, 40.0).astype(jnp.bfloat16)


def level_of(rng, dims, shards, least, largest):
    loudness = 1.0
    for axis_at, blocks in shards:
        heights = jax.random.uniform(jax.random.fold_in(jax.random.fold_in(rng, 6), axis_at), (blocks,), jnp.float32, least / len(shards), largest / len(shards))
        loudness = loudness * jnp.repeat(jnp.exp(heights), dims[axis_at] // blocks).reshape((-1,) + (1,) * (len(dims) - 1 - axis_at))
    return loudness


def noise(rng, shape, scale, reach, cuts=(), held_as=jnp.bfloat16):
    factor_of = level_of(rng, shape, cuts, -0.22, 0.18) if cuts else 1.0
    result = jax.random.normal(rng, shape, jnp.float32) * scale * factor_of
    return jnp.minimum(jnp.maximum(result, -reach), reach).astype(held_as)


def setup_inputs(seed: int = 0) -> dict:
    key_of = jax.random.split(jax.random.key(seed), 7)
    return {
        "queries": draw_queries(jax.random.fold_in(key_of[6], 71), 0),
        "keys": draw_keys(jax.random.fold_in(key_of[6], 71), 0),
        "values": noise(key_of[2], (TOKENS, KVH * HDIM), 1.0, 6.0, ((0, 1024),)),
        "out_weight": noise(key_of[3], (HQ * HDIM, D), (HQ * HDIM) ** -0.5, 0.09375, ((0, 16), (1, 64))),
        "residual": draw_residual(jax.random.fold_in(key_of[6], 71), 0),
        "norm_gain": jnp.clip(1.0 + 0.1 * jax.random.normal(key_of[5], (D,), jnp.float32), 0.5, 1.5),
    }


def attend(queries, keys, values):
    sequences = queries.shape[0] // LEN
    group = HQ // KVH
    query_heads = queries.reshape(sequences, LEN, HQ, HDIM).astype(jnp.float32)
    key_heads = jnp.repeat(keys.reshape(sequences, LEN, KVH, HDIM).astype(jnp.float32), group, axis=2)
    value_heads = jnp.repeat(values.reshape(sequences, LEN, KVH, HDIM).astype(jnp.float32), group, axis=2)
    scores = jnp.einsum('slhd,smhd->shlm', query_heads, key_heads) / math.sqrt(HDIM)
    causal = jnp.arange(LEN)[:, None] >= jnp.arange(LEN)[None, :]
    scores = jnp.where(causal, scores, -1e+30)
    highest = lax.optimization_barrier(jnp.max(scores, axis=-1, keepdims=True))
    powers = jnp.exp(scores - highest)
    weights = (powers / lax.optimization_barrier(jnp.sum(powers, axis=-1, keepdims=True))).astype(jnp.bfloat16)
    attended = jnp.einsum('shlm,smhd->slhd', weights.astype(jnp.float32), value_heads)
    return attended.astype(jnp.bfloat16).reshape(queries.shape[0], HQ * HDIM)

def reference(queries, keys, values, out_weight, residual, norm_gain):
    attended = attend(queries, keys, values)
    width = HQ * HDIM // N_TP
    projected = jnp.zeros((queries.shape[0], D), jnp.float32)
    for block in range(N_TP):
        term = jnp.dot(attended[:, block * width:(block + 1) * width], out_weight[block * width:(block + 1) * width], preferred_element_type=jnp.float32)
        rounded = lax.optimization_barrier(term.astype(jnp.bfloat16))
        projected = projected + rounded.astype(jnp.float32)
    updated = residual.astype(jnp.float32) + projected
    hidden_out = updated.astype(jnp.bfloat16)
    meansq = lax.optimization_barrier(jnp.mean(updated * updated, axis=-1, keepdims=True))
    normed = (updated * lax.rsqrt(meansq + 1e-05) * norm_gain).astype(jnp.bfloat16)
    return (hidden_out, normed)
```

```python
import functools
import math

import jax
import jax.numpy as jnp
from jax import lax
from jax.experimental import pallas as pl
from jax.experimental.pallas import tpu as pltpu
from jax.sharding import Mesh
from jax.sharding import PartitionSpec as P

MESH = pl.DeviceIdType.MESH
F32, BF16 = jnp.float32, jnp.bfloat16

ORDER = (0, 1, -1, 3, -3, 2, -2, 4, -4, 6, -6, 5, -5, 7, -7, 8)
SLOT = {d: i for i, d in enumerate(ORDER)}
PIECES = 4
NT = (((1,), (1,)), ((), ()))


def kernel(
    q, k, v, w, res, gain, hid, nrm,
    qall, kvl, kvr, kvp, wv, wcross, wall, bias, att, psend, xr, ssend, rbuf, u, resv, gv, hidv, nrmv,
    lsem, ssem, qsem, qdsem, ksem, kxsem, kdsem, wsem, wcsem, wdsem, xsem, asem,
):
    yl, z, x, yh, c = (lax.axis_index(a) for a in ("yl", "z", "x", "yh", "c"))
    y = yh * 4 + yl
    sends = []

    def dev(dy=0, dz=0, dx=0, flip=False):
        yt = lax.rem(y + (dy + 8), 8)
        return (
            lax.rem(yt, 4),
            lax.rem(z + (dz + 16), 16),
            lax.rem(x + dx, 4),
            lax.div(yt, 4),
            1 - c if flip else c,
        )

    def remote(src, dst, send_sem, recv_sem, to):
        return pltpu.make_async_remote_copy(
            src_ref=src, dst_ref=dst, send_sem=send_sem, recv_sem=recv_sem, device_id=to, device_id_type=MESH
        )

    def send(src, dst, recv_sem, to):
        copy = remote(src, dst, ssem.at[len(sends)], recv_sem, to)
        copy.start()
        sends.append(copy)

    def received(dst, recv_sem):
        remote(dst, dst, ssem.at[0], recv_sem, dev(flip=True)).wait_recv()

    def halfway(gs, h):
        first = lax.div(yl + gs, 4)
        return 1 - first if h else first

    def keeper(gs):
        return jnp.where(lax.rem(yh + halfway(gs, 0), 2) == c, 0, 1)

    local = [
        pltpu.make_async_copy(w, wv, lsem.at[0]),
        pltpu.make_async_copy(k, kvl.at[0], lsem.at[1]),
        pltpu.make_async_copy(v, kvl.at[1], lsem.at[2]),
        pltpu.make_async_copy(q.at[:, c], qall.at[0, 0, 0], lsem.at[3]),
        pltpu.make_async_copy(res, resv, lsem.at[4]),
        pltpu.make_async_copy(gain, gv, lsem.at[5]),
    ]
    for copy in local:
        copy.start()
    peers = [dev(flip=True), dev(dy=1), dev(dy=-1), dev(dy=4)]
    peers += [dev(dz=d) for d in (1, -1, 2, -2, 3, -3)]
    peers += [dev(dx=d) for d in (1, 2, 3)]
    barrier = pltpu.get_barrier_semaphore()
    for peer in peers:
        pl.semaphore_signal(barrier, inc=1, device_id=peer, device_id_type=MESH)

    row = lax.broadcasted_iota(jnp.int32, (128, 128), 0)
    col = lax.broadcasted_iota(jnp.int32, (128, 128), 1)
    half = jnp.where(col < 64, c, 1 - c)
    place = half * 16 + lax.rem(col, 16)
    same = lax.div(row, 32) == lax.div(lax.rem(col, 64), 16)
    bias[...] = jnp.where(same & (place <= lax.rem(row, 32)), 0.0, -1e30)

    local[0].wait()
    turned = wv[...].astype(F32).T.astype(BF16)
    top, bottom = turned[:64], turned[64:]
    wall[0, 0, 0] = jnp.where(yh == 0, top, bottom)
    wcross[...] = jnp.where(yh == 0, bottom, top)
    local[1].wait()
    local[2].wait()
    kvr[0, 0, x] = kvl[:, :, pl.ds(pl.multiple_of(x * 128, 128), 128)]
    local[3].wait()

    pl.semaphore_wait(barrier, len(peers))

    def wsend(wk, source, hop):
        dst = SLOT[source - hop if source - hop != -8 else 8]
        send(wall.at[SLOT[source], wk, 0], wall.at[dst, wk, 0], wsem.at[dst, wk], dev(dz=hop))

    def worigin(wk):
        for hop in (3, -3, 1, -1):
            wsend(wk, 0, hop)

    def wgot(d, wk):
        received(wall.at[SLOT[d], wk, 0], wsem.at[SLOT[d], wk])

    def wrelay(wk, d):
        wgot(d, wk)
        sign = 1 if d < 0 else -1
        if abs(d) == 3:
            for hop in (3 * sign, sign, -sign):
                wsend(wk, d, hop)
        else:
            if (d < 0) == (wk == 0):
                wsend(wk, d, 2 * sign)
            for hop in (sign, -sign):
                wsend(wk, d, hop)

    def wpass(p, wk):
        send(
            wall.at[pl.ds(4 * p, 4), wk, 0], wall.at[pl.ds(4 * p, 4), wk, 1], wdsem.at[p, wk], dev(flip=True)
        )

    def wpassed(p, wk):
        received(wall.at[pl.ds(4 * p, 4), wk, 1], wdsem.at[p, wk])

    def place_of(r):
        return (r, 0) if r >= 0 else (r + 4, 1)

    def qsend(r, s, hop):
        gs, h = place_of(r)
        gt, ht = place_of(r - hop if r - hop != 4 else -4)
        send(qall.at[gs, h, s], qall.at[gt, ht, s], qsem.at[gt, ht, s], dev(dy=hop))

    def qgot(r, s):
        gs, h = place_of(r)
        received(qall.at[gs, h, s], qsem.at[gs, h, s])

    def qrelay(r, s):
        qgot(r, s)
        if abs(r) < 3 or s == (0 if r < 0 else 1):
            qsend(r, s, 1 if r < 0 else -1)

    def ksend(r, hop):
        gs, h = place_of(r)
        gt, ht = place_of(r - hop if r - hop != 4 else -4)
        if (gt, ht) == (0, 1):
            part = 0 if hop > 0 else 1
            rows = pl.ds(2 * part, 2)
            send(kvr.at[gs, h, rows], kvr.at[gt, ht, rows], ksem.at[gt, ht, part], dev(dy=hop))
        else:
            send(kvr.at[gs, h], kvr.at[gt, ht], ksem.at[gt, ht, 0], dev(dy=hop))

    def kgot(r):
        gs, h = place_of(r)
        if r == -4:
            for part in range(2):
                received(kvr.at[gs, h, pl.ds(2 * part, 2)], ksem.at[gs, h, part])
        else:
            received(kvr.at[gs, h], ksem.at[gs, h, 0])

    def krelay(r):
        kgot(r)
        ksend(r, 1 if r < 0 else -1)

    def kpass(gs):
        send(kvr.at[gs, 1 - keeper(gs)], kvp.at[gs], kdsem.at[gs], dev(flip=True))

    def kpassed(gs):
        received(kvp.at[gs], kdsem.at[gs])

    def attend(gs, h):
        kept = kvr[gs, keeper(gs)]
        passed = kvp[gs]
        keys = jnp.concatenate([kept[:, 0].reshape(64, 128), passed[:, 0].reshape(64, 128)], axis=0)
        values = jnp.concatenate([kept[:, 1].reshape(64, 128), passed[:, 1].reshape(64, 128)], axis=0)
        for s in range(2):
            for j in range(2):
                lanes = slice(j * 128, j * 128 + 128)
                queries = qall[gs, h, s, :, :, lanes].reshape(128, 128)
                scores = lax.dot_general(queries, keys, NT, preferred_element_type=F32)
                scores = scores * (1.0 / math.sqrt(128.0)) + bias[...]
                powers = jnp.exp(scores - jnp.max(scores, axis=-1, keepdims=True))
                weights = powers * (1.0 / jnp.sum(powers, axis=-1, keepdims=True))
                heads = jnp.dot(weights.astype(BF16), values, preferred_element_type=F32)
                att[gs, h, s, :, lanes] = heads.astype(BF16)

    def piece(gs, p):
        total = None
        for h in range(2):
            wk = halfway(gs, h)
            for s in range(2):
                rows = wall[pl.ds(4 * p, 4), wk, s].reshape(256, 256)
                term = lax.dot_general(att[gs, h, s], rows, NT, preferred_element_type=F32)
                total = term if total is None else total + term
        psend[gs, p] = total.astype(BF16).reshape(4, 32, 256)
        for d in (2, 1, 3):
            send(psend.at[gs, p, lax.rem(x + d, 4)], xr.at[gs, p, d - 1], xsem.at[gs, p, d - 1], dev(dx=d))

    pending = []

    def reduced(gs, p):
        total = psend[gs, p, x].astype(F32)
        for d in range(3):
            received(xr.at[gs, p, d], xsem.at[gs, p, d])
            total = total + xr[gs, p, d].astype(F32)
        ssend[gs, p] = total.astype(BF16).reshape(2, 16, 256)
        home = (lax.rem(yl + gs, 4), z, x, c)
        send(ssend.at[gs, p, 1 - c], rbuf.at[y, p], asem.at[y, p], home + (1 - c,))
        if gs:
            send(ssend.at[gs, p, c], rbuf.at[y, p], asem.at[y, p], home + (c,))
        else:
            copy = remote(ssend.at[0, p, c], rbuf.at[y, p], ssem.at[len(sends)], asem.at[y, p], home + (c,))
            sends.append(None)
            pending.append(copy)

            @pl.when(yh != c)
            def _():
                copy.start()

            @pl.when(yh == c)
            def _():
                rbuf[y, p] = ssend[0, p, c]

    squares = [jnp.zeros((16, 128), F32)]

    def finish(p):
        for source in range(8):

            @pl.when((y != source) | (yh != c))
            def _(source=source):
                received(rbuf.at[source, p], asem.at[source, p])

        low = lax.broadcasted_iota(jnp.int32, (16, 128), 1) < 64
        for part in range(4):
            for t in range(2):
                lanes = slice(t * 128, t * 128 + 128)
                a = rbuf[part, p, :, lanes].astype(F32)
                b = rbuf[4 + part, p, :, lanes].astype(F32)
                pair = (
                    jnp.where(low, a, pltpu.roll(b, 64, 1)),
                    jnp.where(low, pltpu.roll(a, 64, 1), b),
                )
                for i in range(2):
                    block = part * 16 + lax.rem(z + (ORDER[4 * p + 2 * t + i] + 16), 16)
                    at = pl.ds(pl.multiple_of(block * 128, 128), 128)
                    updated = resv[:, at].astype(F32) + pair[i]
                    u[:, at] = updated
                    hidv[:, at] = updated.astype(BF16)
                    squares[0] = squares[0] + updated * updated

    worigin(0)
    send(wcross, wall.at[0, 1, 0], wcsem.at[0], dev(dy=4))
    for d in (2, 1, 3):
        head = pl.ds(pl.multiple_of(lax.rem(x + d, 4) * 128, 128), 128)
        send(kvl.at[:, :, head], kvr.at[0, 0, x], kxsem.at[d - 1], dev(dx=d))
    send(q.at[:, 1 - c], qall.at[0, 0, 1], qdsem.at[0], dev(flip=True))
    qsend(0, 0, 1)
    qsend(0, 0, -1)
    received(qall.at[0, 0, 1], qdsem.at[0])
    qsend(0, 1, 1)
    qsend(0, 1, -1)
    qrelay(-1, 0)
    qrelay(1, 0)
    wrelay(0, -3)
    wrelay(0, 3)
    for d in range(1, 4):
        received(kvr.at[0, 0, lax.rem(x + (4 - d), 4)], kxsem.at[d - 1])
    ksend(0, 1)
    ksend(0, -1)
    qrelay(-1, 1)
    qrelay(1, 1)
    received(wall.at[0, 1, 0], wcsem.at[0])
    worigin(1)
    krelay(-1)
    krelay(1)
    qrelay(-2, 0)
    qrelay(2, 0)
    wrelay(0, -6)
    wrelay(0, 6)
    qrelay(-2, 1)
    qrelay(2, 1)
    wgot(1, 0)
    wgot(-1, 0)
    wpass(0, 0)
    krelay(-2)
    krelay(2)
    kpass(2)
    wrelay(1, -3)
    wrelay(1, 3)
    wgot(1, 1)
    wgot(-1, 1)
    wpass(0, 1)
    qrelay(-3, 0)
    qrelay(3, 0)
    wgot(2, 0)
    wgot(-2, 0)
    wgot(4, 0)
    wpass(1, 0)
    qrelay(-3, 1)
    qrelay(3, 1)
    kpassed(2)
    attend(2, 0)
    attend(2, 1)
    krelay(-3)
    krelay(3)
    kpass(1)
    kpass(3)
    wrelay(1, -6)
    wrelay(1, 6)
    wpassed(0, 0)
    wpassed(0, 1)
    piece(2, 0)
    wgot(2, 1)
    wgot(-2, 1)
    wgot(4, 1)
    wpass(1, 1)
    wgot(-4, 0)
    wgot(5, 0)
    wpass(2, 0)
    kpassed(1)
    attend(1, 0)
    attend(1, 1)
    kpassed(3)
    attend(3, 0)
    attend(3, 1)
    wgot(-4, 1)
    wgot(5, 1)
    wpass(2, 1)
    kgot(-4)
    kpass(0)
    qgot(-4, 0)
    qgot(-4, 1)
    wgot(-5, 0)
    wgot(7, 0)
    wgot(-7, 0)
    wgot(8, 0)
    wpass(3, 0)
    piece(1, 0)
    piece(3, 0)
    wgot(-5, 1)
    wgot(7, 1)
    wgot(-7, 1)
    wgot(8, 1)
    wpass(3, 1)
    kpassed(0)
    attend(0, 0)
    attend(0, 1)
    piece(0, 0)
    for p in range(1, PIECES):
        wpassed(p, 0)
        wpassed(p, 1)
        for gs in (2, 1, 3, 0):
            piece(gs, p)
        for gs in (2, 1, 3, 0):
            reduced(gs, p - 1)
    for gs in (2, 1, 3, 0):
        reduced(gs, PIECES - 1)
    local[4].wait()
    local[5].wait()
    for p in range(PIECES):
        finish(p)
    scale = lax.rsqrt(jnp.sum(squares[0], axis=-1, keepdims=True) * (1.0 / 8192.0) + 1e-05)
    out = pltpu.make_async_copy(hidv, hid, lsem.at[6])
    out.start()
    for block in range(64):
        lanes = slice(block * 128, block * 128 + 128)
        nrmv[:, lanes] = (u[:, lanes] * scale * gv[block : block + 1, :]).astype(BF16)
    last = pltpu.make_async_copy(nrmv, nrm, lsem.at[7])
    last.start()
    for copy in sends:
        if copy is not None:
            copy.wait_send()
    for copy in pending:

        @pl.when(yh != c)
        def _(copy=copy):
            copy.wait_send()

    out.wait()
    last.wait()


def local(queries, keys, values, out_weight, residual, norm_gain):
    any_space = pl.BlockSpec(memory_space=pl.ANY)
    vmem = pltpu.VMEM
    dma = pltpu.SemaphoreType.DMA
    return pl.pallas_call(
        kernel,
        out_shape=(jax.ShapeDtypeStruct((16, 8192), BF16),) * 2,
        in_specs=[any_space] * 6,
        out_specs=(any_space,) * 2,
        scratch_shapes=[
            vmem((4, 2, 2, 4, 32, 256), BF16),
            vmem((2, 16, 512), BF16),
            vmem((4, 2, 4, 2, 16, 128), BF16),
            vmem((4, 4, 2, 16, 128), BF16),
            vmem((256, 128), BF16),
            vmem((64, 256), BF16),
            vmem((16, 2, 2, 64, 256), BF16),
            vmem((128, 128), F32),
            vmem((4, 2, 2, 128, 256), BF16),
            vmem((4, PIECES, 4, 32, 256), BF16),
            vmem((4, PIECES, 3, 32, 256), BF16),
            vmem((4, PIECES, 2, 16, 256), BF16),
            vmem((8, PIECES, 16, 256), BF16),
            vmem((16, 8192), F32),
            vmem((16, 8192), BF16),
            vmem((64, 128), F32),
            vmem((16, 8192), BF16),
            vmem((16, 8192), BF16),
            dma((8,)),
            dma((200,)),
            dma((4, 2, 2)),
            dma((1,)),
            dma((4, 2, 2)),
            dma((3,)),
            dma((4,)),
            dma((16, 2)),
            dma((1,)),
            dma((PIECES, 2)),
            dma((4, PIECES, 3)),
            dma((8, PIECES)),
        ],
        compiler_params=pltpu.CompilerParams(collective_id=0, has_side_effects=True),
        name="layer",
    )(
        queries.reshape(4, 2, 32, 256),
        keys,
        values,
        out_weight,
        residual,
        norm_gain.reshape(64, 128),
    )


def solution(mesh):
    finer = Mesh(mesh.devices.reshape(4, 16, 4, 2, 2), ("yl", "z", "x", "yh", "c"))
    rows, heads = ("yl", "z"), ("x", "yh", "c")
    both = rows + heads
    in_specs = (P(rows, heads), P(both, None), P(both, None), P(heads, rows), P(both, None), P())
    out_specs = (P(both, None), P(both, None))
    return jax.shard_map(local, mesh=finer, in_specs=in_specs, out_specs=out_specs, check_vma=False)
```

```python
import math

import jax
import jax.numpy as jnp
from jax import lax
from jax.experimental import pallas as pl
from jax.experimental.pallas import tpu as pltpu
from jax.sharding import Mesh
from jax.sharding import PartitionSpec as P

MESH = pl.DeviceIdType.MESH
F32, BF16 = jnp.float32, jnp.bfloat16
NT = (((1,), (1,)), ((), ()))

QC, WC = 0, 1
VMEM = 60 * 1024 * 1024
PIECES = 4
GROUPS = (2, 1, 3, 0)

ORDER = (0, 1, -1, 3, -3, 2, -2, 4, -4, 6, -6, 5, -5, 7, -7, 8)
SLOT = {d: i for i, d in enumerate(ORDER)}

SPREAD = (
    {0: (3, -3, 1, -1), 3: (6, 4, 2), -3: (-6, -4, -2), 6: (8, 7, 5), -6: (-7, -5)},
    {0: (3, -3, 1, -1), 3: (6, 4, 2), -3: (-6, -4, -2), 6: (7, 5), -6: (8, -7, -5)},
)
RELAYS = [(wave, core, d) for wave in range(2) for core in range(2) for d in SPREAD[wave] if d]


def seat(d):
    return -d if d != 8 else 8


LEAVES = [
    [
        (d, wave, core)
        for d in ORDER[4 * p : 4 * p + 4]
        for wave in range(2)
        for core in range(2)
        if d and (wave, core, seat(d)) not in RELAYS
    ]
    for p in range(PIECES)
]

PLAN_Q = (
    ("q_begin",), ("q_own",),
    ("q_relay", -1, 0), ("q_relay", 1, 0), ("k_own",), ("q_relay", -1, 1), ("q_relay", 1, 1),
    ("q_relay", -2, 0), ("q_relay", 2, 0), ("k_relay", -1), ("k_relay", 1),
    ("q_relay", -2, 1), ("q_relay", 2, 1), ("k_relay", -2), ("k_relay", 2),
    ("q_relay", -3, 0), ("q_relay", 3, 0), ("attend", 2),
    ("q_relay", -3, 1), ("q_relay", 3, 1), ("k_relay", -3), ("k_relay", 3),
    ("attend", 1), ("attend", 3),
    ("q_last",), ("k_last",), ("attend", 0),
    ("w_passed", 0), ("piece", 0),
    ("w_passed", 1), ("piece", 1),
    ("reduced", 0, 2), ("reduced", 0, 1), ("reduced", 0, 3), ("reduced", 0, 0),
    ("reduced", 1, 2), ("reduced", 1, 1), ("reduced", 1, 3), ("reduced", 1, 0),
)

PLAN_W = (
    ("w_begin",), ("w_other",),
    ("w_relay", 0, WC, 3), ("w_relay", 0, WC, -3), ("w_relay", 0, QC, 3), ("w_relay", 0, QC, -3),
    ("w_crossed", WC), ("w_crossed", QC),
    ("w_relay", 0, WC, 6), ("w_relay", 0, WC, -6), ("w_relay", 0, QC, 6), ("w_relay", 0, QC, -6),
    ("w_relay", 1, WC, 3), ("w_relay", 1, WC, -3), ("w_relay", 1, QC, 3), ("w_relay", 1, QC, -3),
    ("w_got", 0), ("w_pass", 0),
    ("w_relay", 1, WC, 6), ("w_relay", 1, WC, -6), ("w_got", 1), ("w_pass", 1),
    ("w_relay", 1, QC, 6), ("w_relay", 1, QC, -6),
    ("a_got", 2), ("a_got", 1), ("a_got", 3), ("a_got", 0),
    ("w_got", 2), ("piece", 2),
    ("w_got", 3), ("piece", 3),
    ("reduced", 2, 2), ("reduced", 2, 1), ("reduced", 2, 3), ("reduced", 2, 0),
    ("reduced", 3, 2), ("reduced", 3, 1), ("reduced", 3, 3), ("reduced", 3, 0),
)


def kernel(
    q, k, v, w, sums,
    qall, kvl, kvr, wv, wt, wcross, wall, bias, att, psend, xr, ssend, rbuf, size,
    lsem, ssem, rsem, wpsem, atsem, xsem, asem, go,
):
    yl, z, x, yh, c = (lax.axis_index(a) for a in ("yl", "z", "x", "yh", "c"))
    y = yh * 4 + yl

    def dev(dy=0, dz=0, dx=0, core=None):
        yt = lax.rem(y + (dy + 8), 8)
        return (lax.rem(yt, 4), lax.rem(z + (dz + 16), 16), lax.rem(x + dx, 4), lax.div(yt, 4), c if core is None else core)

    def remote(src, dst, send_sem, recv_sem, to):
        return pltpu.make_async_remote_copy(
            src_ref=src, dst_ref=dst, send_sem=send_sem, recv_sem=recv_sem, device_id=to, device_id_type=MESH
        )

    sent = [0]

    def send(src, dst, recv_sem, to):
        remote(src, dst, ssem.at[0], recv_sem, to).start()
        sent[0] += math.prod(src.shape) * 2

    def received(dst, recv_sem):
        remote(dst, dst, ssem.at[0], recv_sem, dev(core=1 - c)).wait_recv()

    def sized(bytes_):
        assert bytes_ % 8192 == 0
        return size.at[pl.ds(0, bytes_ // 8192)]

    def half_of(r):
        return lax.div(lax.rem(y + (r + 8), 8), 4)

    w_load = pltpu.make_async_copy(w, wv, lsem.at[0])
    q_load = pltpu.make_async_copy(q, qall.at[0, yh, c], lsem.at[1])
    kv_load = [pltpu.make_async_copy(k, kvl.at[0], lsem.at[2]), pltpu.make_async_copy(v, kvl.at[1], lsem.at[2])]
    barrier = pltpu.get_barrier_semaphore()
    around_q = [dict(dy=1), dict(dy=-1), dict(dx=1), dict(dx=2), dict(dx=3)]
    hops = sorted({t - s for spread in SPREAD for s, ts in spread.items() for t in ts})
    around_w = [dict(dy=4)] + [dict(dz=d) for d in sorted({d for h in hops for d in (h, -h)})]

    @pl.when(c == QC)
    def _():
        for peer in around_q:
            pl.semaphore_signal(barrier, inc=1, device_id=dev(**peer), device_id_type=MESH)

    @pl.when(c == WC)
    def _():
        pl.semaphore_signal(barrier, inc=1, device_id=dev(core=QC), device_id_type=MESH)
        for peer in around_w:
            pl.semaphore_signal(barrier, inc=1, device_id=dev(**peer), device_id_type=MESH)

    w_load.start()
    for copy in kv_load:
        copy.start()
    q_load.start()

    w_load.wait()
    wt[...] = wv[...].astype(F32).T.astype(BF16).reshape(2, 64, 256)

    def lanes_of(half, core):
        return pl.ds(pl.multiple_of((half * 2 + core) * 256, 256), 256)

    def head_of(i):
        return pl.ds(pl.multiple_of(i * 128, 128), 128)

    def unit(d, wave, core):
        return wall.at[SLOT[d], :, lanes_of(1 - yh if wave else yh, core)]

    def w_sem(d, wave, core):
        if d == 0:
            return rsem.at[core if wave else 2]
        if (wave, core, seat(d)) in RELAYS:
            return rsem.at[3 + PIECES + RELAYS.index((wave, core, seat(d)))]
        return rsem.at[3 + SLOT[d] // 4]

    def w_spread(wave, core, d):
        for t in SPREAD[wave].get(d, ()):
            send(unit(seat(d), wave, core), unit(seat(t), wave, core), w_sem(seat(t), wave, core), dev(dz=t - d))

    def w_origin(core):
        send(wcross.at[core], wall.at[0, :, lanes_of(yh, core)], w_sem(0, 1, core), dev(dy=4))
        w_spread(0, core, 0)

    def w_other():
        received(sized(65536), rsem.at[2])
        w_origin(QC)

    def w_crossed(core):
        received(unit(0, 1, core), w_sem(0, 1, core))
        w_spread(1, core, 0)

    def w_relay(wave, core, d):
        received(unit(seat(d), wave, core), w_sem(seat(d), wave, core))
        w_spread(wave, core, d)

    def w_got(p):
        received(sized(len(LEAVES[p]) * 32768), rsem.at[3 + p])

    def w_pass(p):
        rows = pl.ds(4 * p, 4)
        send(wall.at[rows], wall.at[rows], wpsem.at[p], dev(core=QC))

    def w_passed(p):
        received(wall.at[pl.ds(4 * p, 4)], wpsem.at[p])

    def q_send(r, s, hop):
        t = (r - hop) % 8
        sem = rsem.at[0 if t == 4 else 1 + 2 * t + s]
        send(qall.at[r % 4, half_of(r), s], qall.at[t % 4, half_of(r), s], sem, dev(dy=hop))

    def q_relay(r, s):
        received(qall.at[r % 4, half_of(r), s], rsem.at[1 + 2 * (r % 8) + s])
        if abs(r) < 3 or s == (0 if r < 0 else 1):
            q_send(r, s, 1 if r < 0 else -1)

    def q_last():
        received(qall.at[0, half_of(4)], rsem.at[0])

    def k_send(r, hop):
        t = (r - hop) % 8
        some = pl.ds(0 if hop > 0 else 2, 2) if t == 4 else pl.ds(0, 4)
        send(kvr.at[r % 4, half_of(r), some], kvr.at[t % 4, half_of(r), some], rsem.at[17 + t], dev(dy=hop))

    def k_relay(r):
        received(kvr.at[r % 4, half_of(r)], rsem.at[17 + r % 8])
        k_send(r, 1 if r < 0 else -1)

    def k_last():
        received(kvr.at[0, half_of(4)], rsem.at[21])

    def k_spread():
        for copy in kv_load:
            copy.wait()
        for d in (2, 1, 3):
            head = head_of(lax.rem(x + d, 4))
            send(kvl.at[:, :, head], kvr.at[0, yh, x, :, c], rsem.at[17], dev(dx=d, core=QC))

    def k_own():
        received(sized(7 * 8192), rsem.at[17])
        k_send(0, 1)
        k_send(0, -1)

    def q_own():
        received(qall.at[0, yh, WC], rsem.at[1 + WC])
        q_send(0, WC, 1)
        q_send(0, WC, -1)

    def q_begin():
        pl.semaphore_wait(barrier, len(around_q) + 1)
        pl.semaphore_signal(go, inc=1, device_id=dev(core=WC), device_id_type=MESH)
        send(wt.at[yh], unit(0, 0, QC), rsem.at[2], dev(core=WC))
        send(wt.at[1 - yh], wcross.at[QC], rsem.at[2], dev(core=WC))
        k_spread()
        kvr[0, yh, x, :, QC] = kvl[:, :, head_of(x)]
        q_load.wait()
        q_send(0, QC, 1)
        q_send(0, QC, -1)
        row = lax.broadcasted_iota(jnp.int32, (128, 128), 0)
        col = lax.broadcasted_iota(jnp.int32, (128, 128), 1)
        bias[...] = jnp.where((lax.div(row, 32) == lax.div(col, 32)) & (col <= row), 0.0, -1e30)

    def w_greet():
        pl.semaphore_wait(barrier, len(around_w))
        w_origin(WC)

    def w_give():
        pl.semaphore_wait(go, 1)
        q_load.wait()
        send(qall.at[0, yh, WC], qall.at[0, yh, WC], rsem.at[1 + WC], dev(core=QC))
        k_spread()
        send(kvl.at[:, :, head_of(x)], kvr.at[0, yh, x, :, WC], rsem.at[17], dev(core=QC))

    def w_begin():
        wall[0, :, lanes_of(yh, WC)] = wt[yh]
        wcross[WC] = wt[1 - yh]
        before = sent[0]

        @pl.when(z < 8)
        def _():
            w_give()
            w_greet()

        sent[0] = before

        @pl.when(z >= 8)
        def _():
            w_greet()
            w_give()

    def attend(gs):
        for t in range(2):
            pair = kvr[gs, t]
            keys, values = pair[:, 0].reshape(128, 128), pair[:, 1].reshape(128, 128)
            values = jnp.concatenate([values, jnp.ones((128, 128), BF16)], axis=1)
            for h in range(2):
                queries = jnp.concatenate(
                    [
                        qall[gs, h, s, :, j * 128 : j * 128 + 128].reshape(4, 2, 32, 128)[:, t].reshape(128, 128)
                        for s in range(2)
                        for j in range(2)
                    ],
                    axis=0,
                )
                scores = lax.dot_general(queries, keys, NT, preferred_element_type=F32)
                scores = scores * (1.0 / math.sqrt(128.0)) + jnp.concatenate([bias[...]] * 4, axis=0)
                powers = jnp.exp(scores - jnp.max(scores, axis=-1, keepdims=True)).astype(BF16)
                sums = jnp.dot(powers, values, preferred_element_type=F32)
                heads = (sums[:, :128] / sums[:, 128:]).astype(BF16)
                for i in range(4):
                    att[gs, t, :, h * 512 + i * 128 : h * 512 + i * 128 + 128] = heads[i * 128 : i * 128 + 128]
        send(att.at[gs], att.at[gs], atsem.at[gs], dev(core=WC))

    def a_got(gs):
        received(att.at[gs], atsem.at[gs])

    def piece(p):
        rows = wall[4 * p : 4 * p + 4].reshape(256, 1024)
        total = lax.dot_general(att[...].reshape(1024, 1024), rows, NT, preferred_element_type=F32)
        psend[p % 2] = total.astype(BF16).reshape(4, 2, 4, 32, 256)
        for gs in GROUPS:
            for d in (2, 1, 3):
                there = lax.rem(x + d, 4)
                send(psend.at[p % 2, gs, :, there], xr.at[p % 2, gs, d - 1], xsem.at[p % 2, gs], dev(dx=d))

    def reduced(p, gs):
        received(xr.at[p % 2, gs], xsem.at[p % 2, gs])
        total = psend[p % 2, gs, :, x].astype(F32)
        for d in range(3):
            total = total + xr[p % 2, gs, d].astype(F32)
        ssend[p % 2, gs] = total.astype(BF16).reshape(2, 2, 16, 256)
        for other in (1, 0):
            half = 1 - yh if other else yh
            there = half * 4 + lax.rem(yl + gs, 4)
            place = lax.rem(y + 8 - there, 8)
            for core in (1 - c, c):
                home = (lax.rem(yl + gs, 4), z, x, half, core)
                if gs or other:
                    send(ssend.at[p % 2, gs, half, core], rbuf.at[p, place], asem.at[p], home)
                elif core is c:
                    rbuf[p, 0] = ssend[p % 2, 0, yh, c]
                else:
                    send(ssend.at[p % 2, 0, yh, core], rbuf.at[p, 0], asem.at[4 + p % 2], home)

    steps = dict(
        q_begin=q_begin, w_begin=w_begin, q_own=q_own, q_relay=q_relay, q_last=q_last, k_own=k_own, k_relay=k_relay,
        k_last=k_last, attend=attend, w_origin=w_origin, w_other=w_other, w_crossed=w_crossed, w_relay=w_relay,
        w_got=w_got, w_pass=w_pass, w_passed=w_passed, a_got=a_got, piece=piece, reduced=reduced,
    )

    def follow(plan):
        sent[0] = 0
        for name, *numbers in plan:
            with jax.named_scope("_".join(map(str, (name, *numbers)))):
                steps[name](*numbers)

    def arrive(mine):
        with jax.named_scope("arrive"):
            outs = []
            for p in range(PIECES):
                received(rbuf.at[p, pl.ds(1, 7)], asem.at[p])
                if p // 2 != mine:
                    received(rbuf.at[p, 0], asem.at[4 + p % 2])
                outs.append(pltpu.make_async_copy(rbuf.at[p], sums.at[p], lsem.at[3 + p]))
                outs[-1].start()
            stand_in = sized(sent[0])
            remote(stand_in, stand_in, ssem.at[0], ssem.at[0], dev(core=1 - c)).wait_send()
            for copy in outs:
                copy.wait()

    @pl.when(c == QC)
    def _():
        follow(PLAN_Q)
        arrive(0)

    @pl.when(c == WC)
    def _():
        follow(PLAN_W)
        arrive(1)


def last_kernel(sums, res, gain, hid, nrm, rbuf, resv, gv, u, hidv, nrmv, sem):
    yl, z, yh = (lax.axis_index(a) for a in ("yl", "z", "yh"))
    y = yh * 4 + yl
    loads = [
        pltpu.make_async_copy(res, resv, sem.at[0]),
        pltpu.make_async_copy(gain, gv, sem.at[0]),
    ]
    loads += [pltpu.make_async_copy(sums.at[p], rbuf.at[p], sem.at[1 + p]) for p in range(PIECES)]
    for copy in loads:
        copy.start()
    for copy in loads[:2]:
        copy.wait()
    squares = jnp.zeros((16, 128), F32)
    low = lax.broadcasted_iota(jnp.int32, (16, 128), 1) < 64
    for p in range(PIECES):
        loads[2 + p].wait()
        for r in range(4):
            here = lax.div(lax.rem(y + r, 8), 4)
            first, second = r + 4 * here, r + 4 - 4 * here
            for t in range(2):
                lanes = slice(t * 128, t * 128 + 128)
                a = rbuf[p, first, :, lanes].astype(F32)
                b = rbuf[p, second, :, lanes].astype(F32)
                pair = (jnp.where(low, a, pltpu.roll(b, 64, 1)), jnp.where(low, pltpu.roll(a, 64, 1), b))
                for i in range(2):
                    block = lax.rem(yl + r, 4) * 16 + lax.rem(z + (ORDER[4 * p + 2 * t + i] + 16), 16)
                    at = pl.ds(pl.multiple_of(block * 128, 128), 128)
                    updated = resv[:, at].astype(F32) + pair[i]
                    u[:, at] = updated
                    hidv[:, at] = updated.astype(BF16)
                    squares = squares + updated * updated
    stores = [pltpu.make_async_copy(hidv, hid, sem.at[5])]
    stores[0].start()
    scale = lax.rsqrt(jnp.sum(squares, axis=-1, keepdims=True) * (1.0 / 8192.0) + 1e-05)
    for part in range(2):
        for block in range(32 * part, 32 * part + 32):
            lanes = slice(block * 128, block * 128 + 128)
            nrmv[:, lanes] = (u[:, lanes] * scale * gv[block : block + 1, :]).astype(BF16)
        lanes = pl.ds(4096 * part, 4096)
        stores.append(pltpu.make_async_copy(nrmv.at[:, lanes], nrm.at[:, lanes], sem.at[6 + part]))
        stores[-1].start()
    for copy in stores:
        copy.wait()


def local(queries, keys, values, out_weight, residual, norm_gain):
    in_hbm = pl.BlockSpec(memory_space=pltpu.HBM)
    vmem = pltpu.VMEM
    dma = pltpu.SemaphoreType.DMA
    sums = pl.pallas_call(
        kernel,
        out_shape=jax.ShapeDtypeStruct((PIECES, 8, 16, 256), BF16),
        in_specs=[in_hbm] * 4,
        out_specs=in_hbm,
        scratch_shapes=[
            vmem((4, 2, 2, 256, 256), BF16),
            vmem((2, 16, 512), BF16),
            vmem((4, 2, 4, 2, 2, 16, 128), BF16),
            vmem((256, 128), BF16),
            vmem((2, 64, 256), BF16),
            vmem((2, 64, 256), BF16),
            vmem((16, 64, 1024), BF16),
            vmem((128, 128), F32),
            vmem((4, 2, 128, 1024), BF16),
            vmem((2, 4, 2, 4, 32, 256), BF16),
            vmem((2, 4, 3, 2, 32, 256), BF16),
            vmem((2, 4, 2, 2, 16, 256), BF16),
            vmem((PIECES, 8, 16, 256), BF16),
            vmem((800, 16, 256), BF16),
            dma((3 + PIECES,)),
            dma((1,)),
            dma((max(25, 3 + PIECES + len(RELAYS)),)),
            dma((2,)),
            dma((4,)),
            dma((2, 4)),
            dma((6,)),
            pltpu.SemaphoreType.REGULAR,
        ],
        compiler_params=pltpu.CompilerParams(collective_id=0, has_side_effects=True, vmem_limit_bytes=VMEM),
        name="layer",
    )(queries, keys, values, out_weight)
    return pl.pallas_call(
        last_kernel,
        out_shape=(jax.ShapeDtypeStruct((16, 8192), BF16),) * 2,
        in_specs=[in_hbm] * 3,
        out_specs=(in_hbm,) * 2,
        scratch_shapes=[
            vmem((PIECES, 8, 16, 256), BF16),
            vmem((16, 8192), BF16),
            vmem((64, 128), F32),
            vmem((16, 8192), F32),
            vmem((16, 8192), BF16),
            vmem((16, 8192), BF16),
            dma((8,)),
        ],
        compiler_params=pltpu.CompilerParams(vmem_limit_bytes=VMEM),
        name="final",
    )(sums, residual, norm_gain.reshape(64, 128))


def solution(mesh):
    finer = Mesh(mesh.devices.reshape(4, 16, 4, 2, 2), ("yl", "z", "x", "yh", "c"))
    rows, heads = ("yl", "z"), ("x", "yh", "c")
    both = rows + heads
    in_specs = (P(rows, heads), P(both, None), P(both, None), P(heads, rows), P(both, None), P())
    out_specs = (P(both, None), P(both, None))
    return jax.shard_map(local, mesh=finer, in_specs=in_specs, out_specs=out_specs, check_vma=False)
```

```python
import math

import jax
import jax.numpy as jnp
from jax import lax
from jax.experimental import pallas as pl
from jax.experimental.pallas import tpu as pltpu
from jax.sharding import Mesh
from jax.sharding import PartitionSpec as P

MESH = pl.DeviceIdType.MESH
F32, BF16 = jnp.float32, jnp.bfloat16
NT = (((1,), (1,)), ((), ()))

QC, WC = 0, 1
VMEM = 60 * 1024 * 1024
PIECES = 4

ORDER = (
    (0, 2, 3, 1, 4, 13, 5, 12, 7, 11, 6, 10, 15, 14, 9, 8),
    (1, 0, 2, 4, 3, 5, 6, 7, 13, 12, 15, 14, 11, 10, 9, 8),
    (2, 1, 3, 0, 5, 6, 4, 7, 15, 14, 8, 13, 9, 10, 11, 12),
    (3, 1, 0, 2, 5, 4, 6, 7, 8, 15, 12, 9, 10, 11, 14, 13),
    (4, 3, 2, 0, 1, 7, 6, 9, 15, 10, 14, 13, 12, 5, 8, 11),
    (5, 6, 1, 7, 2, 0, 4, 10, 9, 15, 8, 11, 3, 13, 12, 14),
    (6, 4, 3, 10, 2, 7, 1, 8, 11, 9, 12, 14, 13, 15, 5, 0),
    (7, 6, 9, 4, 3, 1, 2, 10, 5, 11, 8, 12, 15, 14, 0, 13),
    (8, 7, 9, 6, 10, 5, 3, 12, 14, 11, 0, 4, 1, 15, 2, 13),
    (9, 8, 10, 11, 6, 12, 7, 5, 14, 4, 3, 2, 1, 15, 0, 13),
    (10, 9, 8, 11, 7, 12, 13, 14, 0, 1, 4, 3, 5, 6, 2, 15),
    (11, 10, 8, 12, 13, 9, 14, 0, 15, 5, 1, 7, 4, 6, 2, 3),
    (12, 11, 13, 10, 9, 8, 0, 15, 14, 7, 4, 5, 1, 6, 3, 2),
    (13, 0, 14, 15, 8, 1, 2, 7, 6, 5, 9, 3, 11, 10, 4, 12),
    (14, 13, 15, 2, 1, 8, 6, 0, 9, 7, 11, 10, 12, 4, 3, 5),
    (15, 14, 13, 9, 12, 2, 11, 1, 10, 0, 8, 6, 7, 5, 3, 4),
)

FIRST = (
    (1, 2, 3, 5),
    (0, 2, 3, 4, 5),
    (0, 1, 3, 4, 6),
    (0, 2, 4, 6),
    (1, 2, 3, 5, 6, 7),
    (2, 3, 4, 6, 7),
    (2, 4, 5, 7),
    (2, 3, 5, 6),
    (3, 4, 5, 6, 7, 9, 10, 11, 12, 13),
    (4, 5, 6, 7, 8, 10, 11, 12),
    (0, 5, 6, 7, 8, 9, 11, 12, 13),
    (0, 6, 7, 9, 10, 12, 13),
    (0, 9, 10, 11, 13, 14, 15),
    (0, 3, 8, 10, 11, 12, 14, 15),
    (0, 1, 2, 3, 4, 8, 9, 10, 11, 13, 15),
    (0, 1, 2, 4, 11, 12, 13, 14),
)

ROUTES = (
    (
        (0, 0, 0, 0, 1, 5, 2, 3), (0, 0, 1, 0, 1, 5, 2, 3), (0, 1, 0, 0, 1, 3, 5, 2), (0, 1, 1, 0, 1, 3, 5, 2),
        (0, 0, 0, 2, 1), (0, 0, 1, 2, 1), (0, 0, 0, 3, 1), (0, 0, 1, 3, 1), (0, 0, 0, 1), (0, 0, 1, 1), (3, 13),
        (1, 0, 0, 0, 13), (1, 0, 1, 0, 13), (1, 1, 0, 0, 13), (1, 1, 1, 0, 13), (1, 0, 0, 1, 13), (1, 0, 1, 1, 13),
        (0, 1, 0, 2, 1), (3, 14), (1, 0, 0, 2, 14), (1, 0, 1, 2, 14), (1, 0, 0, 1, 14), (1, 0, 1, 1, 14),
        (1, 1, 0, 2, 14), (0, 1, 1, 2, 1, 14), (3, 15), (0, 1, 0, 3, 1), (0, 1, 1, 3, 1), (0, 0, 1, 13, 15, 1),
        (0, 1, 0, 1, 14, 13), (0, 0, 1, 12, 15, 3, 1), (0, 1, 1, 1, 14, 13), (2, 0), (0, 0, 1, 11, 15, 1),
        (0, 0, 0, 13, 15, 1), (0, 0, 0, 12, 15, 3, 1), (0, 0, 1, 10, 1, 15), (0, 0, 0, 11, 15, 1),
        (0, 0, 0, 10, 1, 15), (0, 1, 1, 13, 1, 15), (0, 1, 1, 12, 15, 3, 1), (0, 1, 0, 13, 1, 15),
        (0, 1, 1, 11, 15, 1), (0, 1, 0, 12, 15, 3, 1), (2, 1), (0, 1, 1, 10, 1, 15), (0, 0, 1, 8, 15, 1),
        (0, 0, 0, 8, 15, 1), (0, 1, 0, 11, 15, 1), (0, 1, 0, 10, 1, 15), (2, 2), (0, 1, 1, 8, 1, 15), (2, 3),
        (0, 1, 0, 8, 1, 15), (2, 4),
    ),
    (
        (0, 0, 0, 1, 5, 2), (0, 0, 1, 1, 5, 2), (0, 1, 0, 1, 5, 2), (0, 1, 1, 1, 5, 2), (0, 0, 0, 4, 0, 2, 3),
        (0, 0, 1, 4, 0, 2, 3), (0, 0, 0, 5, 0), (3, 14), (0, 0, 1, 5, 0), (0, 0, 1, 6, 0, 14), (0, 0, 0, 6, 0, 14),
        (0, 1, 0, 4, 2, 0, 3), (0, 1, 1, 4, 2, 0, 3), (2, 0), (0, 0, 1, 13, 4, 2), (0, 1, 0, 5, 0), (0, 1, 1, 5, 0),
        (0, 0, 1, 11, 2, 3), (0, 0, 0, 13, 4, 2), (0, 1, 1, 6, 0, 14), (0, 1, 0, 6, 0, 14), (0, 0, 0, 11, 2, 3),
        (0, 1, 1, 13, 4, 2), (2, 1), (0, 1, 0, 13, 4, 2), (0, 1, 1, 11, 3, 2), (2, 2), (0, 1, 0, 11, 3, 2), (2, 3),
        (2, 4),
    ),
    (
        (0, 0, 0, 2, 0, 4), (0, 0, 1, 2, 0, 4), (0, 0, 0, 1, 6, 3, 0), (0, 0, 1, 1, 6, 3, 0), (0, 1, 0, 2, 4, 0),
        (0, 1, 1, 2, 4, 0), (0, 0, 0, 5, 3, 1), (0, 0, 1, 5, 3, 1), (0, 0, 1, 6, 1, 4), (0, 1, 0, 1, 6, 0, 3),
        (0, 0, 0, 6, 1, 4), (0, 1, 1, 1, 6, 0, 3), (0, 0, 1, 7, 0, 1), (0, 0, 0, 7, 0, 1), (0, 1, 0, 5, 3, 1), (2, 0),
        (0, 0, 1, 15, 1, 3, 0, 4), (0, 1, 1, 5, 3, 1), (0, 0, 1, 14, 4, 0, 1), (0, 0, 0, 15, 1, 3, 0, 4),
        (0, 1, 1, 6, 4, 1), (0, 0, 0, 14, 4, 0, 1), (0, 1, 0, 6, 4, 1), (0, 1, 1, 7, 1, 0), (0, 1, 0, 7, 1, 0),
        (0, 1, 1, 15, 0, 4, 3, 1), (2, 1), (0, 1, 1, 14, 1, 0, 4), (0, 1, 0, 15, 0, 4, 3, 1), (0, 1, 0, 14, 1, 0, 4),
        (2, 2), (2, 3), (2, 4),
    ),
    (
        (0, 0, 0, 3, 4, 6, 2, 0), (0, 0, 1, 3, 4, 6, 2, 0), (0, 0, 0, 0, 4), (0, 1, 0, 3, 4, 2, 0, 6),
        (0, 1, 1, 3, 4, 2, 0, 6), (0, 0, 1, 0, 4), (3, 13), (3, 14), (0, 1, 0, 0, 4), (0, 0, 1, 8, 6, 2),
        (0, 1, 1, 0, 4), (2, 0), (0, 0, 0, 8, 6, 2), (0, 0, 1, 12, 2, 14, 13, 4), (0, 1, 1, 8, 2, 6), (2, 1),
        (0, 1, 0, 8, 2, 6), (0, 0, 0, 12, 2, 14, 13, 4), (0, 1, 1, 12, 2, 14, 13, 4), (0, 1, 0, 12, 2, 14, 13, 4),
        (2, 2), (2, 3), (2, 4),
    ),
    (
        (0, 0, 0, 4, 6, 1), (0, 0, 1, 4, 6, 1), (0, 0, 0, 2, 7, 6, 5, 3), (0, 0, 1, 2, 7, 6, 5, 3),
        (0, 1, 0, 4, 1, 6), (0, 1, 1, 4, 1, 6), (3, 14), (3, 15), (0, 1, 0, 2, 5, 3, 6, 7), (0, 1, 1, 2, 5, 3, 6, 7),
        (0, 0, 1, 9, 3, 5, 2, 6), (0, 0, 0, 9, 3, 5, 2, 6), (0, 0, 1, 15, 5, 7), (2, 0), (0, 0, 1, 14, 7, 6, 3),
        (0, 0, 0, 15, 5, 7), (0, 0, 0, 14, 7, 6, 3), (0, 1, 1, 9, 5, 6, 2, 3), (0, 0, 1, 13, 6, 3, 5),
        (0, 1, 1, 15, 7, 5), (0, 1, 0, 9, 5, 6, 2, 3), (2, 1), (0, 0, 0, 13, 6, 3, 5), (0, 1, 1, 14, 6, 7, 3),
        (0, 0, 0, 5, 15, 14, 6), (0, 1, 0, 15, 7, 5), (0, 1, 1, 13, 3, 5, 6), (0, 1, 0, 14, 6, 7, 3),
        (0, 1, 0, 13, 3, 5, 6), (2, 2), (0, 0, 1, 5, 15, 14, 6), (0, 1, 0, 5, 15, 14, 6), (0, 1, 1, 5, 15, 14, 6),
        (2, 3), (2, 4),
    ),
    (
        (0, 0, 0, 5, 2), (0, 0, 1, 5, 2), (0, 0, 0, 1, 4, 7), (0, 0, 1, 1, 4, 7), (0, 0, 1, 7, 4, 3, 6),
        (0, 1, 0, 5, 2), (0, 1, 1, 5, 2), (0, 0, 0, 7, 4, 3, 6), (3, 8), (1, 0, 0, 5, 8), (1, 0, 1, 5, 8),
        (1, 1, 0, 5, 8), (1, 1, 1, 5, 8), (3, 10), (1, 0, 0, 1, 10), (1, 0, 1, 1, 10), (0, 1, 1, 7, 3, 4, 6),
        (0, 1, 0, 1, 4, 7, 10), (0, 1, 1, 1, 4, 7, 10), (0, 1, 0, 7, 3, 4, 6), (2, 0), (0, 0, 1, 10, 3, 4, 2),
        (0, 0, 0, 10, 3, 4, 2), (0, 1, 1, 10, 4, 2, 3), (0, 1, 0, 10, 4, 2, 3), (2, 1), (2, 2), (2, 3), (2, 4),
    ),
    (
        (0, 0, 1, 6, 5, 2, 7), (0, 0, 0, 6, 5, 2, 7), (0, 0, 0, 3, 7), (0, 0, 0, 4, 7, 5), (0, 0, 1, 4, 7, 5),
        (0, 0, 1, 3, 7), (0, 1, 1, 6, 5, 2, 7), (0, 1, 0, 6, 5, 2, 7), (3, 9), (1, 0, 0, 4, 9), (1, 0, 1, 4, 9),
        (3, 8), (1, 0, 0, 3, 8), (1, 0, 1, 3, 8), (0, 0, 1, 10, 7, 5), (0, 0, 1, 11, 5, 4, 8), (0, 0, 0, 10, 7, 5),
        (0, 1, 0, 3, 7, 8), (0, 1, 0, 4, 5, 7, 9), (0, 1, 1, 4, 5, 7, 9), (0, 0, 0, 11, 5, 4, 8), (0, 1, 1, 3, 7, 8),
        (0, 1, 1, 10, 7, 5), (0, 1, 0, 10, 7, 5), (2, 0), (0, 0, 1, 8, 5, 4, 7), (0, 1, 1, 11, 8, 4, 5),
        (0, 0, 0, 8, 5, 4, 7), (0, 1, 1, 8, 4, 5, 7), (0, 0, 1, 13, 9, 8, 7), (0, 1, 0, 8, 4, 5, 7), (2, 1),
        (0, 1, 0, 11, 8, 4, 5), (0, 0, 0, 13, 9, 8, 7), (0, 1, 1, 13, 9, 8, 7), (2, 2), (0, 1, 0, 13, 9, 8, 7),
        (2, 3), (2, 4),
    ),
    (
        (0, 0, 1, 7, 5, 2), (0, 0, 0, 7, 5, 2), (0, 0, 1, 6, 3), (0, 0, 0, 6, 3), (3, 9), (1, 0, 1, 6, 9),
        (1, 0, 0, 6, 9), (0, 1, 1, 7, 5, 2), (3, 8), (1, 0, 1, 7, 8), (1, 0, 0, 7, 8), (1, 0, 1, 6, 8),
        (1, 0, 0, 6, 8), (1, 1, 1, 7, 8), (3, 10), (1, 0, 1, 7, 10), (1, 0, 0, 7, 10), (1, 1, 1, 7, 10),
        (0, 1, 0, 7, 8, 5, 10, 2), (0, 1, 1, 6, 8, 3, 9), (0, 1, 0, 6, 8, 3, 9), (2, 0), (2, 1),
        (0, 0, 1, 15, 9, 10, 8, 6), (0, 0, 0, 15, 9, 10, 8, 6), (0, 1, 1, 15, 9, 6, 10, 8), (2, 2),
        (0, 1, 0, 15, 9, 6, 10, 8), (2, 3), (2, 4),
    ),
    (
        (0, 0, 1, 8, 9, 12, 10, 3, 11), (0, 0, 0, 8, 9, 12, 10, 3, 11), (0, 1, 1, 8, 9, 11, 3, 12, 10),
        (0, 1, 0, 8, 9, 11, 3, 12, 10), (0, 0, 0, 3, 10, 13, 5, 9), (0, 0, 1, 3, 10, 13, 5, 9), (2, 0),
        (0, 0, 0, 5, 11, 4, 9, 7), (0, 0, 1, 5, 11, 4, 9, 7), (0, 1, 0, 5, 7, 11, 9, 4), (0, 1, 1, 5, 7, 11, 9, 4),
        (0, 1, 0, 3, 13, 9, 5, 10), (0, 1, 1, 3, 13, 9, 5, 10), (2, 1), (0, 0, 0, 0, 6, 7, 9), (0, 0, 1, 0, 6, 7, 9),
        (0, 1, 0, 0, 9, 7, 6), (0, 1, 1, 0, 9, 7, 6), (2, 2), (2, 3), (2, 4),
    ),
    (
        (0, 0, 1, 9, 7, 8, 10, 4, 12), (0, 0, 0, 9, 7, 8, 10, 4, 12), (0, 1, 1, 9, 4, 7, 8, 12, 10),
        (0, 1, 0, 9, 4, 7, 8, 12, 10), (0, 0, 1, 12, 7, 6, 5, 8), (0, 0, 0, 12, 7, 6, 5, 8), (0, 0, 0, 4, 8, 10, 12),
        (0, 0, 1, 4, 8, 10, 12), (2, 0), (0, 1, 1, 12, 5, 8, 6, 7), (0, 1, 0, 12, 5, 8, 6, 7),
        (0, 1, 0, 4, 12, 10, 8), (2, 1), (0, 1, 1, 4, 12, 10, 8), (0, 0, 0, 2, 11, 10, 8, 12),
        (0, 0, 1, 2, 11, 10, 8, 12), (0, 1, 0, 2, 11, 8, 12, 10), (0, 1, 1, 2, 11, 8, 12, 10), (2, 2), (2, 3), (2, 4),
    ),
    (
        (0, 0, 1, 10, 12, 9, 6, 0, 11, 8), (0, 0, 0, 10, 12, 9, 6, 0, 11, 8), (0, 1, 1, 10, 6, 11, 8, 0, 12, 9),
        (0, 1, 0, 10, 6, 11, 8, 0, 12, 9), (0, 0, 1, 7, 13, 9), (0, 0, 1, 14, 9, 12, 11, 5), (0, 0, 0, 7, 13, 9),
        (0, 1, 1, 7, 13, 9), (2, 0), (0, 1, 0, 7, 13, 9), (0, 0, 0, 14, 9, 12, 11, 5), (0, 1, 1, 14, 9, 12, 11, 5),
        (0, 1, 0, 14, 9, 12, 11, 5), (0, 0, 0, 1, 12, 8, 9, 11), (2, 1), (0, 0, 1, 1, 12, 8, 9, 11),
        (0, 1, 0, 1, 9, 12, 8, 11), (0, 1, 1, 1, 9, 12, 8, 11), (2, 2), (2, 3), (2, 4),
    ),
    (
        (0, 0, 1, 11, 6, 9, 0, 10, 12, 7), (0, 0, 0, 11, 6, 9, 0, 10, 12, 7), (0, 1, 1, 11, 6, 12, 9, 10, 7, 0),
        (0, 1, 0, 11, 6, 12, 9, 10, 7, 0), (2, 0), (0, 0, 0, 5, 13, 12, 10), (0, 0, 1, 5, 13, 12, 10),
        (0, 1, 0, 5, 13, 10, 12), (2, 1), (0, 1, 1, 5, 13, 10, 12), (2, 2), (2, 3), (2, 4),
    ),
    (
        (0, 0, 1, 12, 10, 0, 11, 9), (0, 0, 0, 12, 10, 0, 11, 9), (0, 1, 1, 12, 10, 9, 0, 11), (0, 0, 1, 9, 11, 15),
        (0, 1, 0, 12, 10, 9, 0, 11), (0, 0, 0, 9, 11, 15), (0, 0, 1, 8, 14, 0, 13), (0, 0, 0, 8, 14, 0, 13),
        (0, 1, 1, 9, 11, 15), (2, 0), (0, 1, 0, 9, 11, 15), (0, 1, 1, 8, 0, 14, 13), (0, 0, 0, 0, 14, 10, 15, 11),
        (0, 1, 0, 8, 0, 14, 13), (0, 0, 1, 0, 14, 10, 15, 11), (0, 1, 0, 0, 11, 15, 10, 14),
        (0, 1, 1, 0, 11, 15, 10, 14), (0, 0, 0, 4, 13, 11, 15, 14), (0, 0, 1, 4, 13, 11, 15, 14), (2, 1),
        (0, 1, 0, 4, 11, 14, 13, 15), (0, 1, 1, 4, 11, 14, 13, 15), (2, 2), (2, 3), (2, 4),
    ),
    (
        (0, 0, 1, 13, 11, 12, 0, 14, 10), (0, 0, 0, 13, 11, 12, 0, 14, 10), (0, 1, 1, 13, 0, 12, 11, 14, 10),
        (0, 1, 0, 13, 0, 12, 11, 14, 10), (0, 0, 0, 0, 12, 8), (0, 0, 1, 0, 12, 8), (0, 1, 0, 0, 12, 8),
        (0, 1, 1, 0, 12, 8), (0, 0, 1, 7, 12, 14, 15, 11), (2, 0), (0, 0, 0, 7, 12, 14, 15, 11),
        (0, 1, 1, 7, 11, 12, 15, 14), (0, 0, 1, 6, 12), (0, 0, 0, 3, 11, 14, 12, 15), (0, 1, 0, 7, 11, 12, 15, 14),
        (2, 1), (0, 0, 0, 6, 12), (0, 0, 1, 3, 11, 14, 12, 15), (0, 1, 1, 6, 12), (0, 1, 0, 3, 15, 14, 11, 12),
        (0, 1, 0, 6, 12), (0, 1, 1, 3, 15, 14, 11, 12), (2, 2), (2, 3), (2, 4),
    ),
    (
        (0, 0, 1, 14, 8, 10, 15, 13, 2), (0, 0, 0, 14, 8, 10, 15, 13, 2), (0, 1, 1, 14, 10, 8, 15, 2, 13),
        (0, 1, 0, 14, 10, 8, 15, 2, 13), (0, 0, 0, 2, 9, 13, 15), (0, 0, 1, 2, 9, 13, 15), (0, 0, 0, 1, 15),
        (0, 0, 1, 1, 15), (0, 1, 0, 2, 15, 9, 13), (0, 1, 1, 2, 15, 9, 13), (2, 0), (0, 0, 1, 6, 13, 10, 15, 11),
        (0, 1, 0, 1, 15), (0, 1, 1, 1, 15), (0, 0, 0, 6, 13, 10, 15, 11), (0, 1, 1, 6, 10, 13, 11, 15),
        (0, 1, 0, 6, 10, 13, 11, 15), (2, 1), (2, 2), (2, 3), (2, 4),
    ),
    (
        (0, 0, 1, 15, 12, 11, 14, 2, 13), (0, 0, 0, 15, 12, 11, 14, 2, 13), (0, 1, 1, 15, 2, 14, 11, 13, 12),
        (0, 1, 0, 15, 2, 14, 11, 13, 12), (0, 0, 1, 9, 14, 0, 13, 1), (0, 0, 0, 9, 14, 0, 13, 1),
        (0, 0, 1, 11, 14, 13), (0, 0, 1, 10, 14, 13), (0, 0, 0, 11, 14, 13), (0, 0, 0, 10, 14, 13),
        (0, 1, 1, 9, 1, 0, 14, 13), (0, 1, 1, 11, 13, 14), (0, 1, 0, 9, 1, 0, 14, 13), (2, 0), (0, 1, 1, 10, 13, 14),
        (0, 1, 0, 11, 13, 14), (2, 1), (0, 1, 0, 10, 13, 14), (2, 2), (2, 3), (2, 4),
    ),
)

SLOT = [{source: i for i, source in enumerate(order)} for order in ORDER]
RELAYS = [[tuple(step[1:4]) for step in route if step[0] == 0 and step[3] != z] for z, route in enumerate(ROUTES)]
BOUNDS = (0, 4, 8, 12, 14, 16)
PART = [sum(slot >= bound for bound in BOUNDS[1:]) for slot in range(16)]
RSEMS = 10 + max(map(len, RELAYS))


def leaves(z, p):
    return [
        (wave, core, source)
        for source in ORDER[z][BOUNDS[p] : BOUNDS[p + 1]]
        for wave in range(2)
        for core in range(2)
        if source != z and (wave, core, source) not in RELAYS[z]
    ]


RING = (
    ("q_begin",), ("q_own",),
    ("q_relay", -1, 0, 0), ("q_relay", 1, 0, 0), ("q_relay", -1, 0, 1), ("q_relay", 1, 0, 1),
    ("k_own",),
    ("q_relay", -2, 0, 0), ("q_relay", 2, 0, 0), ("q_relay", -1, 1, 0), ("q_relay", 1, 1, 0),
    ("q_relay", -2, 0, 1), ("q_relay", 2, 0, 1), ("q_relay", -1, 1, 1), ("q_relay", 1, 1, 1),
    ("k_relay", -1), ("k_relay", 1),
    ("q_relay", -3, 0, 0), ("q_relay", 3, 0, 0), ("q_relay", -2, 1, 0), ("q_relay", 2, 1, 0),
    ("q_relay", -3, 0, 1), ("q_relay", 3, 0, 1), ("q_relay", -2, 1, 1), ("q_relay", 2, 1, 1),
    ("k_relay", -2), ("k_relay", 2),
    ("q_relay", -3, 1, 0), ("q_relay", 3, 1, 0), ("q_relay", -3, 1, 1), ("q_relay", 3, 1, 1),
    ("k_relay", -3), ("k_relay", 3),
)

LATE_RING = (
    ("q_begin",), ("q_own_first",),
    ("q_relay", -1, 1, 0), ("q_relay", 1, 1, 0), ("q_relay", -1, 1, 1), ("q_relay", 1, 1, 1),
    ("q_relay", -2, 1, 0), ("q_relay", 2, 1, 0), ("q_relay", -2, 1, 1), ("q_relay", 2, 1, 1),
    ("q_relay", -3, 1, 0), ("q_relay", 3, 1, 0), ("q_relay", -3, 1, 1), ("q_relay", 3, 1, 1),
    ("q_own_last",), ("k_own",),
    ("q_relay", -1, 0, 0), ("q_relay", 1, 0, 0), ("q_relay", -1, 0, 1), ("q_relay", 1, 0, 1),
    ("k_relay", -1), ("k_relay", 1),
    ("q_relay", -2, 0, 0), ("q_relay", 2, 0, 0), ("q_relay", -2, 0, 1), ("q_relay", 2, 0, 1),
    ("k_relay", -2), ("k_relay", 2),
    ("q_relay", -3, 0, 0), ("q_relay", 3, 0, 0), ("q_relay", -3, 0, 1), ("q_relay", 3, 0, 1),
    ("k_relay", -3), ("k_relay", 3),
)

PLAN_Q = (
    ("ring",),
    ("attend", 2), ("attend", 1), ("attend", 3),
    ("w_passed", 0), ("piece", 0, 1), ("w_passed", 1), ("piece", 1, 1),
    ("q_last",), ("k_last",), ("attend", 0),
    ("piece", 0, 0), ("piece", 1, 0),
    ("reduced", 0, 2), ("reduced", 0, 1), ("reduced", 0, 3), ("reduced", 1, 2), ("reduced", 1, 1), ("reduced", 1, 3),
    ("reduced", 0, 0), ("reduced", 1, 0),
)

PLAN_W = (
    ("w_begin",), ("w_route", 0),
    ("a_got", 2), ("a_got", 1), ("a_got", 3), ("a_got", 0),
    ("w_piece", 2, 0, 4), ("w_route", 1), ("w_piece", 3, 0, 2), ("w_route", 2), ("w_piece", 3, 2, 2),
    ("reduced", 2, 0), ("reduced", 2, 1), ("reduced", 2, 3), ("reduced", 2, 2),
    ("reduced", 3, 0), ("reduced", 3, 1), ("reduced", 3, 3), ("reduced", 3, 2),
)


def by_place(z, do, low=0, high=16):
    if high - low == 1:
        do(low)
        return
    middle = (low + high) // 2
    pl.when(z < middle)(lambda: by_place(z, do, low, middle))
    pl.when(z >= middle)(lambda: by_place(z, do, middle, high))


def kernel(
    q, k, v, w, sums,
    qall, kvl, kvr, wv, wt, wcross, wall, bias, att, psend, xr, ssend, rbuf, size,
    lsem, ssem, rsem, wpsem, atsem, xsem, asem, go, late,
):
    yl, z, x, yh, c = (lax.axis_index(a) for a in ("yl", "z", "x", "yh", "c"))
    y = yh * 4 + yl

    def dev(dy=0, dz=0, dx=0, to_z=None, role=None):
        yt = lax.rem(y + (dy + 8), 8)
        zt = lax.rem(z + (dz + 16), 16) if to_z is None else to_z
        xt = lax.rem(x + dx, 4)
        core = role if to_z else jnp.where(xt + yt + zt == 0, 1 - role, role)
        return (lax.rem(yt, 4), zt, xt, lax.div(yt, 4), core)

    origin = x + y + z == 0
    for_q = jnp.where(origin, 1 - QC, QC) == c
    one_more = jnp.where(origin, 0, 1)

    def remote(src, dst, send_sem, recv_sem, to):
        return pltpu.make_async_remote_copy(
            src_ref=src, dst_ref=dst, send_sem=send_sem, recv_sem=recv_sem, device_id=to, device_id_type=MESH
        )

    sent = [0]

    def send(src, dst, recv_sem, to):
        remote(src, dst, ssem.at[0], recv_sem, to).start()
        sent[0] += math.prod(src.shape) * 2

    def received(dst, recv_sem):
        remote(dst, dst, ssem.at[0], recv_sem, (yl, z, x, yh, 1 - c)).wait_recv()

    def sized(bytes_):
        assert bytes_ % 8192 == 0 and bytes_ // 8192 <= size.shape[0]
        return size.at[pl.ds(0, bytes_ // 8192)]

    def half_of(r):
        return lax.div(lax.rem(y + (r + 8), 8), 4)

    w_load = pltpu.make_async_copy(w, wv, lsem.at[0])
    q_load = pltpu.make_async_copy(q, qall.at[0, yh, c], lsem.at[1])
    kv_load = [pltpu.make_async_copy(k, kvl.at[0], lsem.at[2]), pltpu.make_async_copy(v, kvl.at[1], lsem.at[2])]
    barrier = pltpu.get_barrier_semaphore()
    around_q = [dict(dy=1), dict(dy=-1), dict(dx=1), dict(dx=2), dict(dx=3)]

    w_load.start()
    for copy in kv_load:
        copy.start()
    q_load.start()

    @pl.when(for_q)
    def _():
        for peer in around_q:
            pl.semaphore_signal(barrier, inc=1, device_id=dev(role=QC, **peer), device_id_type=MESH)

    @pl.when(~for_q)
    def _():
        pl.semaphore_signal(barrier, inc=1, device_id=dev(dy=4, role=WC), device_id_type=MESH)

        @pl.when(~origin)
        def _():
            pl.semaphore_signal(barrier, inc=1, device_id=dev(role=QC), device_id_type=MESH)

        def greet(place):
            for other in range(16):
                if place in FIRST[other]:
                    pl.semaphore_signal(barrier, inc=1, device_id=dev(to_z=other, role=WC), device_id_type=MESH)

        by_place(z, greet)

    w_load.wait()
    wt[...] = wv[...].astype(F32).T.astype(BF16).reshape(2, 64, 256)
    for copy in kv_load:
        copy.wait()

    def lanes_of(half, core):
        return pl.ds(pl.multiple_of((half * 2 + core) * 256, 256), 256)

    def head_of(i):
        return pl.ds(pl.multiple_of(i * 128, 128), 128)

    def unit(slot, wave, core):
        return wall.at[slot, :, lanes_of(1 - yh if wave else yh, core)]

    def w_sem(place, wave, core, source):
        if (wave, core, source) in RELAYS[place]:
            return rsem.at[10 + RELAYS[place].index((wave, core, source))]
        return rsem.at[5 + PART[SLOT[place][source]]]

    def w_sends(place, wave, core, source, targets):
        for t in targets:
            here, there = SLOT[place][source], SLOT[t][source]
            to = dev(to_z=t, role=WC)
            send(unit(here, wave, core), unit(there, wave, core), w_sem(t, wave, core, source), to)

    def w_cross(core):
        send(wcross.at[core], wall.at[0, :, lanes_of(yh, core)], rsem.at[2 + core], dev(dy=4, role=WC))

    waited = []

    def w_step(place, kind, *step):
        if kind == 3:
            pl.semaphore_wait(late.at[step[0] - 8], 1)
            return
        if kind == 2:
            p = step[0]
            if leaves(place, p):
                received(sized(len(leaves(place, p)) * 32768), rsem.at[5 + p])
            if p < 2:
                rows = pl.ds(4 * p, 4)
                send(wall.at[rows], wall.at[rows], wpsem.at[p], dev(role=QC))
            return
        wave, core, source, *targets = step
        if kind == 0:
            if source != place:
                received(unit(SLOT[place][source], wave, core), w_sem(place, wave, core, source))
            elif wave:
                received(unit(0, 1, core), rsem.at[2 + core])
            else:
                if (core == QC or place == 0) and place not in waited:
                    received(sized(65536), rsem.at[4])
                    waited.append(place)
                w_cross(core)
        w_sends(place, wave, core, source, targets)

    def w_route(part):
        totals = []

        def go_on(place):
            route = ROUTES[place]
            first = 1 + max(i for i, step in enumerate(route) if step[0] != 2 or step[1] == 2)
            cuts = (0, first, max(first, 1 + route.index((2, 3))), len(route))
            start = sent[0]
            for step in route[cuts[part] : cuts[part + 1]]:
                with jax.named_scope("_".join(map(str, ("at", place, *step)))):
                    w_step(place, *step)
            totals.append(sent[0] - start)
            sent[0] = start

        by_place(z, go_on)
        w_totals.append(totals)

    w_totals = []

    def w_passed(p):
        received(wall.at[pl.ds(4 * p, 4)], wpsem.at[p])

    def q_part(r, s, u):
        return qall.at[r % 4, half_of(r), s, pl.ds(128 * u, 128)]

    def q_sem(t, s, u):
        return rsem.at[0 if t == 4 else 8 + 4 * (t if t < 4 else t - 1) + 2 * s + u]

    def q_send(r, s, u, hop):
        t = (r - hop) % 8
        rows = pl.ds(128 * u, 128)
        dst = qall.at[t % 4, half_of(r), s, rows]
        send(q_part(r, s, u), dst, q_sem(t, s, u), dev(dy=hop, role=QC))

    def q_relay(r, s, u):
        received(q_part(r, s, u), q_sem(r % 8, s, u))
        if abs(r) < 3 or s == (0 if r < 0 else 1):
            q_send(r, s, u, 1 if r < 0 else -1)

    def q_last():
        received(qall.at[0, half_of(4)], rsem.at[0])

    def k_send(r, hop):
        t = (r - hop) % 8
        some = pl.ds(0 if hop > 0 else 2, 2) if t == 4 else pl.ds(0, 4)
        src, dst = kvr.at[r % 4, half_of(r), some], kvr.at[t % 4, half_of(r), some]
        send(src, dst, rsem.at[t if t else 8], dev(dy=hop, role=QC))

    def k_relay(r):
        received(kvr.at[r % 4, half_of(r)], rsem.at[r % 8])
        k_send(r, 1 if r < 0 else -1)

    def k_last():
        received(kvr.at[0, half_of(4)], rsem.at[4])

    def k_spread():
        for d in (2, 1, 3):
            head = head_of(lax.rem(x + d, 4))
            send(kvl.at[:, :, head], kvr.at[0, yh, x, :, c], rsem.at[8], dev(dx=d, role=QC))

    def k_own():
        received(sized(7 * 8192), rsem.at[8])
        k_send(0, 1)
        k_send(0, -1)

    def ring():
        before = sent[0]
        for late, plan in ((False, RING), (True, LATE_RING)):
            sent[0] = before

            def go_round(plan=plan):
                for step in plan:
                    do(*step)

            pl.when((x + z == 0) if late else (x + z > 0))(go_round)

    def q_own_first():
        once(~origin, None, q_own)

    def q_own_last():
        before = sent[0]
        pl.when(origin)(q_own)
        sent[0] = before

    def w_hand():
        send(wt.at[yh], unit(0, 0, c), rsem.at[4], dev(role=WC))
        send(wt.at[1 - yh], wcross.at[c], rsem.at[4], dev(role=WC))

    def once(first, second, do):
        before = sent[0]
        pl.when(second if first is None else first)(do)
        if first is None:
            sent[0] = before

    def q_own():
        received(qall.at[0, yh, 1 - c], rsem.at[9])
        for u in range(2):
            for hop in (1, -1):
                q_send(0, 1 - c, u, hop)
        before = sent[0]
        pl.when(origin)(w_hand)
        sent[0] = before

    def q_begin():
        pl.semaphore_wait(barrier, len(around_q) + one_more)

        def meet():
            pl.semaphore_signal(go, inc=1, device_id=dev(role=WC), device_id_type=MESH)
            w_hand()

        once(~origin, None, meet)

        @pl.when(origin)
        def _():
            pl.semaphore_signal(barrier, inc=1, device_id=dev(role=WC), device_id_type=MESH)

        k_spread()
        kvr[0, yh, x, :, c] = kvl[:, :, head_of(x)]
        q_load.wait()
        for u in range(2):
            for hop in (1, -1):
                q_send(0, c, u, hop)
        row = lax.broadcasted_iota(jnp.int32, (128, 128), 0)
        col = lax.broadcasted_iota(jnp.int32, (128, 128), 1)
        bias[...] = jnp.where((lax.div(row, 32) == lax.div(col, 32)) & (col <= row), 0.0, -1e30)

    def w_begin():
        wall[0, :, lanes_of(yh, c)] = wt[yh]
        wcross[c] = wt[1 - yh]
        q_load.wait()

        def give():
            send(qall.at[0, yh, c], qall.at[0, yh, c], rsem.at[9], dev(role=QC))
            k_spread()
            send(kvl.at[:, :, head_of(x)], kvr.at[0, yh, x, :, c], rsem.at[8], dev(role=QC))

        def meet():
            pl.semaphore_wait(go, 1)
            give()

        once(~origin, None, meet)

        def greeted(place):
            pl.semaphore_wait(barrier, 2 + len(FIRST[place]) - one_more)
            for other in range(8):
                if (3, place) in ROUTES[other]:
                    to = dev(to_z=other, role=WC)
                    pl.semaphore_signal(late.at[place - 8], inc=1, device_id=to, device_id_type=MESH)

        by_place(z, greeted)
        once(None, origin, give)

    def attend(gs):
        for t in range(2):
            pair = kvr[gs, t]
            keys, values = pair[:, 0].reshape(128, 128), pair[:, 1].reshape(128, 128)
            values = jnp.concatenate([values, jnp.ones((128, 128), BF16)], axis=1)
            for h in range(2):
                queries = jnp.concatenate(
                    [
                        qall[gs, h, s, :, j * 128 : j * 128 + 128].reshape(4, 2, 32, 128)[:, t].reshape(128, 128)
                        for s in range(2)
                        for j in range(2)
                    ],
                    axis=0,
                )
                scores = lax.dot_general(queries, keys, NT, preferred_element_type=F32)
                scores = scores * (1.0 / math.sqrt(128.0)) + jnp.concatenate([bias[...]] * 4, axis=0)
                powers = jnp.exp(scores - jnp.max(scores, axis=-1, keepdims=True)).astype(BF16)
                total = jnp.dot(powers, values, preferred_element_type=F32)
                heads = (total[:, :128] / total[:, 128:]).astype(BF16)
                for i in range(4):
                    att[gs, t, :, h * 512 + i * 128 : h * 512 + i * 128 + 128] = heads[i * 128 : i * 128 + 128]
        send(att.at[gs], att.at[gs], atsem.at[gs], dev(role=WC))

    def a_got(gs):
        received(att.at[gs], atsem.at[gs])

    def spread(p, gs, lanes):
        for d in (2, 1, 3):
            src = psend.at[p % 2, gs, :, lax.rem(x + d, 4), :, lanes]
            dst = xr.at[p % 2, gs, d - 1, :, :, lanes]
            send(src, dst, xsem.at[p % 2, gs], dev(dx=d, role=QC if p < 2 else WC))

    def piece(p, most):
        groups = slice(1, 4) if most else slice(0, 1)
        n = 3 if most else 1
        rows = wall[4 * p : 4 * p + 4].reshape(256, 1024)
        total = lax.dot_general(att[groups].reshape(n * 256, 1024), rows, NT, preferred_element_type=F32)
        psend[p, groups] = total.astype(BF16).reshape(n, 2, 4, 32, 256)
        for gs in (2, 1, 3) if most else (0,):
            spread(p, gs, pl.ds(0, 256))

    def w_piece(p, slot, n):
        slots = slice(4 * p + slot, 4 * p + slot + n)
        rows = wall[slots].reshape(64 * n, 1024)
        total = lax.dot_general(att[...].reshape(1024, 1024), rows, NT, preferred_element_type=F32)
        lanes = slice(64 * slot, 64 * (slot + n))
        psend[p - 2, :, :, :, :, lanes] = total.astype(BF16).reshape(4, 2, 4, 32, 64 * n)
        for gs in (0, 1, 3, 2):
            spread(p, gs, pl.ds(64 * slot, 64 * n))

    def reduced(p, gs):
        received(xr.at[p % 2, gs], xsem.at[p % 2, gs])
        total = psend[p % 2, gs, :, x].astype(F32)
        for d in range(3):
            total = total + xr[p % 2, gs, d].astype(F32)
        ssend[p % 2, gs] = total.astype(BF16).reshape(2, 2, 16, 256)
        for other in (1, 0):
            half = 1 - yh if other else yh
            there = half * 4 + lax.rem(yl + gs, 4)
            place = lax.rem(y + 8 - there, 8)
            for core in (1 - c, c):
                home = (lax.rem(yl + gs, 4), z, x, half, core)
                if gs or other:
                    send(ssend.at[p % 2, gs, half, core], rbuf.at[p, place], asem.at[p], home)
                elif core is c:
                    rbuf[p, 0] = ssend[p % 2, 0, yh, c]
                else:
                    send(ssend.at[p % 2, 0, yh, core], rbuf.at[p, 0], asem.at[4 + p % 2], home)

    steps = dict(
        q_begin=q_begin, w_begin=w_begin, q_own=q_own, q_relay=q_relay, q_last=q_last, k_own=k_own, k_relay=k_relay,
        k_last=k_last, attend=attend, w_route=w_route, w_passed=w_passed, a_got=a_got, piece=piece, w_piece=w_piece, reduced=reduced,
        ring=ring, q_own_first=q_own_first, q_own_last=q_own_last,
    )

    def do(name, *numbers):
        with jax.named_scope("_".join(map(str, (name, *numbers)))):
            steps[name](*numbers)

    def follow(plan):
        sent[0] = 0
        for step in plan:
            do(*step)

    def drain(bytes_):
        stand_in = sized(bytes_)
        remote(stand_in, stand_in, ssem.at[0], ssem.at[0], (yl, z, x, yh, 1 - c)).wait_send()

    def arrive(mine):
        with jax.named_scope("arrive"):
            outs = []
            for p in range(PIECES):
                received(rbuf.at[p, pl.ds(1, 7)], asem.at[p])
                if p // 2 != mine:
                    received(rbuf.at[p, 0], asem.at[4 + p % 2])
                outs.append(pltpu.make_async_copy(rbuf.at[p], sums.at[p], lsem.at[3 + p]))
                outs[-1].start()
            if mine:
                by_place(z, lambda place: drain(sent[0] + sum(totals[place] for totals in w_totals)))
            else:
                drain(sent[0])
            for copy in outs:
                copy.wait()

    @pl.when(for_q)
    def _():
        follow(PLAN_Q)
        arrive(0)

    @pl.when(~for_q)
    def _():
        follow(PLAN_W)
        arrive(1)


def last_kernel(sums, res, gain, hid, nrm, rbuf, resv, gv, u, hidv, nrmv, sem):
    yl, z, yh = (lax.axis_index(a) for a in ("yl", "z", "yh"))
    y = yh * 4 + yl
    loads = [
        pltpu.make_async_copy(res, resv, sem.at[0]),
        pltpu.make_async_copy(gain, gv, sem.at[0]),
    ]
    loads += [pltpu.make_async_copy(sums.at[p], rbuf.at[p], sem.at[1 + p]) for p in range(PIECES)]
    for copy in loads:
        copy.start()

    def source_of(slot):
        low, high = (
            sum(ORDER[8 * part + i][slot] << (4 * i) for i in range(8)) for part in range(2)
        )
        low, high = (n - (1 << 32) if n >> 31 else n for n in (low, high))
        word = jnp.where(z < 8, jnp.int32(low), jnp.int32(high))
        return lax.shift_right_logical(word, 4 * lax.rem(z, 8)) & 15

    for copy in loads[:2]:
        copy.wait()
    squares = jnp.zeros((16, 128), F32)
    low = lax.broadcasted_iota(jnp.int32, (16, 128), 1) < 64
    for p in range(PIECES):
        sources = [source_of(4 * p + i) for i in range(4)]
        loads[2 + p].wait()
        for r in range(4):
            here = lax.div(lax.rem(y + r, 8), 4)
            first, second = r + 4 * here, r + 4 - 4 * here
            for t in range(2):
                lanes = slice(t * 128, t * 128 + 128)
                a = rbuf[p, first, :, lanes].astype(F32)
                b = rbuf[p, second, :, lanes].astype(F32)
                pair = (jnp.where(low, a, pltpu.roll(b, 64, 1)), jnp.where(low, pltpu.roll(a, 64, 1), b))
                for i in range(2):
                    block = lax.rem(yl + r, 4) * 16 + sources[2 * t + i]
                    at = pl.ds(pl.multiple_of(block * 128, 128), 128)
                    updated = resv[:, at].astype(F32) + pair[i]
                    u[:, at] = updated
                    hidv[:, at] = updated.astype(BF16)
                    squares = squares + updated * updated
    stores = [pltpu.make_async_copy(hidv, hid, sem.at[5])]
    stores[0].start()
    scale = lax.rsqrt(jnp.sum(squares, axis=-1, keepdims=True) * (1.0 / 8192.0) + 1e-05)
    for part in range(2):
        for block in range(32 * part, 32 * part + 32):
            lanes = slice(block * 128, block * 128 + 128)
            nrmv[:, lanes] = (u[:, lanes] * scale * gv[block : block + 1, :]).astype(BF16)
        lanes = pl.ds(4096 * part, 4096)
        stores.append(pltpu.make_async_copy(nrmv.at[:, lanes], nrm.at[:, lanes], sem.at[6 + part]))
        stores[-1].start()
    for copy in stores:
        copy.wait()


def local(queries, keys, values, out_weight, residual, norm_gain):
    in_hbm = pl.BlockSpec(memory_space=pltpu.HBM)
    vmem = pltpu.VMEM
    dma = pltpu.SemaphoreType.DMA
    sums = pl.pallas_call(
        kernel,
        out_shape=jax.ShapeDtypeStruct((PIECES, 8, 16, 256), BF16),
        in_specs=[in_hbm] * 4,
        out_specs=in_hbm,
        scratch_shapes=[
            vmem((4, 2, 2, 256, 256), BF16),
            vmem((2, 16, 512), BF16),
            vmem((4, 2, 4, 2, 2, 16, 128), BF16),
            vmem((256, 128), BF16),
            vmem((2, 64, 256), BF16),
            vmem((2, 64, 256), BF16),
            vmem((16, 64, 1024), BF16),
            vmem((128, 128), F32),
            vmem((4, 2, 128, 1024), BF16),
            vmem((2, 4, 2, 4, 32, 256), BF16),
            vmem((2, 4, 3, 2, 32, 256), BF16),
            vmem((2, 4, 2, 2, 16, 256), BF16),
            vmem((PIECES, 8, 16, 256), BF16),
            vmem((1200, 16, 256), BF16),
            dma((3 + PIECES,)),
            dma((1,)),
            dma((max(40, RSEMS),)),
            dma((2,)),
            dma((4,)),
            dma((2, 4)),
            dma((6,)),
            pltpu.SemaphoreType.REGULAR,
            pltpu.SemaphoreType.REGULAR((8,)),
        ],
        compiler_params=pltpu.CompilerParams(collective_id=0, has_side_effects=True, vmem_limit_bytes=VMEM),
        name="layer",
    )(queries, keys, values, out_weight)
    return pl.pallas_call(
        last_kernel,
        out_shape=(jax.ShapeDtypeStruct((16, 8192), BF16),) * 2,
        in_specs=[in_hbm] * 3,
        out_specs=(in_hbm,) * 2,
        scratch_shapes=[
            vmem((PIECES, 8, 16, 256), BF16),
            vmem((16, 8192), BF16),
            vmem((64, 128), F32),
            vmem((16, 8192), F32),
            vmem((16, 8192), BF16),
            vmem((16, 8192), BF16),
            dma((8,)),
        ],
        compiler_params=pltpu.CompilerParams(vmem_limit_bytes=VMEM),
        name="final",
    )(sums, residual, norm_gain.reshape(64, 128))


def solution(mesh):
    finer = Mesh(mesh.devices.reshape(4, 16, 4, 2, 2), ("yl", "z", "x", "yh", "c"))
    rows, heads = ("yl", "z"), ("x", "yh", "c")
    both = rows + heads
    in_specs = (P(rows, heads), P(both, None), P(both, None), P(heads, rows), P(both, None), P())
    out_specs = (P(both, None), P(both, None))
    return jax.shard_map(local, mesh=finer, in_specs=in_specs, out_specs=out_specs, check_vma=False)
```

```python
import math

import jax
import jax.numpy as jnp
from jax import lax
from jax.experimental import pallas as pl
from jax.experimental.pallas import tpu as pltpu
from jax.sharding import Mesh
from jax.sharding import PartitionSpec as P

MESH = pl.DeviceIdType.MESH
F32, BF16 = jnp.float32, jnp.bfloat16
NT = (((1,), (1,)), ((), ()))

QC, WC = 0, 1
VMEM = 60 * 1024 * 1024
PIECES = 4

ORDER = (
    (0, 2, 3, 1, 4, 13, 5, 12, 6, 11, 7, 15, 10, 14, 8, 9),
    (1, 0, 4, 2, 3, 5, 6, 7, 13, 15, 12, 14, 11, 10, 9, 8),
    (2, 1, 3, 5, 0, 6, 4, 7, 15, 14, 13, 8, 9, 11, 10, 12),
    (3, 1, 0, 2, 5, 7, 4, 6, 8, 15, 9, 12, 10, 14, 11, 13),
    (4, 3, 2, 7, 0, 1, 6, 9, 15, 10, 14, 13, 11, 12, 5, 8),
    (5, 6, 7, 1, 2, 4, 0, 10, 9, 11, 15, 3, 13, 8, 12, 14),
    (6, 4, 3, 10, 7, 2, 1, 11, 9, 8, 12, 14, 13, 15, 5, 0),
    (7, 6, 9, 4, 3, 1, 2, 10, 5, 11, 12, 15, 8, 14, 0, 13),
    (8, 7, 9, 6, 10, 5, 3, 12, 11, 14, 4, 0, 2, 15, 13, 1),
    (9, 10, 8, 11, 6, 12, 7, 4, 14, 2, 5, 3, 15, 0, 1, 13),
    (10, 9, 11, 8, 7, 12, 13, 14, 4, 0, 1, 3, 2, 5, 6, 15),
    (11, 10, 12, 8, 13, 9, 15, 14, 0, 7, 5, 4, 2, 6, 1, 3),
    (12, 11, 13, 10, 9, 8, 15, 0, 14, 4, 7, 6, 5, 2, 1, 3),
    (13, 14, 15, 8, 0, 7, 2, 1, 6, 9, 4, 11, 10, 3, 5, 12),
    (14, 13, 15, 2, 1, 8, 6, 7, 9, 11, 0, 4, 10, 12, 5, 3),
    (15, 14, 13, 9, 12, 2, 11, 1, 10, 7, 8, 6, 0, 5, 4, 3),
)

FIRST = (
    (1, 2, 3, 5),
    (0, 2, 3, 4, 5),
    (0, 1, 3, 4, 6),
    (0, 2, 4, 6),
    (1, 2, 3, 5, 6, 7),
    (2, 3, 4, 6, 7),
    (2, 4, 5, 7),
    (2, 3, 5, 6),
    (3, 4, 5, 6, 7, 9, 10, 11, 12, 13),
    (4, 5, 6, 7, 8, 10, 11, 12),
    (0, 5, 6, 7, 8, 9, 11, 12, 13),
    (0, 6, 7, 9, 10, 12, 13),
    (0, 9, 10, 11, 13, 14, 15),
    (0, 3, 8, 10, 11, 12, 14, 15),
    (0, 1, 2, 3, 4, 8, 9, 10, 11, 13, 15),
    (0, 1, 2, 4, 11, 12, 13, 14),
)

ROUTES = (
    (
        (0, 0, 0, 0, 1, 5, 2, 3), (0, 0, 1, 0, 1, 5, 2, 3), (0, 0, 0, 2, 1), (0, 0, 1, 2, 1),
        (0, 1, 0, 0, 1, 3, 5, 2), (0, 1, 1, 0, 1, 3, 5, 2), (0, 0, 0, 3, 1), (0, 0, 1, 3, 1), (0, 0, 0, 1),
        (0, 0, 1, 1), (0, 1, 0, 2, 1), (3, 15), (3, 14), (1, 0, 0, 2, 14), (1, 0, 1, 2, 14), (1, 0, 0, 1, 14),
        (1, 0, 1, 1, 14), (1, 1, 0, 2, 14), (3, 13), (1, 0, 0, 0, 13), (1, 0, 1, 0, 13), (1, 1, 0, 0, 13),
        (1, 1, 1, 0, 13), (1, 0, 0, 1, 13), (1, 0, 1, 1, 13), (0, 1, 1, 2, 1, 14), (0, 1, 0, 3, 1), (0, 1, 1, 3, 1),
        (0, 0, 1, 13, 15, 1), (0, 1, 0, 1, 14, 13), (0, 0, 1, 12, 15, 3, 1), (0, 0, 0, 13, 15, 1),
        (0, 1, 1, 1, 14, 13), (0, 0, 0, 12, 15, 3, 1), (0, 0, 1, 11, 15, 1), (0, 0, 0, 11, 15, 1), (2, 0),
        (0, 0, 1, 10, 1, 15), (0, 0, 0, 10, 1, 15), (0, 1, 1, 13, 1, 15), (0, 1, 1, 12, 15, 3, 1),
        (0, 1, 0, 13, 1, 15), (0, 1, 0, 12, 15, 3, 1), (0, 1, 1, 11, 15, 1), (2, 1), (0, 1, 0, 11, 15, 1),
        (0, 0, 0, 8, 15, 1), (0, 1, 1, 10, 1, 15), (0, 0, 1, 8, 15, 1), (0, 1, 0, 10, 1, 15), (2, 2),
        (0, 1, 0, 8, 1, 15), (2, 3), (0, 1, 1, 8, 1, 15), (2, 4),
    ),
    (
        (0, 0, 0, 1, 5, 2), (0, 0, 1, 1, 5, 2), (0, 1, 0, 1, 5, 2), (0, 1, 1, 1, 5, 2), (0, 0, 0, 4, 0, 2, 3),
        (0, 0, 1, 4, 0, 2, 3), (0, 0, 0, 5, 0), (0, 0, 1, 5, 0), (3, 14), (0, 0, 1, 6, 0, 14), (0, 0, 0, 6, 0, 14),
        (0, 1, 0, 4, 2, 0, 3), (0, 1, 1, 4, 2, 0, 3), (0, 1, 0, 5, 0), (2, 0), (0, 0, 1, 13, 4, 2), (0, 1, 1, 5, 0),
        (0, 0, 0, 13, 4, 2), (0, 1, 1, 6, 0, 14), (0, 0, 1, 11, 2, 3), (0, 1, 0, 6, 0, 14), (0, 0, 0, 11, 2, 3),
        (0, 1, 1, 13, 4, 2), (2, 1), (0, 1, 0, 13, 4, 2), (0, 1, 1, 11, 3, 2), (0, 1, 0, 11, 3, 2), (2, 2), (2, 3),
        (2, 4),
    ),
    (
        (0, 0, 0, 2, 0, 4), (0, 0, 1, 2, 0, 4), (0, 0, 0, 1, 6, 3, 0), (0, 0, 1, 1, 6, 3, 0), (0, 1, 0, 2, 4, 0),
        (0, 1, 1, 2, 4, 0), (0, 0, 0, 5, 3, 1), (0, 0, 1, 5, 3, 1), (0, 0, 1, 6, 1, 4), (0, 0, 0, 6, 1, 4),
        (0, 1, 0, 1, 6, 0, 3), (0, 1, 1, 1, 6, 0, 3), (0, 0, 1, 7, 0, 1), (0, 0, 0, 7, 0, 1), (0, 1, 0, 5, 3, 1),
        (0, 1, 1, 5, 3, 1), (0, 0, 1, 15, 1, 3, 0, 4), (2, 0), (0, 0, 0, 15, 1, 3, 0, 4), (0, 0, 1, 14, 4, 0, 1),
        (0, 1, 1, 6, 4, 1), (0, 1, 0, 6, 4, 1), (0, 0, 0, 14, 4, 0, 1), (0, 1, 1, 7, 1, 0), (0, 1, 0, 7, 1, 0),
        (0, 1, 1, 15, 0, 4, 3, 1), (2, 1), (0, 1, 0, 15, 0, 4, 3, 1), (0, 1, 1, 14, 1, 0, 4), (0, 1, 0, 14, 1, 0, 4),
        (2, 2), (2, 3), (2, 4),
    ),
    (
        (0, 0, 0, 3, 4, 6, 2, 0), (0, 0, 1, 3, 4, 6, 2, 0), (0, 1, 0, 3, 4, 2, 0, 6), (0, 1, 1, 3, 4, 2, 0, 6),
        (0, 0, 0, 0, 4), (0, 0, 1, 0, 4), (0, 1, 0, 0, 4), (3, 14), (3, 13), (0, 0, 0, 8, 6, 2), (0, 1, 1, 0, 4),
        (0, 0, 1, 8, 6, 2), (2, 0), (0, 0, 1, 12, 2, 14, 13, 4), (0, 1, 0, 8, 2, 6), (0, 0, 0, 12, 2, 14, 13, 4),
        (0, 1, 1, 8, 2, 6), (2, 1), (0, 1, 1, 12, 2, 14, 13, 4), (0, 1, 0, 12, 2, 14, 13, 4), (2, 2), (2, 3), (2, 4),
    ),
    (
        (0, 0, 0, 4, 6, 1), (0, 0, 1, 4, 6, 1), (0, 0, 0, 2, 7, 6, 5, 3), (0, 0, 1, 2, 7, 6, 5, 3),
        (0, 1, 0, 4, 1, 6), (0, 1, 1, 4, 1, 6), (0, 1, 0, 2, 5, 3, 6, 7), (0, 1, 1, 2, 5, 3, 6, 7), (3, 15), (3, 14),
        (0, 0, 1, 9, 3, 5, 2, 6), (0, 0, 0, 9, 3, 5, 2, 6), (0, 0, 1, 15, 5, 7), (0, 0, 0, 15, 5, 7),
        (0, 1, 1, 9, 5, 6, 2, 3), (2, 0), (0, 0, 1, 14, 7, 6, 3), (0, 1, 0, 9, 5, 6, 2, 3), (0, 0, 0, 14, 7, 6, 3),
        (2, 1), (0, 0, 1, 13, 6, 3, 5), (0, 0, 0, 13, 6, 3, 5), (0, 1, 1, 15, 7, 5), (0, 1, 0, 15, 7, 5),
        (0, 1, 1, 14, 6, 7, 3), (0, 0, 0, 5, 15, 14, 6), (0, 1, 0, 14, 6, 7, 3), (0, 1, 1, 13, 3, 5, 6),
        (0, 1, 0, 13, 3, 5, 6), (0, 0, 1, 5, 15, 14, 6), (2, 2), (0, 1, 0, 5, 15, 14, 6), (2, 3),
        (0, 1, 1, 5, 15, 14, 6), (2, 4),
    ),
    (
        (0, 0, 0, 5, 2), (0, 0, 1, 5, 2), (0, 0, 0, 1, 4, 7), (0, 1, 0, 5, 2), (0, 1, 1, 5, 2), (0, 0, 1, 7, 4, 3, 6),
        (0, 0, 1, 1, 4, 7), (0, 0, 0, 7, 4, 3, 6), (3, 8), (1, 0, 0, 5, 8), (1, 0, 1, 5, 8), (1, 1, 0, 5, 8),
        (1, 1, 1, 5, 8), (3, 10), (1, 0, 0, 1, 10), (1, 0, 1, 1, 10), (0, 1, 1, 7, 3, 4, 6), (0, 1, 0, 1, 4, 7, 10),
        (0, 1, 0, 7, 3, 4, 6), (0, 1, 1, 1, 4, 7, 10), (2, 0), (0, 0, 1, 10, 3, 4, 2), (0, 0, 0, 10, 3, 4, 2),
        (0, 1, 1, 10, 4, 2, 3), (0, 1, 0, 10, 4, 2, 3), (2, 1), (2, 2), (2, 3), (2, 4),
    ),
    (
        (0, 0, 1, 6, 5, 2, 7), (0, 0, 0, 6, 5, 2, 7), (0, 0, 0, 3, 7), (0, 0, 0, 4, 7, 5), (0, 0, 1, 4, 7, 5),
        (0, 0, 1, 3, 7), (0, 1, 1, 6, 5, 2, 7), (0, 1, 0, 6, 5, 2, 7), (3, 9), (1, 0, 0, 4, 9), (1, 0, 1, 4, 9),
        (3, 8), (1, 0, 0, 3, 8), (1, 0, 1, 3, 8), (0, 1, 0, 3, 7, 8), (0, 1, 0, 4, 5, 7, 9), (0, 1, 1, 4, 5, 7, 9),
        (0, 0, 1, 10, 7, 5), (0, 0, 0, 10, 7, 5), (0, 1, 1, 3, 7, 8), (0, 0, 1, 11, 5, 4, 8), (0, 0, 0, 11, 5, 4, 8),
        (0, 1, 1, 10, 7, 5), (0, 1, 0, 10, 7, 5), (2, 0), (0, 1, 1, 11, 8, 4, 5), (0, 0, 0, 8, 5, 4, 7),
        (0, 0, 1, 8, 5, 4, 7), (0, 1, 0, 11, 8, 4, 5), (2, 1), (0, 1, 0, 8, 4, 5, 7), (0, 0, 1, 13, 9, 8, 7),
        (0, 0, 0, 13, 9, 8, 7), (0, 1, 1, 8, 4, 5, 7), (0, 1, 1, 13, 9, 8, 7), (2, 2), (0, 1, 0, 13, 9, 8, 7), (2, 3),
        (2, 4),
    ),
    (
        (0, 0, 1, 7, 5, 2), (0, 0, 0, 7, 5, 2), (0, 0, 1, 6, 3), (0, 0, 0, 6, 3), (0, 1, 1, 7, 5, 2), (3, 9),
        (1, 0, 1, 6, 9), (1, 0, 0, 6, 9), (0, 1, 0, 7, 5, 2), (3, 8), (1, 0, 1, 7, 8), (1, 0, 0, 7, 8),
        (1, 0, 1, 6, 8), (1, 0, 0, 6, 8), (1, 1, 1, 7, 8), (1, 1, 0, 7, 8), (3, 10), (1, 0, 1, 7, 10),
        (1, 0, 0, 7, 10), (1, 1, 1, 7, 10), (1, 1, 0, 7, 10), (0, 1, 1, 6, 8, 3, 9), (0, 1, 0, 6, 8, 3, 9), (2, 0),
        (0, 0, 1, 15, 9, 10, 8, 6), (0, 0, 0, 15, 9, 10, 8, 6), (2, 1), (0, 1, 1, 15, 9, 6, 10, 8),
        (0, 1, 0, 15, 9, 6, 10, 8), (2, 2), (2, 3), (2, 4),
    ),
    (
        (0, 0, 0, 8, 9, 12, 10, 3, 11), (0, 0, 1, 8, 9, 12, 10, 3, 11), (0, 1, 0, 8, 9, 11, 3, 12, 10),
        (0, 1, 1, 8, 9, 11, 3, 12, 10), (0, 0, 0, 3, 10, 13, 5, 9), (0, 0, 1, 3, 10, 13, 5, 9),
        (0, 0, 0, 5, 11, 4, 9, 7), (2, 0), (0, 0, 1, 5, 11, 4, 9, 7), (0, 1, 0, 5, 7, 11, 9, 4),
        (0, 1, 0, 3, 13, 9, 5, 10), (0, 1, 1, 5, 7, 11, 9, 4), (0, 1, 1, 3, 13, 9, 5, 10), (2, 1),
        (0, 0, 0, 0, 6, 7, 9), (0, 0, 1, 0, 6, 7, 9), (0, 1, 0, 0, 9, 7, 6), (0, 1, 1, 0, 9, 7, 6), (2, 2), (2, 3),
        (2, 4),
    ),
    (
        (0, 0, 1, 9, 7, 8, 10, 4, 12), (0, 0, 0, 9, 7, 8, 10, 4, 12), (0, 1, 1, 9, 4, 7, 8, 12, 10),
        (0, 1, 0, 9, 4, 7, 8, 12, 10), (0, 0, 1, 12, 7, 6, 5, 8), (0, 0, 0, 12, 7, 6, 5, 8), (0, 0, 0, 4, 8, 10, 12),
        (0, 0, 1, 4, 8, 10, 12), (2, 0), (0, 1, 1, 12, 5, 8, 6, 7), (0, 1, 0, 12, 5, 8, 6, 7),
        (0, 1, 0, 4, 12, 10, 8), (0, 1, 1, 4, 12, 10, 8), (0, 0, 0, 2, 11, 10, 8, 12), (0, 0, 1, 2, 11, 10, 8, 12),
        (2, 1), (0, 1, 0, 2, 11, 8, 12, 10), (0, 1, 1, 2, 11, 8, 12, 10), (2, 2), (2, 3), (2, 4),
    ),
    (
        (0, 0, 1, 10, 12, 9, 6, 0, 11, 8), (0, 0, 0, 10, 12, 9, 6, 0, 11, 8), (0, 1, 1, 10, 6, 11, 8, 0, 12, 9),
        (0, 1, 0, 10, 6, 11, 8, 0, 12, 9), (0, 0, 1, 7, 13, 9), (0, 0, 1, 14, 9, 12, 11, 5), (0, 0, 0, 7, 13, 9),
        (0, 1, 1, 7, 13, 9), (0, 0, 0, 14, 9, 12, 11, 5), (0, 1, 0, 7, 13, 9), (2, 0), (0, 1, 1, 14, 9, 12, 11, 5),
        (0, 1, 0, 14, 9, 12, 11, 5), (2, 1), (0, 0, 0, 1, 12, 8, 9, 11), (0, 0, 1, 1, 12, 8, 9, 11),
        (0, 1, 0, 1, 9, 12, 8, 11), (0, 1, 1, 1, 9, 12, 8, 11), (2, 2), (2, 3), (2, 4),
    ),
    (
        (0, 0, 1, 11, 6, 9, 0, 10, 12, 7), (0, 0, 0, 11, 6, 9, 0, 10, 12, 7), (0, 1, 1, 11, 6, 12, 9, 10, 7, 0),
        (0, 1, 0, 11, 6, 12, 9, 10, 7, 0), (2, 0), (0, 0, 0, 5, 13, 12, 10), (0, 0, 1, 5, 13, 12, 10),
        (0, 1, 0, 5, 13, 10, 12), (2, 1), (0, 1, 1, 5, 13, 10, 12), (2, 2), (2, 3), (2, 4),
    ),
    (
        (0, 0, 1, 12, 10, 0, 11, 9), (0, 0, 0, 12, 10, 0, 11, 9), (0, 1, 1, 12, 10, 9, 0, 11), (0, 0, 1, 9, 11, 15),
        (0, 1, 0, 12, 10, 9, 0, 11), (0, 0, 0, 9, 11, 15), (0, 0, 0, 8, 14, 0, 13), (0, 0, 1, 8, 14, 0, 13),
        (0, 1, 1, 9, 11, 15), (0, 1, 0, 9, 11, 15), (0, 1, 0, 8, 0, 14, 13), (2, 0), (0, 1, 1, 8, 0, 14, 13),
        (0, 0, 0, 0, 14, 10, 15, 11), (0, 0, 1, 0, 14, 10, 15, 11), (0, 0, 0, 4, 13, 11, 15, 14),
        (0, 0, 1, 4, 13, 11, 15, 14), (0, 1, 0, 0, 11, 15, 10, 14), (0, 1, 1, 0, 11, 15, 10, 14), (2, 1),
        (0, 1, 0, 4, 11, 14, 13, 15), (0, 1, 1, 4, 11, 14, 13, 15), (2, 2), (2, 3), (2, 4),
    ),
    (
        (0, 0, 1, 13, 11, 12, 0, 14, 10), (0, 0, 0, 13, 11, 12, 0, 14, 10), (0, 1, 1, 13, 0, 12, 11, 14, 10),
        (0, 1, 0, 13, 0, 12, 11, 14, 10), (0, 0, 0, 0, 12, 8), (0, 0, 1, 7, 12, 14, 15, 11), (0, 0, 1, 0, 12, 8),
        (0, 1, 0, 0, 12, 8), (0, 1, 1, 0, 12, 8), (0, 0, 0, 7, 12, 14, 15, 11), (0, 1, 1, 7, 11, 12, 15, 14), (2, 0),
        (0, 1, 0, 7, 11, 12, 15, 14), (0, 0, 0, 3, 11, 14, 12, 15), (0, 0, 1, 3, 11, 14, 12, 15), (0, 0, 1, 6, 12),
        (2, 1), (0, 0, 0, 6, 12), (0, 1, 1, 6, 12), (0, 1, 0, 6, 12), (0, 1, 0, 3, 15, 14, 11, 12), (2, 2),
        (0, 1, 1, 3, 15, 14, 11, 12), (2, 3), (2, 4),
    ),
    (
        (0, 0, 1, 14, 8, 10, 15, 13, 2), (0, 0, 0, 14, 8, 10, 15, 13, 2), (0, 1, 1, 14, 10, 8, 15, 2, 13),
        (0, 1, 0, 14, 10, 8, 15, 2, 13), (0, 0, 0, 2, 9, 13, 15), (0, 0, 1, 2, 9, 13, 15), (0, 0, 0, 1, 15),
        (0, 0, 1, 1, 15), (0, 1, 0, 2, 15, 9, 13), (0, 1, 1, 2, 15, 9, 13), (0, 0, 1, 6, 13, 10, 15, 11),
        (0, 1, 0, 1, 15), (2, 0), (0, 0, 0, 6, 13, 10, 15, 11), (0, 1, 1, 1, 15), (0, 1, 1, 6, 10, 13, 11, 15),
        (0, 1, 0, 6, 10, 13, 11, 15), (2, 1), (2, 2), (2, 3), (2, 4),
    ),
    (
        (0, 0, 1, 15, 12, 11, 14, 2, 13), (0, 0, 0, 15, 12, 11, 14, 2, 13), (0, 1, 1, 15, 2, 14, 11, 13, 12),
        (0, 1, 0, 15, 2, 14, 11, 13, 12), (0, 0, 1, 9, 14, 0, 13, 1), (0, 0, 0, 9, 14, 0, 13, 1),
        (0, 0, 1, 11, 14, 13), (0, 0, 0, 11, 14, 13), (0, 0, 1, 10, 14, 13), (0, 0, 0, 10, 14, 13),
        (0, 1, 1, 9, 1, 0, 14, 13), (0, 1, 0, 9, 1, 0, 14, 13), (2, 0), (0, 1, 1, 11, 13, 14), (0, 1, 0, 11, 13, 14),
        (0, 1, 1, 10, 13, 14), (0, 1, 0, 10, 13, 14), (2, 1), (2, 2), (2, 3), (2, 4),
    ),
)

ASIDE = (
    (),
    (),
    (),
    (),
    (),
    (),
    (),
    (),
    (),
    (),
    (),
    (),
    (),
    (),
    (),
    (),
)

SLOT = [{source: i for i, source in enumerate(order)} for order in ORDER]
RELAYS = [[tuple(step[1:4]) for step in route if step[0] == 0 and step[3] != z] for z, route in enumerate(ROUTES)]
BOUNDS = (0, 4, 8, 12, 14, 16)
PART = [sum(slot >= bound for bound in BOUNDS[1:]) for slot in range(16)]
RSEMS = 10 + max(map(len, RELAYS))


def leaves(z, p):
    return [
        (wave, core, source)
        for source in ORDER[z][BOUNDS[p] : BOUNDS[p + 1]]
        for wave in range(2)
        for core in range(2)
        if source != z and (wave, core, source) not in RELAYS[z]
    ]


RING = (
    ("q_begin",), ("q_own",),
    ("q_relay", -1, 0, 0), ("q_relay", 1, 0, 0), ("q_relay", -1, 0, 1), ("q_relay", 1, 0, 1),
    ("k_own",),
    ("q_relay", -2, 0, 0), ("q_relay", 2, 0, 0), ("q_relay", -1, 1, 0), ("q_relay", 1, 1, 0),
    ("q_relay", -2, 0, 1), ("q_relay", 2, 0, 1), ("q_relay", -1, 1, 1), ("q_relay", 1, 1, 1),
    ("k_relay", -1), ("k_relay", 1),
    ("q_relay", -3, 0, 0), ("q_relay", 3, 0, 0), ("q_relay", -2, 1, 0), ("q_relay", 2, 1, 0),
    ("q_relay", -3, 0, 1), ("q_relay", 3, 0, 1), ("q_relay", -2, 1, 1), ("q_relay", 2, 1, 1),
    ("k_relay", -2), ("k_relay", 2),
    ("q_relay", -3, 1, 0), ("q_relay", 3, 1, 0), ("q_relay", -3, 1, 1), ("q_relay", 3, 1, 1),
    ("k_relay", -3), ("k_relay", 3),
)

LATE_RING = (
    ("q_begin",), ("q_own_first",),
    ("q_relay", -1, 1, 0), ("q_relay", 1, 1, 0), ("q_relay", -1, 1, 1), ("q_relay", 1, 1, 1),
    ("q_relay", -2, 1, 0), ("q_relay", 2, 1, 0), ("q_relay", -2, 1, 1), ("q_relay", 2, 1, 1),
    ("q_relay", -3, 1, 0), ("q_relay", 3, 1, 0), ("q_relay", -3, 1, 1), ("q_relay", 3, 1, 1),
    ("q_own_last",), ("k_own",),
    ("q_relay", -1, 0, 0), ("q_relay", 1, 0, 0), ("q_relay", -1, 0, 1), ("q_relay", 1, 0, 1),
    ("k_relay", -1), ("k_relay", 1),
    ("q_relay", -2, 0, 0), ("q_relay", 2, 0, 0), ("q_relay", -2, 0, 1), ("q_relay", 2, 0, 1),
    ("k_relay", -2), ("k_relay", 2),
    ("q_relay", -3, 0, 0), ("q_relay", 3, 0, 0), ("q_relay", -3, 0, 1), ("q_relay", 3, 0, 1),
    ("k_relay", -3), ("k_relay", 3),
)

PLAN_Q = (
    ("ring",),
    ("attend", 2), ("attend", 1), ("attend", 3),
    ("w_passed", 0), ("piece", 0, 1),
    ("q_last",), ("k_last",), ("attend", 0), ("piece", 0, 0),
    ("w_passed", 1), ("piece", 1, 2),
    ("reduced", 0, 2), ("reduced", 0, 1), ("reduced", 0, 3), ("reduced", 0, 0),
    ("reduced", 1, 2), ("reduced", 1, 1), ("reduced", 1, 3), ("reduced", 1, 0),
)

PLAN_W = (
    ("w_begin",), ("w_route", 0),
    ("a_got", 2), ("a_got", 1), ("a_got", 3), ("a_got", 0),
    ("w_piece", 2, 0, 4), ("w_route", 1), ("w_piece", 3, 0, 2), ("w_route", 2), ("w_piece", 3, 2, 2),
    ("reduced", 2, 0), ("reduced", 2, 1), ("reduced", 2, 3), ("reduced", 2, 2),
    ("reduced", 3, 0), ("reduced", 3, 1), ("reduced", 3, 3), ("reduced", 3, 2),
)


def by_place(z, do, low=0, high=16):
    if high - low == 1:
        do(low)
        return
    middle = (low + high) // 2
    pl.when(z < middle)(lambda: by_place(z, do, low, middle))
    pl.when(z >= middle)(lambda: by_place(z, do, middle, high))


def kernel(
    q, k, v, w, sums,
    qall, kvl, kvr, wv, wt, wcross, wall, bias, att, psend, xr, ssend, rbuf, size,
    lsem, ssem, rsem, wpsem, atsem, xsem, asem, go, late,
):
    yl, z, x, yh, c = (lax.axis_index(a) for a in ("yl", "z", "x", "yh", "c"))
    y = yh * 4 + yl

    def dev(dy=0, dz=0, dx=0, to_z=None, role=None):
        yt = lax.rem(y + (dy + 8), 8)
        zt = lax.rem(z + (dz + 16), 16) if to_z is None else to_z
        xt = lax.rem(x + dx, 4)
        core = role if to_z else jnp.where(xt + yt + zt == 0, 1 - role, role)
        return (lax.rem(yt, 4), zt, xt, lax.div(yt, 4), core)

    origin = x + y + z == 0
    for_q = jnp.where(origin, 1 - QC, QC) == c
    one_more = jnp.where(origin, 0, 1)

    def remote(src, dst, send_sem, recv_sem, to):
        return pltpu.make_async_remote_copy(
            src_ref=src, dst_ref=dst, send_sem=send_sem, recv_sem=recv_sem, device_id=to, device_id_type=MESH
        )

    sent = [0]

    def send(src, dst, recv_sem, to):
        remote(src, dst, ssem.at[0], recv_sem, to).start()
        sent[0] += math.prod(src.shape) * 2

    def received(dst, recv_sem):
        remote(dst, dst, ssem.at[0], recv_sem, (yl, z, x, yh, 1 - c)).wait_recv()

    def sized(bytes_):
        assert bytes_ % 8192 == 0 and bytes_ // 8192 <= size.shape[0]
        return size.at[pl.ds(0, bytes_ // 8192)]

    def half_of(r):
        return lax.div(lax.rem(y + (r + 8), 8), 4)

    w_load = pltpu.make_async_copy(w, wv, lsem.at[0])
    q_load = pltpu.make_async_copy(q, qall.at[0, yh, c], lsem.at[1])
    kv_load = [pltpu.make_async_copy(k, kvl.at[0], lsem.at[2]), pltpu.make_async_copy(v, kvl.at[1], lsem.at[2])]
    barrier = pltpu.get_barrier_semaphore()
    around_q = [dict(dy=1), dict(dy=-1), dict(dx=1), dict(dx=2), dict(dx=3)]

    w_load.start()
    for copy in kv_load:
        copy.start()
    q_load.start()

    @pl.when(for_q)
    def _():
        for peer in around_q:
            pl.semaphore_signal(barrier, inc=1, device_id=dev(role=QC, **peer), device_id_type=MESH)

    @pl.when(~for_q)
    def _():
        pl.semaphore_signal(barrier, inc=1, device_id=dev(dy=4, role=WC), device_id_type=MESH)

        @pl.when(~origin)
        def _():
            pl.semaphore_signal(barrier, inc=1, device_id=dev(role=QC), device_id_type=MESH)

        def greet(place):
            for other in range(16):
                if place in FIRST[other]:
                    pl.semaphore_signal(barrier, inc=1, device_id=dev(to_z=other, role=WC), device_id_type=MESH)
                if place in ASIDE[other]:
                    to = dev(dy=4, to_z=other, role=WC)
                    pl.semaphore_signal(barrier, inc=1, device_id=to, device_id_type=MESH)

        by_place(z, greet)

    w_load.wait()
    wt[...] = wv[...].astype(F32).T.astype(BF16).reshape(2, 64, 256)
    for copy in kv_load:
        copy.wait()

    def lanes_of(half, core):
        return pl.ds(pl.multiple_of((half * 2 + core) * 256, 256), 256)

    def head_of(i):
        return pl.ds(pl.multiple_of(i * 128, 128), 128)

    def unit(slot, wave, core):
        return wall.at[slot, :, lanes_of(1 - yh if wave else yh, core)]

    def w_sem(place, wave, core, source):
        if (wave, core, source) in RELAYS[place]:
            return rsem.at[10 + RELAYS[place].index((wave, core, source))]
        return rsem.at[5 + PART[SLOT[place][source]]]

    def w_sends(place, wave, core, source, targets):
        for t in targets:
            here, there = SLOT[place][source], SLOT[t][source]
            to = dev(to_z=t, role=WC)
            send(unit(here, wave, core), unit(there, wave, core), w_sem(t, wave, core, source), to)

    def w_cross(place, core):
        for t in ASIDE[place]:
            there = wall.at[SLOT[t][place], :, lanes_of(yh, core)]
            send(wcross.at[core], there, w_sem(t, 1, core, place), dev(dy=4, to_z=t, role=WC))
        send(wcross.at[core], wall.at[0, :, lanes_of(yh, core)], rsem.at[2 + core], dev(dy=4, role=WC))

    waited = []

    def w_step(place, kind, *step):
        if kind == 3:
            pl.semaphore_wait(late.at[step[0] - 8], 1)
            return
        if kind == 2:
            p = step[0]
            if leaves(place, p):
                received(sized(len(leaves(place, p)) * 32768), rsem.at[5 + p])
            if p < 2:
                rows = pl.ds(4 * p, 4)
                send(wall.at[rows], wall.at[rows], wpsem.at[p], dev(role=QC))
            return
        wave, core, source, *targets = step
        if kind == 0:
            if source != place:
                received(unit(SLOT[place][source], wave, core), w_sem(place, wave, core, source))
            elif wave:
                received(unit(0, 1, core), rsem.at[2 + core])
            else:
                if (core == QC or place == 0) and place not in waited:
                    received(sized(65536), rsem.at[4])
                    waited.append(place)
                w_cross(place, core)
        w_sends(place, wave, core, source, targets)

    def w_route(part):
        totals = []

        def go_on(place):
            route = ROUTES[place]
            first = 1 + max(i for i, step in enumerate(route) if step[0] != 2 or step[1] == 2)
            cuts = (0, first, max(first, 1 + route.index((2, 3))), len(route))
            start = sent[0]
            for step in route[cuts[part] : cuts[part + 1]]:
                with jax.named_scope("_".join(map(str, ("at", place, *step)))):
                    w_step(place, *step)
            totals.append(sent[0] - start)
            sent[0] = start

        by_place(z, go_on)
        w_totals.append(totals)

    w_totals = []

    def w_passed(p):
        received(wall.at[pl.ds(4 * p, 4)], wpsem.at[p])

    def q_part(r, s, u):
        return qall.at[r % 4, half_of(r), s, pl.ds(128 * u, 128)]

    def q_sem(t, s, u):
        return rsem.at[0 if t == 4 else 8 + 4 * (t if t < 4 else t - 1) + 2 * s + u]

    def q_send(r, s, u, hop):
        t = (r - hop) % 8
        rows = pl.ds(128 * u, 128)
        dst = qall.at[t % 4, half_of(r), s, rows]
        send(q_part(r, s, u), dst, q_sem(t, s, u), dev(dy=hop, role=QC))

    def q_relay(r, s, u):
        received(q_part(r, s, u), q_sem(r % 8, s, u))
        if abs(r) < 3 or s == (0 if r < 0 else 1):
            q_send(r, s, u, 1 if r < 0 else -1)

    def q_last():
        received(qall.at[0, half_of(4)], rsem.at[0])

    def k_send(r, hop):
        t = (r - hop) % 8
        some = pl.ds(0 if hop > 0 else 2, 2) if t == 4 else pl.ds(0, 4)
        src, dst = kvr.at[r % 4, half_of(r), some], kvr.at[t % 4, half_of(r), some]
        send(src, dst, rsem.at[t if t else 8], dev(dy=hop, role=QC))

    def k_relay(r):
        received(kvr.at[r % 4, half_of(r)], rsem.at[r % 8])
        k_send(r, 1 if r < 0 else -1)

    def k_last():
        received(kvr.at[0, half_of(4)], rsem.at[4])

    def k_spread():
        for d in (2, 1, 3):
            head = head_of(lax.rem(x + d, 4))
            send(kvl.at[:, :, head], kvr.at[0, yh, x, :, c], rsem.at[8], dev(dx=d, role=QC))

    def k_own():
        received(sized(7 * 8192), rsem.at[8])
        k_send(0, 1)
        k_send(0, -1)

    def ring():
        before = sent[0]
        for late, plan in ((False, RING), (True, LATE_RING)):
            sent[0] = before

            def go_round(plan=plan):
                for step in plan:
                    do(*step)

            pl.when((x + z == 0) if late else (x + z > 0))(go_round)

    def q_own_first():
        once(~origin, None, q_own)

    def q_own_last():
        before = sent[0]
        pl.when(origin)(q_own)
        sent[0] = before

    def w_hand():
        send(wt.at[yh], unit(0, 0, c), rsem.at[4], dev(role=WC))
        send(wt.at[1 - yh], wcross.at[c], rsem.at[4], dev(role=WC))

    def once(first, second, do):
        before = sent[0]
        pl.when(second if first is None else first)(do)
        if first is None:
            sent[0] = before

    def q_own():
        received(qall.at[0, yh, 1 - c], rsem.at[9])
        for u in range(2):
            for hop in (1, -1):
                q_send(0, 1 - c, u, hop)
        before = sent[0]
        pl.when(origin)(w_hand)
        sent[0] = before

    def q_begin():
        pl.semaphore_wait(barrier, len(around_q) + one_more)

        def meet():
            pl.semaphore_signal(go, inc=1, device_id=dev(role=WC), device_id_type=MESH)
            w_hand()

        once(~origin, None, meet)

        @pl.when(origin)
        def _():
            pl.semaphore_signal(barrier, inc=1, device_id=dev(role=WC), device_id_type=MESH)

        k_spread()
        kvr[0, yh, x, :, c] = kvl[:, :, head_of(x)]
        q_load.wait()
        for u in range(2):
            for hop in (1, -1):
                q_send(0, c, u, hop)
        row = lax.broadcasted_iota(jnp.int32, (128, 128), 0)
        col = lax.broadcasted_iota(jnp.int32, (128, 128), 1)
        bias[...] = jnp.where((lax.div(row, 32) == lax.div(col, 32)) & (col <= row), 0.0, -1e30)

    def w_begin():
        wall[0, :, lanes_of(yh, c)] = wt[yh]
        wcross[c] = wt[1 - yh]
        q_load.wait()

        def give():
            send(qall.at[0, yh, c], qall.at[0, yh, c], rsem.at[9], dev(role=QC))
            k_spread()
            send(kvl.at[:, :, head_of(x)], kvr.at[0, yh, x, :, c], rsem.at[8], dev(role=QC))

        def meet():
            pl.semaphore_wait(go, 1)
            give()

        once(~origin, None, meet)

        def greeted(place):
            pl.semaphore_wait(barrier, 2 + len(FIRST[place]) + len(ASIDE[place]) - one_more)
            for other in range(8):
                if (3, place) in ROUTES[other]:
                    to = dev(to_z=other, role=WC)
                    pl.semaphore_signal(late.at[place - 8], inc=1, device_id=to, device_id_type=MESH)

        by_place(z, greeted)
        once(None, origin, give)

    def attend(gs):
        for t in range(2):
            pair = kvr[gs, t]
            keys, values = pair[:, 0].reshape(128, 128), pair[:, 1].reshape(128, 128)
            values = jnp.concatenate([values, jnp.ones((128, 128), BF16)], axis=1)
            for h in range(2):
                queries = jnp.concatenate(
                    [
                        qall[gs, h, s, :, j * 128 : j * 128 + 128].reshape(4, 2, 32, 128)[:, t].reshape(128, 128)
                        for s in range(2)
                        for j in range(2)
                    ],
                    axis=0,
                )
                scores = lax.dot_general(queries, keys, NT, preferred_element_type=F32)
                scores = scores * (1.0 / math.sqrt(128.0)) + jnp.concatenate([bias[...]] * 4, axis=0)
                powers = jnp.exp(scores - jnp.max(scores, axis=-1, keepdims=True)).astype(BF16)
                total = jnp.dot(powers, values, preferred_element_type=F32)
                heads = (total[:, :128] / total[:, 128:]).astype(BF16)
                for i in range(4):
                    att[gs, t, :, h * 512 + i * 128 : h * 512 + i * 128 + 128] = heads[i * 128 : i * 128 + 128]
        send(att.at[gs], att.at[gs], atsem.at[gs], dev(role=WC))

    def a_got(gs):
        received(att.at[gs], atsem.at[gs])

    def spread(p, gs, lanes):
        for d in (2, 1, 3):
            src = psend.at[p % 2, gs, :, lax.rem(x + d, 4), :, lanes]
            dst = xr.at[p % 2, gs, d - 1, :, :, lanes]
            send(src, dst, xsem.at[p % 2, gs], dev(dx=d, role=QC if p < 2 else WC))

    def piece(p, which):
        groups = (slice(0, 1), slice(1, 4), slice(0, 4))[which]
        n = groups.stop - groups.start
        rows = wall[4 * p : 4 * p + 4].reshape(256, 1024)
        total = lax.dot_general(att[groups].reshape(n * 256, 1024), rows, NT, preferred_element_type=F32)
        psend[p, groups] = total.astype(BF16).reshape(n, 2, 4, 32, 256)
        for gs in ((0,), (2, 1, 3), (2, 1, 3, 0))[which]:
            spread(p, gs, pl.ds(0, 256))

    def w_piece(p, slot, n):
        slots = slice(4 * p + slot, 4 * p + slot + n)
        rows = wall[slots].reshape(64 * n, 1024)
        total = lax.dot_general(att[...].reshape(1024, 1024), rows, NT, preferred_element_type=F32)
        lanes = slice(64 * slot, 64 * (slot + n))
        psend[p - 2, :, :, :, :, lanes] = total.astype(BF16).reshape(4, 2, 4, 32, 64 * n)
        for gs in (0, 1, 3, 2):
            spread(p, gs, pl.ds(64 * slot, 64 * n))

    def reduced(p, gs):
        received(xr.at[p % 2, gs], xsem.at[p % 2, gs])
        total = psend[p % 2, gs, :, x].astype(F32)
        for d in range(3):
            total = total + xr[p % 2, gs, d].astype(F32)
        ssend[p % 2, gs] = total.astype(BF16).reshape(2, 2, 16, 256)
        for other in (1, 0):
            half = 1 - yh if other else yh
            there = half * 4 + lax.rem(yl + gs, 4)
            place = lax.rem(y + 8 - there, 8)
            for core in (1 - c, c):
                home = (lax.rem(yl + gs, 4), z, x, half, core)
                if gs or other:
                    send(ssend.at[p % 2, gs, half, core], rbuf.at[p, place], asem.at[p], home)
                elif core is c:
                    rbuf[p, 0] = ssend[p % 2, 0, yh, c]
                else:
                    send(ssend.at[p % 2, 0, yh, core], rbuf.at[p, 0], asem.at[4 + p % 2], home)

    steps = dict(
        q_begin=q_begin, w_begin=w_begin, q_own=q_own, q_relay=q_relay, q_last=q_last, k_own=k_own, k_relay=k_relay,
        k_last=k_last, attend=attend, w_route=w_route, w_passed=w_passed, a_got=a_got, piece=piece, w_piece=w_piece, reduced=reduced,
        ring=ring, q_own_first=q_own_first, q_own_last=q_own_last,
    )

    def do(name, *numbers):
        with jax.named_scope("_".join(map(str, (name, *numbers)))):
            steps[name](*numbers)

    def follow(plan):
        sent[0] = 0
        for step in plan:
            do(*step)

    def drain(bytes_):
        stand_in = sized(bytes_)
        remote(stand_in, stand_in, ssem.at[0], ssem.at[0], (yl, z, x, yh, 1 - c)).wait_send()

    def arrive(mine):
        with jax.named_scope("arrive"):
            outs = []
            for p in range(PIECES):
                received(rbuf.at[p, pl.ds(1, 7)], asem.at[p])
                if p // 2 != mine:
                    received(rbuf.at[p, 0], asem.at[4 + p % 2])
                outs.append(pltpu.make_async_copy(rbuf.at[p], sums.at[p], lsem.at[3 + p]))
                outs[-1].start()
            if mine:
                by_place(z, lambda place: drain(sent[0] + sum(totals[place] for totals in w_totals)))
            else:
                drain(sent[0])
            for copy in outs:
                copy.wait()

    @pl.when(for_q)
    def _():
        follow(PLAN_Q)
        arrive(0)

    @pl.when(~for_q)
    def _():
        follow(PLAN_W)
        arrive(1)


def last_kernel(sums, res, gain, hid, nrm, rbuf, resv, gv, u, hidv, nrmv, sem):
    yl, z, yh = (lax.axis_index(a) for a in ("yl", "z", "yh"))
    y = yh * 4 + yl
    loads = [
        pltpu.make_async_copy(res, resv, sem.at[0]),
        pltpu.make_async_copy(gain, gv, sem.at[0]),
    ]
    loads += [pltpu.make_async_copy(sums.at[p], rbuf.at[p], sem.at[1 + p]) for p in range(PIECES)]
    for copy in loads:
        copy.start()

    def source_of(slot):
        low, high = (
            sum(ORDER[8 * part + i][slot] << (4 * i) for i in range(8)) for part in range(2)
        )
        low, high = (n - (1 << 32) if n >> 31 else n for n in (low, high))
        word = jnp.where(z < 8, jnp.int32(low), jnp.int32(high))
        return lax.shift_right_logical(word, 4 * lax.rem(z, 8)) & 15

    for copy in loads[:2]:
        copy.wait()
    squares = jnp.zeros((16, 128), F32)
    low = lax.broadcasted_iota(jnp.int32, (16, 128), 1) < 64
    for p in range(PIECES):
        sources = [source_of(4 * p + i) for i in range(4)]
        loads[2 + p].wait()
        for r in range(4):
            here = lax.div(lax.rem(y + r, 8), 4)
            first, second = r + 4 * here, r + 4 - 4 * here
            for t in range(2):
                lanes = slice(t * 128, t * 128 + 128)
                a = rbuf[p, first, :, lanes].astype(F32)
                b = rbuf[p, second, :, lanes].astype(F32)
                pair = (jnp.where(low, a, pltpu.roll(b, 64, 1)), jnp.where(low, pltpu.roll(a, 64, 1), b))
                for i in range(2):
                    block = lax.rem(yl + r, 4) * 16 + sources[2 * t + i]
                    at = pl.ds(pl.multiple_of(block * 128, 128), 128)
                    updated = resv[:, at].astype(F32) + pair[i]
                    u[:, at] = updated
                    hidv[:, at] = updated.astype(BF16)
                    squares = squares + updated * updated
    stores = [pltpu.make_async_copy(hidv, hid, sem.at[5])]
    stores[0].start()
    scale = lax.rsqrt(jnp.sum(squares, axis=-1, keepdims=True) * (1.0 / 8192.0) + 1e-05)
    for part in range(2):
        for block in range(32 * part, 32 * part + 32):
            lanes = slice(block * 128, block * 128 + 128)
            nrmv[:, lanes] = (u[:, lanes] * scale * gv[block : block + 1, :]).astype(BF16)
        lanes = pl.ds(4096 * part, 4096)
        stores.append(pltpu.make_async_copy(nrmv.at[:, lanes], nrm.at[:, lanes], sem.at[6 + part]))
        stores[-1].start()
    for copy in stores:
        copy.wait()


def local(queries, keys, values, out_weight, residual, norm_gain):
    in_hbm = pl.BlockSpec(memory_space=pltpu.HBM)
    vmem = pltpu.VMEM
    dma = pltpu.SemaphoreType.DMA
    sums = pl.pallas_call(
        kernel,
        out_shape=jax.ShapeDtypeStruct((PIECES, 8, 16, 256), BF16),
        in_specs=[in_hbm] * 4,
        out_specs=in_hbm,
        scratch_shapes=[
            vmem((4, 2, 2, 256, 256), BF16),
            vmem((2, 16, 512), BF16),
            vmem((4, 2, 4, 2, 2, 16, 128), BF16),
            vmem((256, 128), BF16),
            vmem((2, 64, 256), BF16),
            vmem((2, 64, 256), BF16),
            vmem((16, 64, 1024), BF16),
            vmem((128, 128), F32),
            vmem((4, 2, 128, 1024), BF16),
            vmem((2, 4, 2, 4, 32, 256), BF16),
            vmem((2, 4, 3, 2, 32, 256), BF16),
            vmem((2, 4, 2, 2, 16, 256), BF16),
            vmem((PIECES, 8, 16, 256), BF16),
            vmem((1200, 16, 256), BF16),
            dma((3 + PIECES,)),
            dma((1,)),
            dma((max(40, RSEMS),)),
            dma((2,)),
            dma((4,)),
            dma((2, 4)),
            dma((6,)),
            pltpu.SemaphoreType.REGULAR,
            pltpu.SemaphoreType.REGULAR((8,)),
        ],
        compiler_params=pltpu.CompilerParams(collective_id=0, has_side_effects=True, vmem_limit_bytes=VMEM),
        name="layer",
    )(queries, keys, values, out_weight)
    return pl.pallas_call(
        last_kernel,
        out_shape=(jax.ShapeDtypeStruct((16, 8192), BF16),) * 2,
        in_specs=[in_hbm] * 3,
        out_specs=(in_hbm,) * 2,
        scratch_shapes=[
            vmem((PIECES, 8, 16, 256), BF16),
            vmem((16, 8192), BF16),
            vmem((64, 128), F32),
            vmem((16, 8192), F32),
            vmem((16, 8192), BF16),
            vmem((16, 8192), BF16),
            dma((8,)),
        ],
        compiler_params=pltpu.CompilerParams(vmem_limit_bytes=VMEM),
        name="final",
    )(sums, residual, norm_gain.reshape(64, 128))


def solution(mesh):
    finer = Mesh(mesh.devices.reshape(4, 16, 4, 2, 2), ("yl", "z", "x", "yh", "c"))
    rows, heads = ("yl", "z"), ("x", "yh", "c")
    both = rows + heads
    in_specs = (P(rows, heads), P(both, None), P(both, None), P(heads, rows), P(both, None), P())
    out_specs = (P(both, None), P(both, None))
    return jax.shard_map(local, mesh=finer, in_specs=in_specs, out_specs=out_specs, check_vma=False)
```

```python
import math

import jax
import jax.numpy as jnp
from jax import lax
from jax.experimental import pallas as pl
from jax.experimental.pallas import tpu as pltpu
from jax.sharding import Mesh
from jax.sharding import PartitionSpec as P

MESH = pl.DeviceIdType.MESH
F32, BF16 = jnp.float32, jnp.bfloat16
NT = (((1,), (1,)), ((), ()))

QC, WC = 0, 1
VMEM = 60 * 1024 * 1024
PIECES = 4

ORDER = (
    (0, 2, 3, 1, 4, 13, 5, 12, 6, 11, 7, 15, 10, 14, 8, 9),
    (1, 0, 4, 2, 3, 5, 6, 7, 13, 15, 12, 14, 11, 10, 9, 8),
    (2, 1, 3, 5, 0, 6, 4, 7, 15, 14, 13, 8, 9, 11, 10, 12),
    (3, 1, 0, 2, 5, 7, 4, 6, 8, 15, 9, 12, 10, 14, 11, 13),
    (4, 3, 2, 7, 0, 1, 6, 9, 15, 10, 14, 13, 11, 12, 5, 8),
    (5, 6, 7, 1, 2, 4, 0, 10, 9, 11, 15, 3, 13, 8, 12, 14),
    (6, 4, 3, 10, 7, 2, 1, 11, 9, 8, 12, 14, 13, 15, 5, 0),
    (7, 6, 9, 4, 3, 1, 2, 10, 5, 11, 12, 15, 8, 14, 0, 13),
    (8, 7, 9, 6, 10, 5, 3, 12, 11, 14, 4, 0, 2, 15, 13, 1),
    (9, 10, 8, 11, 6, 12, 7, 4, 14, 2, 5, 3, 15, 0, 1, 13),
    (10, 9, 11, 8, 7, 12, 13, 14, 4, 0, 1, 3, 2, 5, 6, 15),
    (11, 10, 12, 8, 13, 9, 15, 14, 0, 7, 5, 4, 2, 6, 1, 3),
    (12, 11, 13, 10, 9, 8, 15, 0, 14, 4, 7, 6, 5, 2, 1, 3),
    (13, 14, 15, 8, 0, 7, 2, 1, 6, 9, 4, 11, 10, 3, 5, 12),
    (14, 13, 15, 2, 1, 8, 6, 7, 9, 11, 0, 4, 10, 12, 5, 3),
    (15, 14, 13, 9, 12, 2, 11, 1, 10, 7, 8, 6, 0, 5, 4, 3),
)

FIRST = (
    (1, 2, 3, 5),
    (0, 2, 3, 4, 5),
    (0, 1, 3, 4, 6),
    (0, 2, 4, 6),
    (1, 2, 3, 5, 6, 7),
    (2, 3, 4, 6, 7),
    (2, 4, 5, 7),
    (2, 3, 5, 6),
    (3, 4, 5, 6, 7, 9, 10, 11, 12, 13),
    (4, 5, 6, 7, 8, 10, 11, 12),
    (0, 5, 6, 7, 8, 9, 11, 12, 13),
    (0, 6, 7, 9, 10, 12, 13),
    (0, 9, 10, 11, 13, 14, 15),
    (0, 3, 8, 10, 11, 12, 14, 15),
    (0, 1, 2, 3, 4, 8, 9, 10, 11, 13, 15),
    (0, 1, 2, 4, 11, 12, 13, 14),
)

ROUTES = (
    (
        (0, 0, 0, 0, 1, 5, 2, 3), (0, 0, 1, 0, 1, 5, 2, 3), (0, 0, 0, 2, 1), (0, 0, 1, 2, 1),
        (0, 1, 0, 0, 1, 3, 5, 2), (0, 1, 1, 0, 1, 3, 5, 2), (0, 0, 0, 3, 1), (0, 0, 1, 3, 1), (0, 0, 0, 1),
        (0, 0, 1, 1), (0, 1, 0, 2, 1), (3, 15), (3, 14), (1, 0, 0, 2, 14), (1, 0, 1, 2, 14), (1, 0, 0, 1, 14),
        (1, 0, 1, 1, 14), (1, 1, 0, 2, 14), (3, 13), (1, 0, 0, 0, 13), (1, 0, 1, 0, 13), (1, 1, 0, 0, 13),
        (1, 1, 1, 0, 13), (1, 0, 0, 1, 13), (1, 0, 1, 1, 13), (0, 1, 1, 2, 1, 14), (0, 1, 0, 3, 1), (0, 1, 1, 3, 1),
        (0, 0, 1, 13, 15, 1), (0, 1, 0, 1, 14, 13), (0, 0, 1, 12, 15, 3, 1), (0, 0, 0, 13, 15, 1),
        (0, 1, 1, 1, 14, 13), (0, 0, 0, 12, 15, 3, 1), (2, 0), (0, 0, 1, 11, 15, 1), (0, 0, 0, 11, 15, 1),
        (0, 0, 1, 10, 1, 15), (0, 0, 0, 10, 1, 15), (0, 1, 1, 13, 1, 15), (0, 1, 1, 12, 15, 3, 1),
        (0, 1, 0, 13, 1, 15), (0, 1, 0, 12, 15, 3, 1), (2, 1), (0, 1, 1, 11, 15, 1), (0, 1, 0, 11, 15, 1),
        (0, 0, 0, 8, 15, 1), (0, 1, 1, 10, 1, 15), (0, 0, 1, 8, 15, 1), (2, 2), (0, 1, 0, 10, 1, 15),
        (0, 1, 0, 8, 1, 15), (2, 3), (0, 1, 1, 8, 1, 15), (2, 4),
    ),
    (
        (0, 0, 0, 1, 5, 2), (0, 0, 1, 1, 5, 2), (0, 1, 0, 1, 5, 2), (0, 1, 1, 1, 5, 2), (0, 0, 0, 4, 0, 2, 3),
        (0, 0, 1, 4, 0, 2, 3), (0, 0, 0, 5, 0), (0, 0, 1, 5, 0), (3, 14), (0, 0, 1, 6, 0, 14), (0, 0, 0, 6, 0, 14),
        (0, 1, 0, 4, 2, 0, 3), (0, 1, 1, 4, 2, 0, 3), (2, 0), (0, 1, 0, 5, 0), (0, 0, 1, 13, 4, 2), (0, 1, 1, 5, 0),
        (0, 0, 0, 13, 4, 2), (0, 1, 1, 6, 0, 14), (0, 0, 1, 11, 2, 3), (0, 1, 0, 6, 0, 14), (0, 0, 0, 11, 2, 3),
        (2, 1), (0, 1, 1, 13, 4, 2), (0, 1, 0, 13, 4, 2), (0, 1, 1, 11, 3, 2), (2, 2), (0, 1, 0, 11, 3, 2), (2, 3),
        (2, 4),
    ),
    (
        (0, 0, 0, 2, 0, 4), (0, 0, 1, 2, 0, 4), (0, 0, 0, 1, 6, 3, 0), (0, 0, 1, 1, 6, 3, 0), (0, 1, 0, 2, 4, 0),
        (0, 1, 1, 2, 4, 0), (0, 0, 0, 5, 3, 1), (0, 0, 1, 5, 3, 1), (0, 0, 1, 6, 1, 4), (0, 0, 0, 6, 1, 4),
        (0, 1, 0, 1, 6, 0, 3), (0, 1, 1, 1, 6, 0, 3), (0, 0, 1, 7, 0, 1), (0, 0, 0, 7, 0, 1), (0, 1, 0, 5, 3, 1),
        (0, 1, 1, 5, 3, 1), (2, 0), (0, 0, 1, 15, 1, 3, 0, 4), (0, 0, 0, 15, 1, 3, 0, 4), (0, 0, 1, 14, 4, 0, 1),
        (0, 1, 1, 6, 4, 1), (0, 1, 0, 6, 4, 1), (0, 0, 0, 14, 4, 0, 1), (0, 1, 1, 7, 1, 0), (0, 1, 0, 7, 1, 0),
        (2, 1), (0, 1, 1, 15, 0, 4, 3, 1), (0, 1, 0, 15, 0, 4, 3, 1), (0, 1, 1, 14, 1, 0, 4), (0, 1, 0, 14, 1, 0, 4),
        (2, 2), (2, 3), (2, 4),
    ),
    (
        (0, 0, 0, 3, 4, 6, 2, 0), (0, 0, 1, 3, 4, 6, 2, 0), (0, 1, 0, 3, 4, 2, 0, 6), (0, 1, 1, 3, 4, 2, 0, 6),
        (0, 0, 0, 0, 4), (0, 0, 1, 0, 4), (0, 1, 0, 0, 4), (3, 14), (3, 13), (0, 0, 0, 8, 6, 2), (0, 1, 1, 0, 4),
        (2, 0), (0, 0, 1, 8, 6, 2), (0, 0, 1, 12, 2, 14, 13, 4), (2, 1), (0, 1, 0, 8, 2, 6),
        (0, 0, 0, 12, 2, 14, 13, 4), (0, 1, 1, 8, 2, 6), (0, 1, 1, 12, 2, 14, 13, 4), (0, 1, 0, 12, 2, 14, 13, 4),
        (2, 2), (2, 3), (2, 4),
    ),
    (
        (0, 0, 0, 4, 6, 1), (0, 0, 1, 4, 6, 1), (0, 0, 0, 2, 7, 6, 5, 3), (0, 0, 1, 2, 7, 6, 5, 3),
        (0, 1, 0, 4, 1, 6), (0, 1, 1, 4, 1, 6), (0, 1, 0, 2, 5, 3, 6, 7), (0, 1, 1, 2, 5, 3, 6, 7), (3, 15), (3, 14),
        (0, 0, 1, 9, 3, 5, 2, 6), (0, 0, 0, 9, 3, 5, 2, 6), (0, 0, 1, 15, 5, 7), (2, 0), (0, 0, 0, 15, 5, 7),
        (0, 1, 1, 9, 5, 6, 2, 3), (0, 0, 1, 14, 7, 6, 3), (0, 1, 0, 9, 5, 6, 2, 3), (2, 1), (0, 0, 0, 14, 7, 6, 3),
        (0, 0, 1, 13, 6, 3, 5), (0, 0, 0, 13, 6, 3, 5), (0, 1, 1, 15, 7, 5), (0, 1, 0, 15, 7, 5),
        (0, 1, 1, 14, 6, 7, 3), (0, 0, 0, 5, 15, 14, 6), (0, 1, 0, 14, 6, 7, 3), (0, 1, 1, 13, 3, 5, 6),
        (0, 1, 0, 13, 3, 5, 6), (0, 0, 1, 5, 15, 14, 6), (2, 2), (0, 1, 0, 5, 15, 14, 6), (2, 3),
        (0, 1, 1, 5, 15, 14, 6), (2, 4),
    ),
    (
        (0, 0, 0, 5, 2), (0, 0, 1, 5, 2), (0, 0, 0, 1, 4, 7), (0, 1, 0, 5, 2), (0, 1, 1, 5, 2), (0, 0, 1, 7, 4, 3, 6),
        (0, 0, 1, 1, 4, 7), (0, 0, 0, 7, 4, 3, 6), (3, 8), (1, 0, 0, 5, 8), (1, 0, 1, 5, 8), (1, 1, 0, 5, 8),
        (1, 1, 1, 5, 8), (3, 10), (1, 0, 0, 1, 10), (1, 0, 1, 1, 10), (0, 1, 1, 7, 3, 4, 6), (0, 1, 0, 1, 4, 7, 10),
        (0, 1, 0, 7, 3, 4, 6), (0, 1, 1, 1, 4, 7, 10), (2, 0), (0, 0, 1, 10, 3, 4, 2), (0, 0, 0, 10, 3, 4, 2),
        (0, 1, 1, 10, 4, 2, 3), (0, 1, 0, 10, 4, 2, 3), (2, 1), (2, 2), (2, 3), (2, 4),
    ),
    (
        (0, 0, 1, 6, 5, 2, 7), (0, 0, 0, 6, 5, 2, 7), (0, 0, 0, 3, 7), (0, 0, 0, 4, 7, 5), (0, 0, 1, 4, 7, 5),
        (0, 0, 1, 3, 7), (0, 1, 1, 6, 5, 2, 7), (0, 1, 0, 6, 5, 2, 7), (3, 9), (1, 0, 0, 4, 9), (1, 0, 1, 4, 9),
        (3, 8), (1, 0, 0, 3, 8), (1, 0, 1, 3, 8), (0, 1, 0, 3, 7, 8), (0, 1, 0, 4, 5, 7, 9), (0, 1, 1, 4, 5, 7, 9),
        (0, 0, 1, 10, 7, 5), (0, 0, 0, 10, 7, 5), (0, 1, 1, 3, 7, 8), (0, 0, 1, 11, 5, 4, 8), (0, 0, 0, 11, 5, 4, 8),
        (0, 1, 1, 10, 7, 5), (0, 1, 0, 10, 7, 5), (2, 0), (0, 1, 1, 11, 8, 4, 5), (0, 0, 0, 8, 5, 4, 7),
        (0, 0, 1, 8, 5, 4, 7), (0, 1, 0, 11, 8, 4, 5), (2, 1), (0, 1, 0, 8, 4, 5, 7), (0, 0, 1, 13, 9, 8, 7),
        (0, 0, 0, 13, 9, 8, 7), (0, 1, 1, 8, 4, 5, 7), (2, 2), (0, 1, 1, 13, 9, 8, 7), (0, 1, 0, 13, 9, 8, 7), (2, 3),
        (2, 4),
    ),
    (
        (0, 0, 1, 7, 5, 2), (0, 0, 0, 7, 5, 2), (0, 0, 1, 6, 3), (0, 0, 0, 6, 3), (0, 1, 1, 7, 5, 2), (3, 9),
        (1, 0, 1, 6, 9), (1, 0, 0, 6, 9), (0, 1, 0, 7, 5, 2), (3, 8), (1, 0, 1, 7, 8), (1, 0, 0, 7, 8),
        (1, 0, 1, 6, 8), (1, 0, 0, 6, 8), (1, 1, 1, 7, 8), (1, 1, 0, 7, 8), (3, 10), (1, 0, 1, 7, 10),
        (1, 0, 0, 7, 10), (1, 1, 1, 7, 10), (1, 1, 0, 7, 10), (0, 1, 1, 6, 8, 3, 9), (0, 1, 0, 6, 8, 3, 9), (2, 0),
        (2, 1), (0, 0, 1, 15, 9, 10, 8, 6), (0, 0, 0, 15, 9, 10, 8, 6), (0, 1, 1, 15, 9, 6, 10, 8),
        (0, 1, 0, 15, 9, 6, 10, 8), (2, 2), (2, 3), (2, 4),
    ),
    (
        (0, 0, 0, 8, 9, 12, 10, 3, 11), (0, 0, 1, 8, 9, 12, 10, 3, 11), (0, 1, 0, 8, 9, 11, 3, 12, 10),
        (0, 1, 1, 8, 9, 11, 3, 12, 10), (0, 0, 0, 3, 10, 13, 5, 9), (2, 0), (0, 0, 1, 3, 10, 13, 5, 9),
        (0, 0, 0, 5, 11, 4, 9, 7), (0, 0, 1, 5, 11, 4, 9, 7), (0, 1, 0, 5, 7, 11, 9, 4), (0, 1, 0, 3, 13, 9, 5, 10),
        (0, 1, 1, 5, 7, 11, 9, 4), (0, 1, 1, 3, 13, 9, 5, 10), (2, 1), (0, 0, 0, 0, 6, 7, 9), (0, 0, 1, 0, 6, 7, 9),
        (0, 1, 0, 0, 9, 7, 6), (0, 1, 1, 0, 9, 7, 6), (2, 2), (2, 3), (2, 4),
    ),
    (
        (0, 0, 1, 9, 7, 8, 10, 4, 12), (0, 0, 0, 9, 7, 8, 10, 4, 12), (0, 1, 1, 9, 4, 7, 8, 12, 10),
        (0, 1, 0, 9, 4, 7, 8, 12, 10), (0, 0, 1, 12, 7, 6, 5, 8), (0, 0, 0, 12, 7, 6, 5, 8), (0, 0, 0, 4, 8, 10, 12),
        (2, 0), (0, 0, 1, 4, 8, 10, 12), (0, 1, 1, 12, 5, 8, 6, 7), (0, 1, 0, 12, 5, 8, 6, 7),
        (0, 1, 0, 4, 12, 10, 8), (0, 1, 1, 4, 12, 10, 8), (2, 1), (0, 0, 0, 2, 11, 10, 8, 12),
        (0, 0, 1, 2, 11, 10, 8, 12), (0, 1, 0, 2, 11, 8, 12, 10), (0, 1, 1, 2, 11, 8, 12, 10), (2, 2), (2, 3), (2, 4),
    ),
    (
        (0, 0, 1, 10, 12, 9, 6, 0, 11, 8), (0, 0, 0, 10, 12, 9, 6, 0, 11, 8), (0, 1, 1, 10, 6, 11, 8, 0, 12, 9),
        (0, 1, 0, 10, 6, 11, 8, 0, 12, 9), (0, 0, 1, 7, 13, 9), (0, 0, 1, 14, 9, 12, 11, 5), (2, 0),
        (0, 0, 0, 7, 13, 9), (0, 1, 1, 7, 13, 9), (0, 0, 0, 14, 9, 12, 11, 5), (0, 1, 0, 7, 13, 9),
        (0, 1, 1, 14, 9, 12, 11, 5), (0, 1, 0, 14, 9, 12, 11, 5), (2, 1), (0, 0, 0, 1, 12, 8, 9, 11),
        (0, 0, 1, 1, 12, 8, 9, 11), (0, 1, 0, 1, 9, 12, 8, 11), (0, 1, 1, 1, 9, 12, 8, 11), (2, 2), (2, 3), (2, 4),
    ),
    (
        (0, 0, 1, 11, 6, 9, 0, 10, 12, 7), (0, 0, 0, 11, 6, 9, 0, 10, 12, 7), (0, 1, 1, 11, 6, 12, 9, 10, 7, 0),
        (0, 1, 0, 11, 6, 12, 9, 10, 7, 0), (2, 0), (0, 0, 0, 5, 13, 12, 10), (2, 1), (0, 0, 1, 5, 13, 12, 10),
        (0, 1, 0, 5, 13, 10, 12), (0, 1, 1, 5, 13, 10, 12), (2, 2), (2, 3), (2, 4),
    ),
    (
        (0, 0, 1, 12, 10, 0, 11, 9), (0, 0, 0, 12, 10, 0, 11, 9), (0, 1, 1, 12, 10, 9, 0, 11), (0, 0, 1, 9, 11, 15),
        (0, 1, 0, 12, 10, 9, 0, 11), (0, 0, 0, 9, 11, 15), (0, 0, 0, 8, 14, 0, 13), (0, 0, 1, 8, 14, 0, 13),
        (0, 1, 1, 9, 11, 15), (2, 0), (0, 1, 0, 9, 11, 15), (0, 1, 0, 8, 0, 14, 13), (0, 1, 1, 8, 0, 14, 13),
        (0, 0, 0, 0, 14, 10, 15, 11), (0, 0, 1, 0, 14, 10, 15, 11), (0, 0, 0, 4, 13, 11, 15, 14),
        (0, 0, 1, 4, 13, 11, 15, 14), (0, 1, 0, 0, 11, 15, 10, 14), (0, 1, 1, 0, 11, 15, 10, 14), (2, 1),
        (0, 1, 0, 4, 11, 14, 13, 15), (0, 1, 1, 4, 11, 14, 13, 15), (2, 2), (2, 3), (2, 4),
    ),
    (
        (0, 0, 1, 13, 11, 12, 0, 14, 10), (0, 0, 0, 13, 11, 12, 0, 14, 10), (0, 1, 1, 13, 0, 12, 11, 14, 10),
        (0, 1, 0, 13, 0, 12, 11, 14, 10), (0, 0, 0, 0, 12, 8), (0, 0, 1, 7, 12, 14, 15, 11), (0, 0, 1, 0, 12, 8),
        (0, 1, 0, 0, 12, 8), (0, 1, 1, 0, 12, 8), (2, 0), (0, 0, 0, 7, 12, 14, 15, 11), (0, 1, 1, 7, 11, 12, 15, 14),
        (0, 1, 0, 7, 11, 12, 15, 14), (0, 0, 0, 3, 11, 14, 12, 15), (2, 1), (0, 0, 1, 3, 11, 14, 12, 15),
        (0, 0, 1, 6, 12), (0, 0, 0, 6, 12), (0, 1, 1, 6, 12), (0, 1, 0, 6, 12), (2, 2), (0, 1, 0, 3, 15, 14, 11, 12),
        (0, 1, 1, 3, 15, 14, 11, 12), (2, 3), (2, 4),
    ),
    (
        (0, 0, 1, 14, 8, 10, 15, 13, 2), (0, 0, 0, 14, 8, 10, 15, 13, 2), (0, 1, 1, 14, 10, 8, 15, 2, 13),
        (0, 1, 0, 14, 10, 8, 15, 2, 13), (0, 0, 0, 2, 9, 13, 15), (0, 0, 1, 2, 9, 13, 15), (0, 0, 0, 1, 15),
        (0, 0, 1, 1, 15), (0, 1, 0, 2, 15, 9, 13), (0, 1, 1, 2, 15, 9, 13), (2, 0), (0, 0, 1, 6, 13, 10, 15, 11),
        (0, 1, 0, 1, 15), (0, 0, 0, 6, 13, 10, 15, 11), (0, 1, 1, 1, 15), (0, 1, 1, 6, 10, 13, 11, 15),
        (0, 1, 0, 6, 10, 13, 11, 15), (2, 1), (2, 2), (2, 3), (2, 4),
    ),
    (
        (0, 0, 1, 15, 12, 11, 14, 2, 13), (0, 0, 0, 15, 12, 11, 14, 2, 13), (0, 1, 1, 15, 2, 14, 11, 13, 12),
        (0, 1, 0, 15, 2, 14, 11, 13, 12), (0, 0, 1, 9, 14, 0, 13, 1), (0, 0, 0, 9, 14, 0, 13, 1),
        (0, 0, 1, 11, 14, 13), (0, 0, 0, 11, 14, 13), (0, 0, 1, 10, 14, 13), (0, 0, 0, 10, 14, 13),
        (0, 1, 1, 9, 1, 0, 14, 13), (0, 1, 0, 9, 1, 0, 14, 13), (2, 0), (0, 1, 1, 11, 13, 14), (0, 1, 0, 11, 13, 14),
        (0, 1, 1, 10, 13, 14), (2, 1), (0, 1, 0, 10, 13, 14), (2, 2), (2, 3), (2, 4),
    ),
)

ASIDE = (
    (),
    (),
    (),
    (),
    (),
    (),
    (),
    (),
    (),
    (),
    (),
    (),
    (),
    (),
    (),
    (),
)

SLOT = [{source: i for i, source in enumerate(order)} for order in ORDER]
RELAYS = [[tuple(step[1:4]) for step in route if step[0] == 0 and step[3] != z] for z, route in enumerate(ROUTES)]
BOUNDS = (0, 4, 8, 12, 14, 16)
PART = [sum(slot >= bound for bound in BOUNDS[1:]) for slot in range(16)]
RSEMS = 10 + max(map(len, RELAYS))


def leaves(z, p):
    return [
        (wave, core, source)
        for source in ORDER[z][BOUNDS[p] : BOUNDS[p + 1]]
        for wave in range(2)
        for core in range(2)
        if source != z and (wave, core, source) not in RELAYS[z]
    ]


RING = (
    ("q_begin",), ("q_own",),
    ("q_relay", -1, 0, 0), ("q_relay", 1, 0, 0), ("q_relay", -1, 0, 1), ("q_relay", 1, 0, 1),
    ("k_own",),
    ("q_relay", -2, 0, 0), ("q_relay", 2, 0, 0), ("q_relay", -1, 1, 0), ("q_relay", 1, 1, 0),
    ("q_relay", -2, 0, 1), ("q_relay", 2, 0, 1), ("q_relay", -1, 1, 1), ("q_relay", 1, 1, 1),
    ("k_relay", -1), ("k_relay", 1),
    ("q_relay", -3, 0, 0), ("q_relay", 3, 0, 0), ("q_relay", -2, 1, 0), ("q_relay", 2, 1, 0),
    ("q_relay", -3, 0, 1), ("q_relay", 3, 0, 1), ("q_relay", -2, 1, 1), ("q_relay", 2, 1, 1),
    ("k_relay", -2), ("k_relay", 2),
    ("q_relay", -3, 1, 0), ("q_relay", 3, 1, 0), ("q_relay", -3, 1, 1), ("q_relay", 3, 1, 1),
    ("k_relay", -3), ("k_relay", 3),
)

LATE_RING = (
    ("q_begin",), ("q_own_first",),
    ("q_relay", -1, 1, 0), ("q_relay", 1, 1, 0), ("q_relay", -1, 1, 1), ("q_relay", 1, 1, 1),
    ("q_relay", -2, 1, 0), ("q_relay", 2, 1, 0), ("q_relay", -2, 1, 1), ("q_relay", 2, 1, 1),
    ("q_relay", -3, 1, 0), ("q_relay", 3, 1, 0), ("q_relay", -3, 1, 1), ("q_relay", 3, 1, 1),
    ("q_own_last",), ("k_own",),
    ("q_relay", -1, 0, 0), ("q_relay", 1, 0, 0), ("q_relay", -1, 0, 1), ("q_relay", 1, 0, 1),
    ("k_relay", -1), ("k_relay", 1),
    ("q_relay", -2, 0, 0), ("q_relay", 2, 0, 0), ("q_relay", -2, 0, 1), ("q_relay", 2, 0, 1),
    ("k_relay", -2), ("k_relay", 2),
    ("q_relay", -3, 0, 0), ("q_relay", 3, 0, 0), ("q_relay", -3, 0, 1), ("q_relay", 3, 0, 1),
    ("k_relay", -3), ("k_relay", 3),
)

PLAN_Q = (
    ("ring",),
    ("attend", 2), ("attend", 1), ("attend", 3),
    ("w_passed", 0), ("piece", 0, 1),
    ("q_last",), ("k_last",), ("attend", 0), ("piece", 0, 0),
    ("w_passed", 1), ("piece", 1, 2),
    ("reduced", 0, 2), ("reduced", 0, 1), ("reduced", 0, 3), ("reduced", 0, 0),
    ("reduced", 1, 2), ("reduced", 1, 1), ("reduced", 1, 3), ("reduced", 1, 0),
)

PLAN_W = (
    ("w_begin",), ("w_route", 0),
    ("w_rest",), ("w_route", 1), ("w_piece", 3, 0, 2), ("w_route", 2), ("w_piece", 3, 2, 2),
    ("reduced", 2, 0), ("reduced", 2, 1), ("reduced", 2, 3), ("reduced", 2, 2),
    ("reduced", 3, 0), ("reduced", 3, 1), ("reduced", 3, 3), ("reduced", 3, 2),
)


def by_place(z, do, low=0, high=16):
    if high - low == 1:
        do(low)
        return
    middle = (low + high) // 2
    pl.when(z < middle)(lambda: by_place(z, do, low, middle))
    pl.when(z >= middle)(lambda: by_place(z, do, middle, high))


def kernel(
    q, k, v, w, sums,
    qall, kvl, kvr, wv, wt, wcross, wall, bias, att, psend, xr, ssend, rbuf, size,
    lsem, ssem, rsem, wpsem, atsem, xsem, asem, go, late,
):
    yl, z, x, yh, c = (lax.axis_index(a) for a in ("yl", "z", "x", "yh", "c"))
    y = yh * 4 + yl

    def dev(dy=0, dz=0, dx=0, to_z=None, role=None):
        yt = lax.rem(y + (dy + 8), 8)
        zt = lax.rem(z + (dz + 16), 16) if to_z is None else to_z
        xt = lax.rem(x + dx, 4)
        core = role if to_z else jnp.where(xt + yt + zt == 0, 1 - role, role)
        return (lax.rem(yt, 4), zt, xt, lax.div(yt, 4), core)

    origin = x + y + z == 0
    for_q = jnp.where(origin, 1 - QC, QC) == c
    one_more = jnp.where(origin, 0, 1)

    def remote(src, dst, send_sem, recv_sem, to):
        return pltpu.make_async_remote_copy(
            src_ref=src, dst_ref=dst, send_sem=send_sem, recv_sem=recv_sem, device_id=to, device_id_type=MESH
        )

    sent = [0]

    def send(src, dst, recv_sem, to):
        remote(src, dst, ssem.at[0], recv_sem, to).start()
        sent[0] += math.prod(src.shape) * 2

    def received(dst, recv_sem):
        remote(dst, dst, ssem.at[0], recv_sem, (yl, z, x, yh, 1 - c)).wait_recv()

    def sized(bytes_):
        assert bytes_ % 8192 == 0 and bytes_ // 8192 <= size.shape[0]
        return size.at[pl.ds(0, bytes_ // 8192)]

    def half_of(r):
        return lax.div(lax.rem(y + (r + 8), 8), 4)

    w_load = pltpu.make_async_copy(w, wv, lsem.at[0])
    q_load = pltpu.make_async_copy(q, qall.at[0, yh, c], lsem.at[1])
    kv_load = [pltpu.make_async_copy(k, kvl.at[0], lsem.at[2]), pltpu.make_async_copy(v, kvl.at[1], lsem.at[2])]
    barrier = pltpu.get_barrier_semaphore()
    around_q = [dict(dy=1), dict(dy=-1), dict(dx=1), dict(dx=2), dict(dx=3)]

    w_load.start()
    for copy in kv_load:
        copy.start()
    q_load.start()

    @pl.when(for_q)
    def _():
        for peer in around_q:
            pl.semaphore_signal(barrier, inc=1, device_id=dev(role=QC, **peer), device_id_type=MESH)

    @pl.when(~for_q)
    def _():
        pl.semaphore_signal(barrier, inc=1, device_id=dev(dy=4, role=WC), device_id_type=MESH)

        @pl.when(~origin)
        def _():
            pl.semaphore_signal(barrier, inc=1, device_id=dev(role=QC), device_id_type=MESH)

        def greet(place):
            for other in range(16):
                if place in FIRST[other]:
                    pl.semaphore_signal(barrier, inc=1, device_id=dev(to_z=other, role=WC), device_id_type=MESH)
                if place in ASIDE[other]:
                    to = dev(dy=4, to_z=other, role=WC)
                    pl.semaphore_signal(barrier, inc=1, device_id=to, device_id_type=MESH)

        by_place(z, greet)

    w_load.wait()
    wt[...] = wv[...].astype(F32).T.astype(BF16).reshape(2, 64, 256)
    for copy in kv_load:
        copy.wait()

    def lanes_of(half, core):
        return pl.ds(pl.multiple_of((half * 2 + core) * 256, 256), 256)

    def head_of(i):
        return pl.ds(pl.multiple_of(i * 128, 128), 128)

    def unit(slot, wave, core):
        return wall.at[slot, :, lanes_of(1 - yh if wave else yh, core)]

    def w_sem(place, wave, core, source):
        if (wave, core, source) in RELAYS[place]:
            return rsem.at[10 + RELAYS[place].index((wave, core, source))]
        return rsem.at[5 + PART[SLOT[place][source]]]

    def w_sends(place, wave, core, source, targets):
        for t in targets:
            here, there = SLOT[place][source], SLOT[t][source]
            to = dev(to_z=t, role=WC)
            send(unit(here, wave, core), unit(there, wave, core), w_sem(t, wave, core, source), to)

    def w_cross(place, core):
        for t in ASIDE[place]:
            there = wall.at[SLOT[t][place], :, lanes_of(yh, core)]
            send(wcross.at[core], there, w_sem(t, 1, core, place), dev(dy=4, to_z=t, role=WC))
        send(wcross.at[core], wall.at[0, :, lanes_of(yh, core)], rsem.at[2 + core], dev(dy=4, role=WC))

    waited = []

    def w_step(place, kind, *step):
        if kind == 3:
            pl.semaphore_wait(late.at[step[0] - 8], 1)
            return
        if kind == 2:
            p = step[0]
            if leaves(place, p):
                received(sized(len(leaves(place, p)) * 32768), rsem.at[5 + p])
            if p < 2:
                rows = pl.ds(4 * p, 4)
                send(wall.at[rows], wall.at[rows], wpsem.at[p], dev(role=QC))
            return
        wave, core, source, *targets = step
        if kind == 0:
            if source != place:
                received(unit(SLOT[place][source], wave, core), w_sem(place, wave, core, source))
            elif wave:
                received(unit(0, 1, core), rsem.at[2 + core])
            else:
                if (core == QC or place == 0) and place not in waited:
                    received(sized(65536), rsem.at[4])
                    waited.append(place)
                w_cross(place, core)
        w_sends(place, wave, core, source, targets)

    def w_rows():
        for gs in (2, 1, 3, 0):
            a_got(gs)
        w_piece(2, 0, 4)

    def w_rest():
        before = sent[0]
        pl.when(z > 0)(w_rows)
        sent[0] = before

    def w_route(part):
        totals = []

        def go_on(place):
            route = ROUTES[place]
            first = 1 + max(i for i, step in enumerate(route) if step[0] != 2 or step[1] == 2)
            cuts = (0, first, max(first, 1 + route.index((2, 3))), len(route))
            start = sent[0]
            for step in route[cuts[part] : cuts[part + 1]]:
                with jax.named_scope("_".join(map(str, ("at", place, *step)))):
                    w_step(place, *step)
                if place == 0 and step == (2, 2):
                    extra = sent[0]
                    w_rows()
                    w_extra.append(sent[0] - extra)
                    sent[0] = extra
            totals.append(sent[0] - start)
            sent[0] = start

        by_place(z, go_on)
        w_totals.append(totals)

    w_totals, w_extra = [], []

    def w_passed(p):
        received(wall.at[pl.ds(4 * p, 4)], wpsem.at[p])

    def q_part(r, s, u):
        return qall.at[r % 4, half_of(r), s, pl.ds(128 * u, 128)]

    def q_sem(t, s, u):
        return rsem.at[0 if t == 4 else 8 + 4 * (t if t < 4 else t - 1) + 2 * s + u]

    def q_send(r, s, u, hop):
        t = (r - hop) % 8
        rows = pl.ds(128 * u, 128)
        dst = qall.at[t % 4, half_of(r), s, rows]
        send(q_part(r, s, u), dst, q_sem(t, s, u), dev(dy=hop, role=QC))

    def q_relay(r, s, u):
        received(q_part(r, s, u), q_sem(r % 8, s, u))
        if abs(r) < 3 or s == (0 if r < 0 else 1):
            q_send(r, s, u, 1 if r < 0 else -1)

    def q_last():
        received(qall.at[0, half_of(4)], rsem.at[0])

    def k_send(r, hop):
        t = (r - hop) % 8
        some = pl.ds(0 if hop > 0 else 2, 2) if t == 4 else pl.ds(0, 4)
        src, dst = kvr.at[r % 4, half_of(r), some], kvr.at[t % 4, half_of(r), some]
        send(src, dst, rsem.at[t if t else 8], dev(dy=hop, role=QC))

    def k_relay(r):
        received(kvr.at[r % 4, half_of(r)], rsem.at[r % 8])
        k_send(r, 1 if r < 0 else -1)

    def k_last():
        received(kvr.at[0, half_of(4)], rsem.at[4])

    def k_spread():
        for d in (2, 1, 3):
            head = head_of(lax.rem(x + d, 4))
            send(kvl.at[:, :, head], kvr.at[0, yh, x, :, c], rsem.at[8], dev(dx=d, role=QC))

    def k_own():
        received(sized(7 * 8192), rsem.at[8])
        k_send(0, 1)
        k_send(0, -1)

    def ring():
        before = sent[0]
        for late, plan in ((False, RING), (True, LATE_RING)):
            sent[0] = before

            def go_round(plan=plan):
                for step in plan:
                    do(*step)

            pl.when((x + z == 0) if late else (x + z > 0))(go_round)

    def q_own_first():
        once(~origin, None, q_own)

    def q_own_last():
        before = sent[0]
        pl.when(origin)(q_own)
        sent[0] = before

    def w_hand():
        send(wt.at[yh], unit(0, 0, c), rsem.at[4], dev(role=WC))
        send(wt.at[1 - yh], wcross.at[c], rsem.at[4], dev(role=WC))

    def once(first, second, do):
        before = sent[0]
        pl.when(second if first is None else first)(do)
        if first is None:
            sent[0] = before

    def q_own():
        received(qall.at[0, yh, 1 - c], rsem.at[9])
        for u in range(2):
            for hop in (1, -1):
                q_send(0, 1 - c, u, hop)
        before = sent[0]
        pl.when(origin)(w_hand)
        sent[0] = before

    def q_begin():
        pl.semaphore_wait(barrier, len(around_q) + one_more)

        def meet():
            pl.semaphore_signal(go, inc=1, device_id=dev(role=WC), device_id_type=MESH)
            w_hand()

        once(~origin, None, meet)

        @pl.when(origin)
        def _():
            pl.semaphore_signal(barrier, inc=1, device_id=dev(role=WC), device_id_type=MESH)

        k_spread()
        kvr[0, yh, x, :, c] = kvl[:, :, head_of(x)]
        q_load.wait()
        for u in range(2):
            for hop in (1, -1):
                q_send(0, c, u, hop)
        row = lax.broadcasted_iota(jnp.int32, (128, 128), 0)
        col = lax.broadcasted_iota(jnp.int32, (128, 128), 1)
        bias[...] = jnp.where((lax.div(row, 32) == lax.div(col, 32)) & (col <= row), 0.0, -1e30)

    def w_begin():
        wall[0, :, lanes_of(yh, c)] = wt[yh]
        wcross[c] = wt[1 - yh]
        q_load.wait()

        def give():
            send(qall.at[0, yh, c], qall.at[0, yh, c], rsem.at[9], dev(role=QC))
            k_spread()
            send(kvl.at[:, :, head_of(x)], kvr.at[0, yh, x, :, c], rsem.at[8], dev(role=QC))

        def meet():
            pl.semaphore_wait(go, 1)
            give()

        once(~origin, None, meet)

        def greeted(place):
            pl.semaphore_wait(barrier, 2 + len(FIRST[place]) + len(ASIDE[place]) - one_more)
            for other in range(16):
                if (3, place) in ROUTES[other]:
                    to = dev(to_z=other, role=WC)
                    pl.semaphore_signal(late.at[place - 8], inc=1, device_id=to, device_id_type=MESH)

        by_place(z, greeted)
        once(None, origin, give)

    def attend(gs):
        for t in range(2):
            pair = kvr[gs, t]
            keys, values = pair[:, 0].reshape(128, 128), pair[:, 1].reshape(128, 128)
            values = jnp.concatenate([values, jnp.ones((128, 128), BF16)], axis=1)
            for h in range(2):
                queries = jnp.concatenate(
                    [
                        qall[gs, h, s, :, j * 128 : j * 128 + 128].reshape(4, 2, 32, 128)[:, t].reshape(128, 128)
                        for s in range(2)
                        for j in range(2)
                    ],
                    axis=0,
                )
                scores = lax.dot_general(queries, keys, NT, preferred_element_type=F32)
                scores = scores * (1.0 / math.sqrt(128.0)) + jnp.concatenate([bias[...]] * 4, axis=0)
                powers = jnp.exp(scores - jnp.max(scores, axis=-1, keepdims=True)).astype(BF16)
                total = jnp.dot(powers, values, preferred_element_type=F32)
                heads = (total[:, :128] / total[:, 128:]).astype(BF16)
                for i in range(4):
                    att[gs, t, :, h * 512 + i * 128 : h * 512 + i * 128 + 128] = heads[i * 128 : i * 128 + 128]
        send(att.at[gs], att.at[gs], atsem.at[gs], dev(role=WC))

    def a_got(gs):
        received(att.at[gs], atsem.at[gs])

    def spread(p, gs, lanes):
        for d in (2, 1, 3):
            src = psend.at[p % 2, gs, :, lax.rem(x + d, 4), :, lanes]
            dst = xr.at[p % 2, gs, d - 1, :, :, lanes]
            send(src, dst, xsem.at[p % 2, gs], dev(dx=d, role=QC if p < 2 else WC))

    def piece(p, which):
        groups = (slice(0, 1), slice(1, 4), slice(0, 4))[which]
        n = groups.stop - groups.start
        rows = wall[4 * p : 4 * p + 4].reshape(256, 1024)
        total = lax.dot_general(att[groups].reshape(n * 256, 1024), rows, NT, preferred_element_type=F32)
        psend[p, groups] = total.astype(BF16).reshape(n, 2, 4, 32, 256)
        for gs in ((0,), (2, 1, 3), (2, 1, 3, 0))[which]:
            spread(p, gs, pl.ds(0, 256))

    def w_piece(p, slot, n):
        slots = slice(4 * p + slot, 4 * p + slot + n)
        rows = wall[slots].reshape(64 * n, 1024)
        total = lax.dot_general(att[...].reshape(1024, 1024), rows, NT, preferred_element_type=F32)
        lanes = slice(64 * slot, 64 * (slot + n))
        psend[p - 2, :, :, :, :, lanes] = total.astype(BF16).reshape(4, 2, 4, 32, 64 * n)
        for gs in (0, 1, 3, 2):
            spread(p, gs, pl.ds(64 * slot, 64 * n))

    def reduced(p, gs):
        received(xr.at[p % 2, gs], xsem.at[p % 2, gs])
        total = psend[p % 2, gs, :, x].astype(F32)
        for d in range(3):
            total = total + xr[p % 2, gs, d].astype(F32)
        ssend[p % 2, gs] = total.astype(BF16).reshape(2, 2, 16, 256)
        for other in (1, 0):
            half = 1 - yh if other else yh
            there = half * 4 + lax.rem(yl + gs, 4)
            place = lax.rem(y + 8 - there, 8)
            for core in (1 - c, c):
                home = (lax.rem(yl + gs, 4), z, x, half, core)
                if gs or other:
                    send(ssend.at[p % 2, gs, half, core], rbuf.at[p, place], asem.at[p], home)
                elif core is c:
                    rbuf[p, 0] = ssend[p % 2, 0, yh, c]
                else:
                    send(ssend.at[p % 2, 0, yh, core], rbuf.at[p, 0], asem.at[4 + p % 2], home)

    steps = dict(
        q_begin=q_begin, w_begin=w_begin, q_own=q_own, q_relay=q_relay, q_last=q_last, k_own=k_own, k_relay=k_relay,
        k_last=k_last, attend=attend, w_route=w_route, w_passed=w_passed, a_got=a_got, piece=piece, w_piece=w_piece, w_rest=w_rest, reduced=reduced,
        ring=ring, q_own_first=q_own_first, q_own_last=q_own_last,
    )

    def do(name, *numbers):
        with jax.named_scope("_".join(map(str, (name, *numbers)))):
            steps[name](*numbers)

    def follow(plan):
        sent[0] = 0
        for step in plan:
            do(*step)

    def drain(bytes_):
        stand_in = sized(bytes_)
        remote(stand_in, stand_in, ssem.at[0], ssem.at[0], (yl, z, x, yh, 1 - c)).wait_send()

    def arrive(mine):
        with jax.named_scope("arrive"):
            outs = []
            for p in range(PIECES):
                received(rbuf.at[p, pl.ds(1, 7)], asem.at[p])
                if p // 2 != mine:
                    received(rbuf.at[p, 0], asem.at[4 + p % 2])
                outs.append(pltpu.make_async_copy(rbuf.at[p], sums.at[p], lsem.at[3 + p]))
                outs[-1].start()
            if mine:
                by_place(z, lambda place: drain(sent[0] + w_extra[0] + sum(totals[place] for totals in w_totals)))
            else:
                drain(sent[0])
            for copy in outs:
                copy.wait()

    @pl.when(for_q)
    def _():
        follow(PLAN_Q)
        arrive(0)

    @pl.when(~for_q)
    def _():
        follow(PLAN_W)
        arrive(1)


def last_kernel(sums, res, gain, hid, nrm, rbuf, resv, gv, u, hidv, nrmv, sem):
    yl, z, yh = (lax.axis_index(a) for a in ("yl", "z", "yh"))
    y = yh * 4 + yl
    loads = [
        pltpu.make_async_copy(res, resv, sem.at[0]),
        pltpu.make_async_copy(gain, gv, sem.at[0]),
    ]
    loads += [pltpu.make_async_copy(sums.at[p], rbuf.at[p], sem.at[1 + p]) for p in range(PIECES)]
    for copy in loads:
        copy.start()

    def source_of(slot):
        low, high = (
            sum(ORDER[8 * part + i][slot] << (4 * i) for i in range(8)) for part in range(2)
        )
        low, high = (n - (1 << 32) if n >> 31 else n for n in (low, high))
        word = jnp.where(z < 8, jnp.int32(low), jnp.int32(high))
        return lax.shift_right_logical(word, 4 * lax.rem(z, 8)) & 15

    for copy in loads[:2]:
        copy.wait()
    squares = jnp.zeros((16, 128), F32)
    low = lax.broadcasted_iota(jnp.int32, (16, 128), 1) < 64
    for p in range(PIECES):
        sources = [source_of(4 * p + i) for i in range(4)]
        loads[2 + p].wait()
        for r in range(4):
            here = lax.div(lax.rem(y + r, 8), 4)
            first, second = r + 4 * here, r + 4 - 4 * here
            for t in range(2):
                lanes = slice(t * 128, t * 128 + 128)
                a = rbuf[p, first, :, lanes].astype(F32)
                b = rbuf[p, second, :, lanes].astype(F32)
                pair = (jnp.where(low, a, pltpu.roll(b, 64, 1)), jnp.where(low, pltpu.roll(a, 64, 1), b))
                for i in range(2):
                    block = lax.rem(yl + r, 4) * 16 + sources[2 * t + i]
                    at = pl.ds(pl.multiple_of(block * 128, 128), 128)
                    updated = resv[:, at].astype(F32) + pair[i]
                    u[:, at] = updated
                    hidv[:, at] = updated.astype(BF16)
                    squares = squares + updated * updated
    stores = [pltpu.make_async_copy(hidv, hid, sem.at[5])]
    stores[0].start()
    scale = lax.rsqrt(jnp.sum(squares, axis=-1, keepdims=True) * (1.0 / 8192.0) + 1e-05)
    for part in range(2):
        for block in range(32 * part, 32 * part + 32):
            lanes = slice(block * 128, block * 128 + 128)
            nrmv[:, lanes] = (u[:, lanes] * scale * gv[block : block + 1, :]).astype(BF16)
        lanes = pl.ds(4096 * part, 4096)
        stores.append(pltpu.make_async_copy(nrmv.at[:, lanes], nrm.at[:, lanes], sem.at[6 + part]))
        stores[-1].start()
    for copy in stores:
        copy.wait()


def local(queries, keys, values, out_weight, residual, norm_gain):
    in_hbm = pl.BlockSpec(memory_space=pltpu.HBM)
    vmem = pltpu.VMEM
    dma = pltpu.SemaphoreType.DMA
    sums = pl.pallas_call(
        kernel,
        out_shape=jax.ShapeDtypeStruct((PIECES, 8, 16, 256), BF16),
        in_specs=[in_hbm] * 4,
        out_specs=in_hbm,
        scratch_shapes=[
            vmem((4, 2, 2, 256, 256), BF16),
            vmem((2, 16, 512), BF16),
            vmem((4, 2, 4, 2, 2, 16, 128), BF16),
            vmem((256, 128), BF16),
            vmem((2, 64, 256), BF16),
            vmem((2, 64, 256), BF16),
            vmem((16, 64, 1024), BF16),
            vmem((128, 128), F32),
            vmem((4, 2, 128, 1024), BF16),
            vmem((2, 4, 2, 4, 32, 256), BF16),
            vmem((2, 4, 3, 2, 32, 256), BF16),
            vmem((2, 4, 2, 2, 16, 256), BF16),
            vmem((PIECES, 8, 16, 256), BF16),
            vmem((1200, 16, 256), BF16),
            dma((3 + PIECES,)),
            dma((1,)),
            dma((max(40, RSEMS),)),
            dma((2,)),
            dma((4,)),
            dma((2, 4)),
            dma((6,)),
            pltpu.SemaphoreType.REGULAR,
            pltpu.SemaphoreType.REGULAR((8,)),
        ],
        compiler_params=pltpu.CompilerParams(collective_id=0, has_side_effects=True, vmem_limit_bytes=VMEM),
        name="layer",
    )(queries, keys, values, out_weight)
    return pl.pallas_call(
        last_kernel,
        out_shape=(jax.ShapeDtypeStruct((16, 8192), BF16),) * 2,
        in_specs=[in_hbm] * 3,
        out_specs=(in_hbm,) * 2,
        scratch_shapes=[
            vmem((PIECES, 8, 16, 256), BF16),
            vmem((16, 8192), BF16),
            vmem((64, 128), F32),
            vmem((16, 8192), F32),
            vmem((16, 8192), BF16),
            vmem((16, 8192), BF16),
            dma((8,)),
        ],
        compiler_params=pltpu.CompilerParams(vmem_limit_bytes=VMEM),
        name="final",
    )(sums, residual, norm_gain.reshape(64, 128))


def solution(mesh):
    finer = Mesh(mesh.devices.reshape(4, 16, 4, 2, 2), ("yl", "z", "x", "yh", "c"))
    rows, heads = ("yl", "z"), ("x", "yh", "c")
    both = rows + heads
    in_specs = (P(rows, heads), P(both, None), P(both, None), P(heads, rows), P(both, None), P())
    out_specs = (P(both, None), P(both, None))
    return jax.shard_map(local, mesh=finer, in_specs=in_specs, out_specs=out_specs, check_vma=False)
```

```python
import math

import jax
import jax.numpy as jnp
from jax import lax
from jax.experimental import pallas as pl
from jax.experimental.pallas import tpu as pltpu
from jax.sharding import Mesh
from jax.sharding import PartitionSpec as P

MESH = pl.DeviceIdType.MESH
F32, BF16 = jnp.float32, jnp.bfloat16
NT = (((1,), (1,)), ((), ()))

QC, WC = 0, 1
VMEM = 60 * 1024 * 1024
PIECES = 4

ORDER = (
    (0, 2, 3, 1, 4, 13, 5, 12, 6, 11, 7, 15, 10, 14, 8, 9),
    (1, 0, 4, 2, 3, 5, 6, 7, 13, 15, 12, 14, 11, 10, 9, 8),
    (2, 1, 3, 5, 0, 6, 4, 7, 15, 14, 13, 8, 9, 11, 10, 12),
    (3, 1, 0, 2, 5, 7, 4, 6, 8, 15, 9, 12, 10, 14, 11, 13),
    (4, 3, 2, 7, 0, 1, 6, 9, 15, 10, 14, 13, 11, 12, 5, 8),
    (5, 6, 7, 1, 2, 4, 0, 10, 9, 11, 15, 3, 13, 8, 12, 14),
    (6, 4, 3, 10, 7, 2, 1, 11, 9, 8, 12, 14, 13, 15, 5, 0),
    (7, 6, 9, 4, 3, 1, 2, 10, 5, 11, 12, 15, 8, 14, 0, 13),
    (8, 7, 9, 6, 10, 5, 3, 12, 11, 14, 4, 0, 2, 15, 13, 1),
    (9, 10, 8, 11, 6, 12, 7, 4, 14, 2, 5, 3, 15, 0, 1, 13),
    (10, 9, 11, 8, 7, 12, 13, 14, 4, 0, 1, 3, 2, 5, 6, 15),
    (11, 10, 12, 8, 13, 9, 15, 14, 0, 7, 5, 4, 2, 6, 1, 3),
    (12, 11, 13, 10, 9, 8, 15, 0, 14, 4, 7, 6, 5, 2, 1, 3),
    (13, 14, 15, 8, 0, 7, 2, 1, 6, 9, 4, 11, 10, 3, 5, 12),
    (14, 13, 15, 2, 1, 8, 6, 7, 9, 11, 0, 4, 10, 12, 5, 3),
    (15, 14, 13, 9, 12, 2, 11, 1, 10, 7, 8, 6, 0, 5, 4, 3),
)

FIRST = (
    (1, 2, 3, 5),
    (0, 2, 3, 4, 5),
    (0, 1, 3, 4, 6),
    (0, 2, 4, 6),
    (1, 2, 3, 5, 6, 7),
    (2, 3, 4, 6, 7),
    (2, 4, 5, 7),
    (2, 3, 5, 6),
    (3, 4, 5, 6, 7, 9, 10, 11, 12, 13),
    (4, 5, 6, 7, 8, 10, 11, 12),
    (0, 5, 6, 7, 8, 9, 11, 12, 13),
    (0, 6, 7, 9, 10, 12, 13),
    (0, 9, 10, 11, 13, 14, 15),
    (0, 3, 8, 10, 11, 12, 14, 15),
    (0, 1, 2, 3, 4, 8, 9, 10, 11, 13, 15),
    (0, 1, 2, 4, 11, 12, 13, 14),
)

ROUTES = (
    (
        (0, 0, 0, 0, 1, 5, 2, 3), (0, 0, 1, 0, 1, 5, 2, 3), (0, 0, 0, 2, 1), (0, 0, 1, 2, 1),
        (0, 1, 0, 0, 1, 3, 5, 2), (0, 1, 1, 0, 1, 3, 5, 2), (0, 0, 0, 3, 1), (0, 0, 1, 3, 1), (0, 0, 0, 1),
        (0, 0, 1, 1), (0, 1, 0, 2, 1), (3, 15), (3, 14), (1, 0, 0, 2, 14), (1, 0, 1, 2, 14), (1, 0, 0, 1, 14),
        (1, 0, 1, 1, 14), (1, 1, 0, 2, 14), (3, 13), (1, 0, 0, 0, 13), (1, 0, 1, 0, 13), (1, 1, 0, 0, 13),
        (1, 1, 1, 0, 13), (1, 0, 0, 1, 13), (1, 0, 1, 1, 13), (0, 1, 1, 2, 1, 14), (0, 1, 0, 3, 1), (0, 1, 1, 3, 1),
        (0, 0, 1, 13, 15, 1), (0, 1, 0, 1, 14, 13), (0, 0, 1, 12, 15, 3, 1), (0, 0, 0, 13, 15, 1),
        (0, 1, 1, 1, 14, 13), (0, 0, 0, 12, 15, 3, 1), (2, 0), (0, 0, 1, 11, 15, 1), (0, 0, 0, 11, 15, 1),
        (0, 0, 1, 10, 1, 15), (0, 0, 0, 10, 1, 15), (0, 1, 1, 13, 1, 15), (0, 1, 1, 12, 15, 3, 1),
        (0, 1, 0, 13, 1, 15), (2, 1), (0, 1, 0, 12, 15, 3, 1), (2, 2), (0, 1, 1, 11, 15, 1), (0, 1, 0, 11, 15, 1),
        (0, 0, 0, 8, 15, 1), (0, 1, 1, 10, 1, 15), (0, 0, 1, 8, 15, 1), (2, 3), (0, 1, 0, 10, 1, 15),
        (0, 1, 0, 8, 1, 15), (2, 4), (0, 1, 1, 8, 1, 15), (2, 5),
    ),
    (
        (0, 0, 0, 1, 5, 2), (0, 0, 1, 1, 5, 2), (0, 1, 0, 1, 5, 2), (0, 1, 1, 1, 5, 2), (0, 0, 0, 4, 0, 2, 3),
        (0, 0, 1, 4, 0, 2, 3), (0, 0, 0, 5, 0), (0, 0, 1, 5, 0), (3, 14), (0, 0, 1, 6, 0, 14), (0, 0, 0, 6, 0, 14),
        (0, 1, 0, 4, 2, 0, 3), (0, 1, 1, 4, 2, 0, 3), (2, 0), (0, 1, 0, 5, 0), (0, 0, 1, 13, 4, 2), (0, 1, 1, 5, 0),
        (2, 1), (0, 0, 0, 13, 4, 2), (0, 1, 1, 6, 0, 14), (0, 0, 1, 11, 2, 3), (0, 1, 0, 6, 0, 14),
        (0, 0, 0, 11, 2, 3), (2, 2), (0, 1, 1, 13, 4, 2), (0, 1, 0, 13, 4, 2), (0, 1, 1, 11, 3, 2), (2, 3),
        (0, 1, 0, 11, 3, 2), (2, 4), (2, 5),
    ),
    (
        (0, 0, 0, 2, 0, 4), (0, 0, 1, 2, 0, 4), (0, 0, 0, 1, 6, 3, 0), (0, 0, 1, 1, 6, 3, 0), (0, 1, 0, 2, 4, 0),
        (0, 1, 1, 2, 4, 0), (0, 0, 0, 5, 3, 1), (0, 0, 1, 5, 3, 1), (0, 0, 1, 6, 1, 4), (0, 0, 0, 6, 1, 4),
        (0, 1, 0, 1, 6, 0, 3), (0, 1, 1, 1, 6, 0, 3), (0, 0, 1, 7, 0, 1), (0, 0, 0, 7, 0, 1), (0, 1, 0, 5, 3, 1),
        (0, 1, 1, 5, 3, 1), (2, 0), (0, 0, 1, 15, 1, 3, 0, 4), (0, 0, 0, 15, 1, 3, 0, 4), (0, 0, 1, 14, 4, 0, 1),
        (0, 1, 1, 6, 4, 1), (0, 1, 0, 6, 4, 1), (2, 1), (0, 0, 0, 14, 4, 0, 1), (0, 1, 1, 7, 1, 0),
        (0, 1, 0, 7, 1, 0), (2, 2), (0, 1, 1, 15, 0, 4, 3, 1), (0, 1, 0, 15, 0, 4, 3, 1), (0, 1, 1, 14, 1, 0, 4),
        (0, 1, 0, 14, 1, 0, 4), (2, 3), (2, 4), (2, 5),
    ),
    (
        (0, 0, 0, 3, 4, 6, 2, 0), (0, 0, 1, 3, 4, 6, 2, 0), (0, 1, 0, 3, 4, 2, 0, 6), (0, 1, 1, 3, 4, 2, 0, 6),
        (0, 0, 0, 0, 4), (0, 0, 1, 0, 4), (0, 1, 0, 0, 4), (3, 14), (3, 13), (0, 0, 0, 8, 6, 2), (0, 1, 1, 0, 4),
        (2, 0), (0, 0, 1, 8, 6, 2), (2, 1), (0, 0, 1, 12, 2, 14, 13, 4), (2, 2), (0, 1, 0, 8, 2, 6),
        (0, 0, 0, 12, 2, 14, 13, 4), (0, 1, 1, 8, 2, 6), (0, 1, 1, 12, 2, 14, 13, 4), (0, 1, 0, 12, 2, 14, 13, 4),
        (2, 3), (2, 4), (2, 5),
    ),
    (
        (0, 0, 0, 4, 6, 1), (0, 0, 1, 4, 6, 1), (0, 0, 0, 2, 7, 6, 5, 3), (0, 0, 1, 2, 7, 6, 5, 3),
        (0, 1, 0, 4, 1, 6), (0, 1, 1, 4, 1, 6), (0, 1, 0, 2, 5, 3, 6, 7), (0, 1, 1, 2, 5, 3, 6, 7), (3, 15), (3, 14),
        (0, 0, 1, 9, 3, 5, 2, 6), (0, 0, 0, 9, 3, 5, 2, 6), (0, 0, 1, 15, 5, 7), (2, 0), (0, 0, 0, 15, 5, 7), (2, 1),
        (0, 1, 1, 9, 5, 6, 2, 3), (0, 0, 1, 14, 7, 6, 3), (0, 1, 0, 9, 5, 6, 2, 3), (2, 2), (0, 0, 0, 14, 7, 6, 3),
        (0, 0, 1, 13, 6, 3, 5), (0, 0, 0, 13, 6, 3, 5), (0, 1, 1, 15, 7, 5), (0, 1, 0, 15, 7, 5),
        (0, 1, 1, 14, 6, 7, 3), (0, 0, 0, 5, 15, 14, 6), (0, 1, 0, 14, 6, 7, 3), (0, 1, 1, 13, 3, 5, 6),
        (0, 1, 0, 13, 3, 5, 6), (0, 0, 1, 5, 15, 14, 6), (2, 3), (0, 1, 0, 5, 15, 14, 6), (2, 4),
        (0, 1, 1, 5, 15, 14, 6), (2, 5),
    ),
    (
        (0, 0, 0, 5, 2), (0, 0, 1, 5, 2), (0, 0, 0, 1, 4, 7), (0, 1, 0, 5, 2), (0, 1, 1, 5, 2), (0, 0, 1, 7, 4, 3, 6),
        (0, 0, 1, 1, 4, 7), (0, 0, 0, 7, 4, 3, 6), (3, 8), (1, 0, 0, 5, 8), (1, 0, 1, 5, 8), (1, 1, 0, 5, 8),
        (1, 1, 1, 5, 8), (3, 10), (1, 0, 0, 1, 10), (1, 0, 1, 1, 10), (0, 1, 1, 7, 3, 4, 6), (0, 1, 0, 1, 4, 7, 10),
        (0, 1, 0, 7, 3, 4, 6), (0, 1, 1, 1, 4, 7, 10), (2, 0), (2, 1), (0, 0, 1, 10, 3, 4, 2), (0, 0, 0, 10, 3, 4, 2),
        (0, 1, 1, 10, 4, 2, 3), (0, 1, 0, 10, 4, 2, 3), (2, 2), (2, 3), (2, 4), (2, 5),
    ),
    (
        (0, 0, 1, 6, 5, 2, 7), (0, 0, 0, 6, 5, 2, 7), (0, 0, 0, 3, 7), (0, 0, 0, 4, 7, 5), (0, 0, 1, 4, 7, 5),
        (0, 0, 1, 3, 7), (0, 1, 1, 6, 5, 2, 7), (0, 1, 0, 6, 5, 2, 7), (3, 9), (1, 0, 0, 4, 9), (1, 0, 1, 4, 9),
        (3, 8), (1, 0, 0, 3, 8), (1, 0, 1, 3, 8), (0, 1, 0, 3, 7, 8), (0, 1, 0, 4, 5, 7, 9), (0, 1, 1, 4, 5, 7, 9),
        (0, 0, 1, 10, 7, 5), (0, 0, 0, 10, 7, 5), (0, 1, 1, 3, 7, 8), (0, 0, 1, 11, 5, 4, 8), (0, 0, 0, 11, 5, 4, 8),
        (0, 1, 1, 10, 7, 5), (0, 1, 0, 10, 7, 5), (2, 0), (2, 1), (0, 1, 1, 11, 8, 4, 5), (0, 0, 0, 8, 5, 4, 7),
        (0, 0, 1, 8, 5, 4, 7), (0, 1, 0, 11, 8, 4, 5), (2, 2), (0, 1, 0, 8, 4, 5, 7), (0, 0, 1, 13, 9, 8, 7),
        (0, 0, 0, 13, 9, 8, 7), (0, 1, 1, 8, 4, 5, 7), (2, 3), (0, 1, 1, 13, 9, 8, 7), (0, 1, 0, 13, 9, 8, 7), (2, 4),
        (2, 5),
    ),
    (
        (0, 0, 1, 7, 5, 2), (0, 0, 0, 7, 5, 2), (0, 0, 1, 6, 3), (0, 0, 0, 6, 3), (0, 1, 1, 7, 5, 2), (3, 9),
        (1, 0, 1, 6, 9), (1, 0, 0, 6, 9), (0, 1, 0, 7, 5, 2), (3, 8), (1, 0, 1, 7, 8), (1, 0, 0, 7, 8),
        (1, 0, 1, 6, 8), (1, 0, 0, 6, 8), (1, 1, 1, 7, 8), (1, 1, 0, 7, 8), (3, 10), (1, 0, 1, 7, 10),
        (1, 0, 0, 7, 10), (1, 1, 1, 7, 10), (1, 1, 0, 7, 10), (0, 1, 1, 6, 8, 3, 9), (0, 1, 0, 6, 8, 3, 9), (2, 0),
        (2, 1), (2, 2), (0, 0, 1, 15, 9, 10, 8, 6), (0, 0, 0, 15, 9, 10, 8, 6), (0, 1, 1, 15, 9, 6, 10, 8),
        (0, 1, 0, 15, 9, 6, 10, 8), (2, 3), (2, 4), (2, 5),
    ),
    (
        (0, 0, 0, 8, 9, 12, 10, 3, 11), (0, 0, 1, 8, 9, 12, 10, 3, 11), (0, 1, 0, 8, 9, 11, 3, 12, 10),
        (0, 1, 1, 8, 9, 11, 3, 12, 10), (0, 0, 0, 3, 10, 13, 5, 9), (2, 0), (0, 0, 1, 3, 10, 13, 5, 9),
        (0, 0, 0, 5, 11, 4, 9, 7), (0, 0, 1, 5, 11, 4, 9, 7), (0, 1, 0, 5, 7, 11, 9, 4), (0, 1, 0, 3, 13, 9, 5, 10),
        (0, 1, 1, 5, 7, 11, 9, 4), (2, 1), (0, 1, 1, 3, 13, 9, 5, 10), (2, 2), (0, 0, 0, 0, 6, 7, 9),
        (0, 0, 1, 0, 6, 7, 9), (0, 1, 0, 0, 9, 7, 6), (0, 1, 1, 0, 9, 7, 6), (2, 3), (2, 4), (2, 5),
    ),
    (
        (0, 0, 1, 9, 7, 8, 10, 4, 12), (0, 0, 0, 9, 7, 8, 10, 4, 12), (0, 1, 1, 9, 4, 7, 8, 12, 10),
        (0, 1, 0, 9, 4, 7, 8, 12, 10), (0, 0, 1, 12, 7, 6, 5, 8), (0, 0, 0, 12, 7, 6, 5, 8), (0, 0, 0, 4, 8, 10, 12),
        (2, 0), (0, 0, 1, 4, 8, 10, 12), (0, 1, 1, 12, 5, 8, 6, 7), (0, 1, 0, 12, 5, 8, 6, 7), (2, 1),
        (0, 1, 0, 4, 12, 10, 8), (0, 1, 1, 4, 12, 10, 8), (2, 2), (0, 0, 0, 2, 11, 10, 8, 12),
        (0, 0, 1, 2, 11, 10, 8, 12), (0, 1, 0, 2, 11, 8, 12, 10), (0, 1, 1, 2, 11, 8, 12, 10), (2, 3), (2, 4), (2, 5),
    ),
    (
        (0, 0, 1, 10, 12, 9, 6, 0, 11, 8), (0, 0, 0, 10, 12, 9, 6, 0, 11, 8), (0, 1, 1, 10, 6, 11, 8, 0, 12, 9),
        (0, 1, 0, 10, 6, 11, 8, 0, 12, 9), (0, 0, 1, 7, 13, 9), (0, 0, 1, 14, 9, 12, 11, 5), (2, 0),
        (0, 0, 0, 7, 13, 9), (0, 1, 1, 7, 13, 9), (0, 0, 0, 14, 9, 12, 11, 5), (0, 1, 0, 7, 13, 9), (2, 1),
        (0, 1, 1, 14, 9, 12, 11, 5), (0, 1, 0, 14, 9, 12, 11, 5), (2, 2), (0, 0, 0, 1, 12, 8, 9, 11),
        (0, 0, 1, 1, 12, 8, 9, 11), (0, 1, 0, 1, 9, 12, 8, 11), (0, 1, 1, 1, 9, 12, 8, 11), (2, 3), (2, 4), (2, 5),
    ),
    (
        (0, 0, 1, 11, 6, 9, 0, 10, 12, 7), (0, 0, 0, 11, 6, 9, 0, 10, 12, 7), (0, 1, 1, 11, 6, 12, 9, 10, 7, 0),
        (0, 1, 0, 11, 6, 12, 9, 10, 7, 0), (2, 0), (2, 1), (0, 0, 0, 5, 13, 12, 10), (2, 2), (0, 0, 1, 5, 13, 12, 10),
        (0, 1, 0, 5, 13, 10, 12), (0, 1, 1, 5, 13, 10, 12), (2, 3), (2, 4), (2, 5),
    ),
    (
        (0, 0, 1, 12, 10, 0, 11, 9), (0, 0, 0, 12, 10, 0, 11, 9), (0, 1, 1, 12, 10, 9, 0, 11), (0, 0, 1, 9, 11, 15),
        (0, 1, 0, 12, 10, 9, 0, 11), (0, 0, 0, 9, 11, 15), (0, 0, 0, 8, 14, 0, 13), (0, 0, 1, 8, 14, 0, 13),
        (0, 1, 1, 9, 11, 15), (2, 0), (0, 1, 0, 9, 11, 15), (0, 1, 0, 8, 0, 14, 13), (0, 1, 1, 8, 0, 14, 13), (2, 1),
        (0, 0, 0, 0, 14, 10, 15, 11), (0, 0, 1, 0, 14, 10, 15, 11), (0, 0, 0, 4, 13, 11, 15, 14),
        (0, 0, 1, 4, 13, 11, 15, 14), (0, 1, 0, 0, 11, 15, 10, 14), (0, 1, 1, 0, 11, 15, 10, 14), (2, 2),
        (0, 1, 0, 4, 11, 14, 13, 15), (0, 1, 1, 4, 11, 14, 13, 15), (2, 3), (2, 4), (2, 5),
    ),
    (
        (0, 0, 1, 13, 11, 12, 0, 14, 10), (0, 0, 0, 13, 11, 12, 0, 14, 10), (0, 1, 1, 13, 0, 12, 11, 14, 10),
        (0, 1, 0, 13, 0, 12, 11, 14, 10), (0, 0, 0, 0, 12, 8), (0, 0, 1, 7, 12, 14, 15, 11), (0, 0, 1, 0, 12, 8),
        (0, 1, 0, 0, 12, 8), (0, 1, 1, 0, 12, 8), (2, 0), (0, 0, 0, 7, 12, 14, 15, 11), (0, 1, 1, 7, 11, 12, 15, 14),
        (0, 1, 0, 7, 11, 12, 15, 14), (2, 1), (0, 0, 0, 3, 11, 14, 12, 15), (2, 2), (0, 0, 1, 3, 11, 14, 12, 15),
        (0, 0, 1, 6, 12), (0, 0, 0, 6, 12), (0, 1, 1, 6, 12), (0, 1, 0, 6, 12), (2, 3), (0, 1, 0, 3, 15, 14, 11, 12),
        (0, 1, 1, 3, 15, 14, 11, 12), (2, 4), (2, 5),
    ),
    (
        (0, 0, 1, 14, 8, 10, 15, 13, 2), (0, 0, 0, 14, 8, 10, 15, 13, 2), (0, 1, 1, 14, 10, 8, 15, 2, 13),
        (0, 1, 0, 14, 10, 8, 15, 2, 13), (0, 0, 0, 2, 9, 13, 15), (0, 0, 1, 2, 9, 13, 15), (0, 0, 0, 1, 15),
        (0, 0, 1, 1, 15), (0, 1, 0, 2, 15, 9, 13), (0, 1, 1, 2, 15, 9, 13), (2, 0), (0, 0, 1, 6, 13, 10, 15, 11),
        (0, 1, 0, 1, 15), (0, 0, 0, 6, 13, 10, 15, 11), (0, 1, 1, 1, 15), (2, 1), (0, 1, 1, 6, 10, 13, 11, 15),
        (0, 1, 0, 6, 10, 13, 11, 15), (2, 2), (2, 3), (2, 4), (2, 5),
    ),
    (
        (0, 0, 1, 15, 12, 11, 14, 2, 13), (0, 0, 0, 15, 12, 11, 14, 2, 13), (0, 1, 1, 15, 2, 14, 11, 13, 12),
        (0, 1, 0, 15, 2, 14, 11, 13, 12), (0, 0, 1, 9, 14, 0, 13, 1), (0, 0, 0, 9, 14, 0, 13, 1),
        (0, 0, 1, 11, 14, 13), (0, 0, 0, 11, 14, 13), (0, 0, 1, 10, 14, 13), (0, 0, 0, 10, 14, 13),
        (0, 1, 1, 9, 1, 0, 14, 13), (0, 1, 0, 9, 1, 0, 14, 13), (2, 0), (0, 1, 1, 11, 13, 14), (0, 1, 0, 11, 13, 14),
        (2, 1), (0, 1, 1, 10, 13, 14), (2, 2), (0, 1, 0, 10, 13, 14), (2, 3), (2, 4), (2, 5),
    ),
)

ASIDE = (
    (),
    (),
    (),
    (),
    (),
    (),
    (),
    (),
    (),
    (),
    (),
    (),
    (),
    (),
    (),
    (),
)

SLOT = [{source: i for i, source in enumerate(order)} for order in ORDER]
RELAYS = [[tuple(step[1:4]) for step in route if step[0] == 0 and step[3] != z] for z, route in enumerate(ROUTES)]
BOUNDS = (0, 4, 6, 8, 12, 14, 16)
PART = [sum(slot >= bound for bound in BOUNDS[1:]) for slot in range(16)]
RSEMS = 11 + max(map(len, RELAYS))


def leaves(z, p):
    return [
        (wave, core, source)
        for source in ORDER[z][BOUNDS[p] : BOUNDS[p + 1]]
        for wave in range(2)
        for core in range(2)
        if source != z and (wave, core, source) not in RELAYS[z]
    ]


RING = (
    ("q_begin",), ("q_own",),
    ("q_relay", -1, 0, 0), ("q_relay", 1, 0, 0), ("q_relay", -1, 0, 1), ("q_relay", 1, 0, 1),
    ("k_own",),
    ("q_relay", -2, 0, 0), ("q_relay", 2, 0, 0), ("q_relay", -1, 1, 0), ("q_relay", 1, 1, 0),
    ("q_relay", -2, 0, 1), ("q_relay", 2, 0, 1), ("q_relay", -1, 1, 1), ("q_relay", 1, 1, 1),
    ("k_relay", -1), ("k_relay", 1),
    ("q_relay", -3, 0, 0), ("q_relay", 3, 0, 0), ("q_relay", -2, 1, 0), ("q_relay", 2, 1, 0),
    ("q_relay", -3, 0, 1), ("q_relay", 3, 0, 1), ("q_relay", -2, 1, 1), ("q_relay", 2, 1, 1),
    ("k_relay", -2), ("k_relay", 2),
    ("q_relay", -3, 1, 0), ("q_relay", 3, 1, 0), ("q_relay", -3, 1, 1), ("q_relay", 3, 1, 1),
    ("k_relay", -3), ("k_relay", 3),
)

LATE_RING = (
    ("q_begin",), ("q_own_first",),
    ("q_relay", -1, 1, 0), ("q_relay", 1, 1, 0), ("q_relay", -1, 1, 1), ("q_relay", 1, 1, 1),
    ("q_relay", -2, 1, 0), ("q_relay", 2, 1, 0), ("q_relay", -2, 1, 1), ("q_relay", 2, 1, 1),
    ("q_relay", -3, 1, 0), ("q_relay", 3, 1, 0), ("q_relay", -3, 1, 1), ("q_relay", 3, 1, 1),
    ("q_own_last",), ("k_own",),
    ("q_relay", -1, 0, 0), ("q_relay", 1, 0, 0), ("q_relay", -1, 0, 1), ("q_relay", 1, 0, 1),
    ("k_relay", -1), ("k_relay", 1),
    ("q_relay", -2, 0, 0), ("q_relay", 2, 0, 0), ("q_relay", -2, 0, 1), ("q_relay", 2, 0, 1),
    ("k_relay", -2), ("k_relay", 2),
    ("q_relay", -3, 0, 0), ("q_relay", 3, 0, 0), ("q_relay", -3, 0, 1), ("q_relay", 3, 0, 1),
    ("k_relay", -3), ("k_relay", 3),
)

PLAN_Q = (
    ("ring",),
    ("attend", 2), ("attend", 1), ("attend", 3),
    ("w_passed", 0), ("piece", 0, 1),
    ("q_last",), ("k_last",), ("attend", 0), ("piece", 0, 0),
    ("w_passed", 1), ("w_piece", 1, 0, 2), ("w_passed", 2), ("w_piece", 1, 2, 2),
    ("reduced", 0, 2), ("reduced", 0, 1), ("reduced", 0, 3), ("reduced", 0, 0),
    ("reduced", 1, 2), ("reduced", 1, 1), ("reduced", 1, 3), ("reduced", 1, 0),
)

PLAN_W = (
    ("w_begin",), ("w_route", 0),
    ("w_rest",), ("w_route", 1), ("w_piece", 3, 0, 2), ("w_route", 2), ("w_piece", 3, 2, 2),
    ("reduced", 2, 0), ("reduced", 2, 1), ("reduced", 2, 3), ("reduced", 2, 2),
    ("reduced", 3, 0), ("reduced", 3, 1), ("reduced", 3, 3), ("reduced", 3, 2),
)


def by_place(z, do, low=0, high=16):
    if high - low == 1:
        do(low)
        return
    middle = (low + high) // 2
    pl.when(z < middle)(lambda: by_place(z, do, low, middle))
    pl.when(z >= middle)(lambda: by_place(z, do, middle, high))


def kernel(
    q, k, v, w, sums,
    qall, kvl, kvr, wv, wt, wcross, wall, bias, att, psend, xr, ssend, rbuf, size,
    lsem, ssem, rsem, wpsem, atsem, xsem, asem, go, late,
):
    yl, z, x, yh, c = (lax.axis_index(a) for a in ("yl", "z", "x", "yh", "c"))
    y = yh * 4 + yl

    def dev(dy=0, dz=0, dx=0, to_z=None, role=None):
        yt = lax.rem(y + (dy + 8), 8)
        zt = lax.rem(z + (dz + 16), 16) if to_z is None else to_z
        xt = lax.rem(x + dx, 4)
        core = role if to_z else jnp.where(xt + yt + zt == 0, 1 - role, role)
        return (lax.rem(yt, 4), zt, xt, lax.div(yt, 4), core)

    origin = x + y + z == 0
    for_q = jnp.where(origin, 1 - QC, QC) == c
    one_more = jnp.where(origin, 0, 1)

    def remote(src, dst, send_sem, recv_sem, to):
        return pltpu.make_async_remote_copy(
            src_ref=src, dst_ref=dst, send_sem=send_sem, recv_sem=recv_sem, device_id=to, device_id_type=MESH
        )

    sent = [0]

    def send(src, dst, recv_sem, to):
        remote(src, dst, ssem.at[0], recv_sem, to).start()
        sent[0] += math.prod(src.shape) * 2

    def received(dst, recv_sem):
        remote(dst, dst, ssem.at[0], recv_sem, (yl, z, x, yh, 1 - c)).wait_recv()

    def sized(bytes_):
        assert bytes_ % 8192 == 0 and bytes_ // 8192 <= size.shape[0]
        return size.at[pl.ds(0, bytes_ // 8192)]

    def half_of(r):
        return lax.div(lax.rem(y + (r + 8), 8), 4)

    w_load = pltpu.make_async_copy(w, wv, lsem.at[0])
    q_load = pltpu.make_async_copy(q, qall.at[0, yh, c], lsem.at[1])
    kv_load = [pltpu.make_async_copy(k, kvl.at[0], lsem.at[2]), pltpu.make_async_copy(v, kvl.at[1], lsem.at[2])]
    barrier = pltpu.get_barrier_semaphore()
    around_q = [dict(dy=1), dict(dy=-1), dict(dx=1), dict(dx=2), dict(dx=3)]

    w_load.start()
    for copy in kv_load:
        copy.start()
    q_load.start()

    @pl.when(for_q)
    def _():
        for peer in around_q:
            pl.semaphore_signal(barrier, inc=1, device_id=dev(role=QC, **peer), device_id_type=MESH)

    @pl.when(~for_q)
    def _():
        pl.semaphore_signal(barrier, inc=1, device_id=dev(dy=4, role=WC), device_id_type=MESH)

        @pl.when(~origin)
        def _():
            pl.semaphore_signal(barrier, inc=1, device_id=dev(role=QC), device_id_type=MESH)

        def greet(place):
            for other in range(16):
                if place in FIRST[other]:
                    pl.semaphore_signal(barrier, inc=1, device_id=dev(to_z=other, role=WC), device_id_type=MESH)
                if place in ASIDE[other]:
                    to = dev(dy=4, to_z=other, role=WC)
                    pl.semaphore_signal(barrier, inc=1, device_id=to, device_id_type=MESH)

        by_place(z, greet)

    w_load.wait()
    wt[...] = wv[...].astype(F32).T.astype(BF16).reshape(2, 64, 256)
    for copy in kv_load:
        copy.wait()

    def lanes_of(half, core):
        return pl.ds(pl.multiple_of((half * 2 + core) * 256, 256), 256)

    def head_of(i):
        return pl.ds(pl.multiple_of(i * 128, 128), 128)

    def unit(slot, wave, core):
        return wall.at[slot, :, lanes_of(1 - yh if wave else yh, core)]

    def w_sem(place, wave, core, source):
        if (wave, core, source) in RELAYS[place]:
            return rsem.at[11 + RELAYS[place].index((wave, core, source))]
        return rsem.at[5 + PART[SLOT[place][source]]]

    def w_sends(place, wave, core, source, targets):
        for t in targets:
            here, there = SLOT[place][source], SLOT[t][source]
            to = dev(to_z=t, role=WC)
            send(unit(here, wave, core), unit(there, wave, core), w_sem(t, wave, core, source), to)

    def w_cross(place, core):
        for t in ASIDE[place]:
            there = wall.at[SLOT[t][place], :, lanes_of(yh, core)]
            send(wcross.at[core], there, w_sem(t, 1, core, place), dev(dy=4, to_z=t, role=WC))
        send(wcross.at[core], wall.at[0, :, lanes_of(yh, core)], rsem.at[2 + core], dev(dy=4, role=WC))

    waited = []

    def w_step(place, kind, *step):
        if kind == 3:
            pl.semaphore_wait(late.at[step[0] - 8], 1)
            return
        if kind == 2:
            p = step[0]
            if leaves(place, p):
                received(sized(len(leaves(place, p)) * 32768), rsem.at[5 + p])
            if p < 3:
                rows = pl.ds(BOUNDS[p], BOUNDS[p + 1] - BOUNDS[p])
                send(wall.at[rows], wall.at[rows], wpsem.at[p], dev(role=QC))
            return
        wave, core, source, *targets = step
        if kind == 0:
            if source != place:
                received(unit(SLOT[place][source], wave, core), w_sem(place, wave, core, source))
            elif wave:
                received(unit(0, 1, core), rsem.at[2 + core])
            else:
                if (core == QC or place == 0) and place not in waited:
                    received(sized(65536), rsem.at[4])
                    waited.append(place)
                w_cross(place, core)
        w_sends(place, wave, core, source, targets)

    def w_rows():
        for gs in (2, 1, 3, 0):
            a_got(gs)
        w_piece(2, 0, 4)

    def w_rest():
        before = sent[0]
        pl.when(z > 0)(w_rows)
        sent[0] = before

    def w_route(part):
        totals = []

        def go_on(place):
            route = ROUTES[place]
            first = 1 + max(i for i, step in enumerate(route) if step[0] != 2 or step[1] == 3)
            cuts = (0, first, max(first, 1 + route.index((2, 4))), len(route))
            start = sent[0]
            for step in route[cuts[part] : cuts[part + 1]]:
                with jax.named_scope("_".join(map(str, ("at", place, *step)))):
                    w_step(place, *step)
                if place == 0 and step == (2, 3):
                    extra = sent[0]
                    w_rows()
                    w_extra.append(sent[0] - extra)
                    sent[0] = extra
            totals.append(sent[0] - start)
            sent[0] = start

        by_place(z, go_on)
        w_totals.append(totals)

    w_totals, w_extra = [], []

    def w_passed(p):
        received(wall.at[pl.ds(BOUNDS[p], BOUNDS[p + 1] - BOUNDS[p])], wpsem.at[p])

    def q_part(r, s, u):
        return qall.at[r % 4, half_of(r), s, pl.ds(128 * u, 128)]

    def q_sem(t, s, u):
        return rsem.at[0 if t == 4 else 8 + 4 * (t if t < 4 else t - 1) + 2 * s + u]

    def q_send(r, s, u, hop):
        t = (r - hop) % 8
        rows = pl.ds(128 * u, 128)
        dst = qall.at[t % 4, half_of(r), s, rows]
        send(q_part(r, s, u), dst, q_sem(t, s, u), dev(dy=hop, role=QC))

    def q_relay(r, s, u):
        received(q_part(r, s, u), q_sem(r % 8, s, u))
        if abs(r) < 3 or s == (0 if r < 0 else 1):
            q_send(r, s, u, 1 if r < 0 else -1)

    def q_last():
        received(qall.at[0, half_of(4)], rsem.at[0])

    def k_send(r, hop):
        t = (r - hop) % 8
        some = pl.ds(0 if hop > 0 else 2, 2) if t == 4 else pl.ds(0, 4)
        src, dst = kvr.at[r % 4, half_of(r), some], kvr.at[t % 4, half_of(r), some]
        send(src, dst, rsem.at[t if t else 8], dev(dy=hop, role=QC))

    def k_relay(r):
        received(kvr.at[r % 4, half_of(r)], rsem.at[r % 8])
        k_send(r, 1 if r < 0 else -1)

    def k_last():
        received(kvr.at[0, half_of(4)], rsem.at[4])

    def k_spread():
        for d in (2, 1, 3):
            head = head_of(lax.rem(x + d, 4))
            send(kvl.at[:, :, head], kvr.at[0, yh, x, :, c], rsem.at[8], dev(dx=d, role=QC))

    def k_own():
        received(sized(7 * 8192), rsem.at[8])
        k_send(0, 1)
        k_send(0, -1)

    def ring():
        before = sent[0]
        for late, plan in ((False, RING), (True, LATE_RING)):
            sent[0] = before

            def go_round(plan=plan):
                for step in plan:
                    do(*step)

            pl.when((x + z == 0) if late else (x + z > 0))(go_round)

    def q_own_first():
        once(~origin, None, q_own)

    def q_own_last():
        before = sent[0]
        pl.when(origin)(q_own)
        sent[0] = before

    def w_hand():
        send(wt.at[yh], unit(0, 0, c), rsem.at[4], dev(role=WC))
        send(wt.at[1 - yh], wcross.at[c], rsem.at[4], dev(role=WC))

    def once(first, second, do):
        before = sent[0]
        pl.when(second if first is None else first)(do)
        if first is None:
            sent[0] = before

    def q_own():
        received(qall.at[0, yh, 1 - c], rsem.at[9])
        for u in range(2):
            for hop in (1, -1):
                q_send(0, 1 - c, u, hop)
        before = sent[0]
        pl.when(origin)(w_hand)
        sent[0] = before

    def q_begin():
        pl.semaphore_wait(barrier, len(around_q) + one_more)

        def meet():
            pl.semaphore_signal(go, inc=1, device_id=dev(role=WC), device_id_type=MESH)
            w_hand()

        once(~origin, None, meet)

        @pl.when(origin)
        def _():
            pl.semaphore_signal(barrier, inc=1, device_id=dev(role=WC), device_id_type=MESH)

        k_spread()
        kvr[0, yh, x, :, c] = kvl[:, :, head_of(x)]
        q_load.wait()
        for u in range(2):
            for hop in (1, -1):
                q_send(0, c, u, hop)
        row = lax.broadcasted_iota(jnp.int32, (128, 128), 0)
        col = lax.broadcasted_iota(jnp.int32, (128, 128), 1)
        bias[...] = jnp.where((lax.div(row, 32) == lax.div(col, 32)) & (col <= row), 0.0, -1e30)

    def w_begin():
        wall[0, :, lanes_of(yh, c)] = wt[yh]
        wcross[c] = wt[1 - yh]
        q_load.wait()

        def give():
            send(qall.at[0, yh, c], qall.at[0, yh, c], rsem.at[9], dev(role=QC))
            k_spread()
            send(kvl.at[:, :, head_of(x)], kvr.at[0, yh, x, :, c], rsem.at[8], dev(role=QC))

        def meet():
            pl.semaphore_wait(go, 1)
            give()

        once(~origin, None, meet)

        def greeted(place):
            pl.semaphore_wait(barrier, 2 + len(FIRST[place]) + len(ASIDE[place]) - one_more)
            for other in range(16):
                if (3, place) in ROUTES[other]:
                    to = dev(to_z=other, role=WC)
                    pl.semaphore_signal(late.at[place - 8], inc=1, device_id=to, device_id_type=MESH)

        by_place(z, greeted)
        once(None, origin, give)

    def attend(gs):
        for t in range(2):
            pair = kvr[gs, t]
            keys, values = pair[:, 0].reshape(128, 128), pair[:, 1].reshape(128, 128)
            values = jnp.concatenate([values, jnp.ones((128, 128), BF16)], axis=1)
            for h in range(2):
                queries = jnp.concatenate(
                    [
                        qall[gs, h, s, :, j * 128 : j * 128 + 128].reshape(4, 2, 32, 128)[:, t].reshape(128, 128)
                        for s in range(2)
                        for j in range(2)
                    ],
                    axis=0,
                )
                scores = lax.dot_general(queries, keys, NT, preferred_element_type=F32)
                scores = scores * (1.0 / math.sqrt(128.0)) + jnp.concatenate([bias[...]] * 4, axis=0)
                powers = jnp.exp(scores - jnp.max(scores, axis=-1, keepdims=True)).astype(BF16)
                total = jnp.dot(powers, values, preferred_element_type=F32)
                heads = (total[:, :128] / total[:, 128:]).astype(BF16)
                for i in range(4):
                    att[gs, t, :, h * 512 + i * 128 : h * 512 + i * 128 + 128] = heads[i * 128 : i * 128 + 128]
        send(att.at[gs], att.at[gs], atsem.at[gs], dev(role=WC))

    def a_got(gs):
        received(att.at[gs], atsem.at[gs])

    def spread(p, gs, lanes):
        for d in (2, 1, 3):
            src = psend.at[p % 2, gs, :, lax.rem(x + d, 4), :, lanes]
            dst = xr.at[p % 2, gs, d - 1, :, :, lanes]
            send(src, dst, xsem.at[p % 2, gs], dev(dx=d, role=QC if p < 2 else WC))

    def piece(p, which):
        groups = (slice(0, 1), slice(1, 4), slice(0, 4))[which]
        n = groups.stop - groups.start
        rows = wall[4 * p : 4 * p + 4].reshape(256, 1024)
        total = lax.dot_general(att[groups].reshape(n * 256, 1024), rows, NT, preferred_element_type=F32)
        psend[p, groups] = total.astype(BF16).reshape(n, 2, 4, 32, 256)
        for gs in ((0,), (2, 1, 3), (2, 1, 3, 0))[which]:
            spread(p, gs, pl.ds(0, 256))

    def w_piece(p, slot, n):
        slots = slice(4 * p + slot, 4 * p + slot + n)
        rows = wall[slots].reshape(64 * n, 1024)
        total = lax.dot_general(att[...].reshape(1024, 1024), rows, NT, preferred_element_type=F32)
        lanes = slice(64 * slot, 64 * (slot + n))
        psend[p % 2, :, :, :, :, lanes] = total.astype(BF16).reshape(4, 2, 4, 32, 64 * n)
        for gs in (0, 1, 3, 2):
            spread(p, gs, pl.ds(64 * slot, 64 * n))

    def reduced(p, gs):
        received(xr.at[p % 2, gs], xsem.at[p % 2, gs])
        total = psend[p % 2, gs, :, x].astype(F32)
        for d in range(3):
            total = total + xr[p % 2, gs, d].astype(F32)
        ssend[p % 2, gs] = total.astype(BF16).reshape(2, 2, 16, 256)
        for other in (1, 0):
            half = 1 - yh if other else yh
            there = half * 4 + lax.rem(yl + gs, 4)
            place = lax.rem(y + 8 - there, 8)
            for core in (1 - c, c):
                home = (lax.rem(yl + gs, 4), z, x, half, core)
                if gs or other:
                    send(ssend.at[p % 2, gs, half, core], rbuf.at[p, place], asem.at[p], home)
                elif core is c:
                    rbuf[p, 0] = ssend[p % 2, 0, yh, c]
                else:
                    send(ssend.at[p % 2, 0, yh, core], rbuf.at[p, 0], asem.at[4 + p % 2], home)

    steps = dict(
        q_begin=q_begin, w_begin=w_begin, q_own=q_own, q_relay=q_relay, q_last=q_last, k_own=k_own, k_relay=k_relay,
        k_last=k_last, attend=attend, w_route=w_route, w_passed=w_passed, a_got=a_got, piece=piece, w_piece=w_piece, w_rest=w_rest, reduced=reduced,
        ring=ring, q_own_first=q_own_first, q_own_last=q_own_last,
    )

    def do(name, *numbers):
        with jax.named_scope("_".join(map(str, (name, *numbers)))):
            steps[name](*numbers)

    def follow(plan):
        sent[0] = 0
        for step in plan:
            do(*step)

    def drain(bytes_):
        stand_in = sized(bytes_)
        remote(stand_in, stand_in, ssem.at[0], ssem.at[0], (yl, z, x, yh, 1 - c)).wait_send()

    def arrive(mine):
        with jax.named_scope("arrive"):
            outs = []
            for p in range(PIECES):
                received(rbuf.at[p, pl.ds(1, 7)], asem.at[p])
                if p // 2 != mine:
                    received(rbuf.at[p, 0], asem.at[4 + p % 2])
                outs.append(pltpu.make_async_copy(rbuf.at[p], sums.at[p], lsem.at[3 + p]))
                outs[-1].start()
            if mine:
                by_place(z, lambda place: drain(sent[0] + w_extra[0] + sum(totals[place] for totals in w_totals)))
            else:
                drain(sent[0])
            for copy in outs:
                copy.wait()

    @pl.when(for_q)
    def _():
        follow(PLAN_Q)
        arrive(0)

    @pl.when(~for_q)
    def _():
        follow(PLAN_W)
        arrive(1)


def last_kernel(sums, res, gain, hid, nrm, rbuf, resv, gv, u, hidv, nrmv, sem):
    yl, z, yh = (lax.axis_index(a) for a in ("yl", "z", "yh"))
    y = yh * 4 + yl
    loads = [
        pltpu.make_async_copy(res, resv, sem.at[0]),
        pltpu.make_async_copy(gain, gv, sem.at[0]),
    ]
    loads += [pltpu.make_async_copy(sums.at[p], rbuf.at[p], sem.at[1 + p]) for p in range(PIECES)]
    for copy in loads:
        copy.start()

    def source_of(slot):
        low, high = (
            sum(ORDER[8 * part + i][slot] << (4 * i) for i in range(8)) for part in range(2)
        )
        low, high = (n - (1 << 32) if n >> 31 else n for n in (low, high))
        word = jnp.where(z < 8, jnp.int32(low), jnp.int32(high))
        return lax.shift_right_logical(word, 4 * lax.rem(z, 8)) & 15

    for copy in loads[:2]:
        copy.wait()
    squares = jnp.zeros((16, 128), F32)
    low = lax.broadcasted_iota(jnp.int32, (16, 128), 1) < 64
    for p in range(PIECES):
        sources = [source_of(4 * p + i) for i in range(4)]
        loads[2 + p].wait()
        for r in range(4):
            here = lax.div(lax.rem(y + r, 8), 4)
            first, second = r + 4 * here, r + 4 - 4 * here
            for t in range(2):
                lanes = slice(t * 128, t * 128 + 128)
                a = rbuf[p, first, :, lanes].astype(F32)
                b = rbuf[p, second, :, lanes].astype(F32)
                pair = (jnp.where(low, a, pltpu.roll(b, 64, 1)), jnp.where(low, pltpu.roll(a, 64, 1), b))
                for i in range(2):
                    block = lax.rem(yl + r, 4) * 16 + sources[2 * t + i]
                    at = pl.ds(pl.multiple_of(block * 128, 128), 128)
                    updated = resv[:, at].astype(F32) + pair[i]
                    u[:, at] = updated
                    hidv[:, at] = updated.astype(BF16)
                    squares = squares + updated * updated
    stores = [pltpu.make_async_copy(hidv, hid, sem.at[5])]
    stores[0].start()
    scale = lax.rsqrt(jnp.sum(squares, axis=-1, keepdims=True) * (1.0 / 8192.0) + 1e-05)
    for part in range(2):
        for block in range(32 * part, 32 * part + 32):
            lanes = slice(block * 128, block * 128 + 128)
            nrmv[:, lanes] = (u[:, lanes] * scale * gv[block : block + 1, :]).astype(BF16)
        lanes = pl.ds(4096 * part, 4096)
        stores.append(pltpu.make_async_copy(nrmv.at[:, lanes], nrm.at[:, lanes], sem.at[6 + part]))
        stores[-1].start()
    for copy in stores:
        copy.wait()


def local(queries, keys, values, out_weight, residual, norm_gain):
    in_hbm = pl.BlockSpec(memory_space=pltpu.HBM)
    vmem = pltpu.VMEM
    dma = pltpu.SemaphoreType.DMA
    sums = pl.pallas_call(
        kernel,
        out_shape=jax.ShapeDtypeStruct((PIECES, 8, 16, 256), BF16),
        in_specs=[in_hbm] * 4,
        out_specs=in_hbm,
        scratch_shapes=[
            vmem((4, 2, 2, 256, 256), BF16),
            vmem((2, 16, 512), BF16),
            vmem((4, 2, 4, 2, 2, 16, 128), BF16),
            vmem((256, 128), BF16),
            vmem((2, 64, 256), BF16),
            vmem((2, 64, 256), BF16),
            vmem((16, 64, 1024), BF16),
            vmem((128, 128), F32),
            vmem((4, 2, 128, 1024), BF16),
            vmem((2, 4, 2, 4, 32, 256), BF16),
            vmem((2, 4, 3, 2, 32, 256), BF16),
            vmem((2, 4, 2, 2, 16, 256), BF16),
            vmem((PIECES, 8, 16, 256), BF16),
            vmem((1200, 16, 256), BF16),
            dma((3 + PIECES,)),
            dma((1,)),
            dma((max(40, RSEMS),)),
            dma((3,)),
            dma((4,)),
            dma((2, 4)),
            dma((6,)),
            pltpu.SemaphoreType.REGULAR,
            pltpu.SemaphoreType.REGULAR((8,)),
        ],
        compiler_params=pltpu.CompilerParams(collective_id=0, has_side_effects=True, vmem_limit_bytes=VMEM),
        name="layer",
    )(queries, keys, values, out_weight)
    return pl.pallas_call(
        last_kernel,
        out_shape=(jax.ShapeDtypeStruct((16, 8192), BF16),) * 2,
        in_specs=[in_hbm] * 3,
        out_specs=(in_hbm,) * 2,
        scratch_shapes=[
            vmem((PIECES, 8, 16, 256), BF16),
            vmem((16, 8192), BF16),
            vmem((64, 128), F32),
            vmem((16, 8192), F32),
            vmem((16, 8192), BF16),
            vmem((16, 8192), BF16),
            dma((8,)),
        ],
        compiler_params=pltpu.CompilerParams(vmem_limit_bytes=VMEM),
        name="final",
    )(sums, residual, norm_gain.reshape(64, 128))


def solution(mesh):
    finer = Mesh(mesh.devices.reshape(4, 16, 4, 2, 2), ("yl", "z", "x", "yh", "c"))
    rows, heads = ("yl", "z"), ("x", "yh", "c")
    both = rows + heads
    in_specs = (P(rows, heads), P(both, None), P(both, None), P(heads, rows), P(both, None), P())
    out_specs = (P(both, None), P(both, None))
    return jax.shard_map(local, mesh=finer, in_specs=in_specs, out_specs=out_specs, check_vma=False)
```
